32 devices in a mesh: dp: 8 (over z, x), tensor: 4 (over y, core).
Axes of the slice: x: 2, y: 2, z: 4, core: 2. Of those that a mesh axis runs over, the one named last changes fastest.
Arguments:
- hidden_in: bfloat16 [8192, 2048], P('dp', 'tensor'), may hold values from -6 to 6
- seg_ids: int32 [16, 512], P('dp'), may hold values from 0 to 15, never falling along the last dimension, each value on 1 to 256 neighbouring positions
- attn_gain: float32 [2048], replicated, may hold values from 0.5 to 1.5
- query_key_value_weight: bfloat16 [3, 2048, 2048], P(None, None, 'tensor'), may hold values from -0.125 to 0.125
- conv_weight: bfloat16 [3, 4, 2048], P(None, None, 'tensor'), may hold values from -3 to 3
- write_strength_weight: bfloat16 [2048, 16], P(None, 'tensor'), may hold values from -0.125 to 0.125
- onorm_gain: float32 [128], replicated, may hold values from 0.5 to 1.5
- output_projection_weight: bfloat16 [2048, 2048], P('tensor'), may hold values from -0.125 to 0.125
- mlp_gain: float32 [2048], replicated, may hold values from 0.5 to 1.5
- gate_up_projection_weight: bfloat16 [2, 2048, 5632], P(None, None, 'tensor'), may hold values from -0.125 to 0.125
- down_projection_weight: bfloat16 [5632, 2048], P('tensor'), may hold values from -0.078125 to 0.078125
- cotangent: bfloat16 [8192, 2048], P('dp', 'tensor'), may hold values from -6 to 6
Outputs:
- layer_out: bfloat16 [8192, 2048], P('dp', 'tensor')
- grad_in: bfloat16 [8192, 2048], P('dp', 'tensor')
- grad_attn_gain: float32 [2048], replicated
- grad_qkv: float32 [3, 2048, 2048], P(None, 'dp', 'tensor')
- grad_conv: float32 [3, 4, 2048], P(None, None, 'tensor')
- grad_beta: float32 [2048, 16], P('dp', 'tensor')
- grad_onorm: float32 [128], replicated
- grad_out: float32 [2048, 2048], P('tensor', 'dp')
- grad_mlp_gain: float32 [2048], replicated
- grad_gate_up: float32 [2, 2048, 5632], P(None, 'dp', 'tensor')
- grad_down: float32 [5632, 2048], P('tensor', 'dp')
The draws below stay inside these ranges and needn't reach their ends.
Inputs may be any that keep to these rules, and one draw needn't show every extreme that they name: seg_ids never fall along a sequence; tokens with equal ids in one sequence form one document.
All inputs are finite; a program needn't handle non-finite values.
Results may differ from the reference program's by a relative error of at most 0.018.
Values may be sent and summed in bfloat16 or wider, within the bound.
A program may use at most 320 MiB of HBM per device.

```python
import math
import jax
import jax.numpy as jnp
import numpy as np
from jax import lax

D = 2048
H = 16
HEAD_DIM = 128
FF = 5632
CONV_SIZE = 4
SPAN = 64
SEQS = 2
SEQ_LEN = 512
KD = 2048
NSEQ = 16
TOKENS = 8192
N_DP = 8


def block_levels(own_key, shape, shards, smallest, high):
    def one(axis_at, shards_of):
        steps = jax.random.uniform(jax.random.fold_in(jax.random.fold_in(own_key, 6), axis_at), (shards_of,), jnp.float32, smallest / len(shards), high / len(shards))
        return jnp.repeat(jnp.exp(steps), shape[axis_at] // shards_of).reshape((-1,) + (1,) * (len(shape) - axis_at - 1))

    loudness = one(*shards[0])
    for cut in shards[1:]:
        loudness = loudness * one(*cut)
    return loudness


def profile(amount, total, limit, skew):
    weights = [(1 << 20) // math.isqrt(rank ** skew) + 1 for rank in range(2, amount + 1)]
    spare, holding = total - limit - (amount - 1), [1] * (amount - 1)
    while spare > 0:
        candidates = [i for i in range(amount - 1) if holding[i] < limit]
        pool, remaining = sum([weights[i] for i in candidates]), spare
        for i in candidates:
            more = min(limit - holding[i], max(1, remaining * weights[i] // pool), spare)
            holding[i] = holding[i] + more
            spare = spare - more
    return np.array([limit] + holding)


def ragged(own_key, number_of, total, limit, lean):
    if number_of == 2:
        one = jax.random.randint(own_key, (), max(1, total - limit), min(limit, total - 1) + 1)
        return jnp.stack([one, total - one])
    tallies = jnp.asarray(profile(number_of, total, limit, lean), jnp.int32)
    couples = (number_of - 1) // 2
    source_of, sink = tallies[1:1 + 2 * couples:2], tallies[2:2 + 2 * couples:2]
    margin = jnp.minimum(source_of - 1, limit - sink)
    moved = jax.random.randint(jax.random.fold_in(own_key, 1), (couples,), 0, 1 << 20) % (margin + 1)
    tallies = tallies.at[1:1 + 2 * couples:2].set(source_of - moved).at[2:2 + 2 * couples:2].set(sink + moved)
    return tallies[jax.random.permutation(jax.random.fold_in(own_key, 2), number_of)]


def gaussian(rng, extent, width, limit, pieces=(), held_as=jnp.bfloat16):
    entries = width * jax.random.normal(rng, extent, jnp.float32)
    if pieces:
        entries = entries * block_levels(rng, extent, pieces, -0.22, 0.18)
    return jnp.clip(entries, -limit, limit).astype(held_as)


def setup_inputs(seed: int = 0) -> dict:
    streams_of = jax.random.split(jax.random.key(seed), 13)
    return {
        "hidden_in": gaussian(streams_of[0], (TOKENS, D), 1.0, 6.0, ((0, 8), (1, 4))),
        "seg_ids": jax.vmap(lambda own: jnp.searchsorted(jnp.cumsum(ragged(own, SEQ_LEN // 32, SEQ_LEN, SEQ_LEN // 2, 2)), jnp.arange(SEQ_LEN), side="right"))(jax.random.split(streams_of[1], NSEQ)).reshape((NSEQ, SEQ_LEN)).astype(jnp.int32),
        "attn_gain": jnp.clip(1.0 + 0.1 * jax.random.normal(streams_of[2], (D,), jnp.float32), 0.5, 1.5),
        "query_key_value_weight": gaussian(streams_of[3], (3, D, KD), D ** -0.5, 0.125, ((2, 4),)),
        "conv_weight": gaussian(streams_of[4], (3, CONV_SIZE, KD), 0.5, 3.0, ((2, 4),)),
        "write_strength_weight": gaussian(streams_of[5], (D, H), D ** -0.5, 0.125, ((1, 4),)),
        "onorm_gain": jnp.clip(1.0 + 0.1 * jax.random.normal(streams_of[6], (HEAD_DIM,), jnp.float32), 0.5, 1.5),
        "output_projection_weight": gaussian(streams_of[7], (KD, D), KD ** -0.5, 0.125, ((0, 4),)),
        "mlp_gain": jnp.clip(1.0 + 0.1 * jax.random.normal(streams_of[8], (D,), jnp.float32), 0.5, 1.5),
        "gate_up_projection_weight": gaussian(streams_of[9], (2, D, FF), D ** -0.5, 0.125, ((2, 4),)),
        "down_projection_weight": gaussian(streams_of[10], (FF, D), FF ** -0.5, 0.078125, ((0, 4),)),
        "cotangent": gaussian(streams_of[11], (TOKENS, D), 1.0, 6.0, ((0, 8), (1, 4))),
    }


EPS = 1e-06
HIGH_ACCURACY = lax.Precision.HIGHEST

@jax.custom_vjp
def low(v):
    return lax.optimization_barrier(v.astype(jnp.bfloat16)).astype(jnp.float32)

@jax.custom_vjp
def low_back(v):
    return v

def low_keep(v):
    return (low(v), None)

def low_pass(kept, grad):
    return (grad,)

def back_keep(v):
    return (v, None)

def back_low(kept, grad):
    return (low(grad),)
low.defvjp(low_keep, low_pass)
low_back.defvjp(back_keep, back_low)

def rms_scale(values):
    return lax.rsqrt(lax.optimization_barrier(jnp.mean(values * values, axis=-1, keepdims=True)) + EPS)

def unit_length(values):
    return values * lax.rsqrt(lax.optimization_barrier(jnp.sum(values * values, axis=-1, keepdims=True)) + EPS)

def short_conv(projected_rows, segments, weight):
    length = projected_rows.shape[2]
    result = jnp.zeros_like(projected_rows)
    for offset in range(CONV_SIZE):
        moved = jnp.pad(projected_rows, ((0, 0), (0, 0), (offset, 0), (0, 0)))[:, :, :length]
        moved_seg = jnp.pad(segments, ((0, 0), (offset, 0)), constant_values=-1)[:, :length]
        same_doc = (moved_seg == segments).astype(jnp.float32)
        result = result + weight[:, CONV_SIZE - 1 - offset][:, None, None, :] * moved * same_doc[None, :, :, None]
    return result

def delta_rule(queries, keys_in, values, beta_rate, segments):
    seq_count = queries.shape[0]
    length = queries.shape[1]
    head_count = queries.shape[2]
    head_width = queries.shape[3]
    prior = jnp.pad(segments, ((0, 0), (1, 0)), constant_values=-1)[:, :length]
    keep_flag = (prior == segments).astype(jnp.float32)

    def token_step(memory, inputs):
        query_t, key_t, value_t, rate_t, keep_t = inputs
        memory = memory * keep_t[:, None, None, None]
        recalled = jnp.einsum('shk,shkv->shv', key_t, memory, precision=HIGH_ACCURACY)
        memory = memory + rate_t[:, :, None, None] * key_t[:, :, :, None] * (value_t - recalled)[:, :, None, :]
        output_t = jnp.einsum('shk,shkv->shv', query_t, memory, precision=HIGH_ACCURACY)
        return (memory, output_t)

    def block_step(memory, block):
        return lax.scan(token_step, memory, block)
    block_fn = jax.checkpoint(block_step)

    def arrange(array):
        moved = jnp.moveaxis(array, 1, 0)
        return moved.reshape((length // SPAN, SPAN) + moved.shape[1:])
    scaled = queries * head_width ** (-0.5)
    start = jnp.zeros((seq_count, head_count, head_width, head_width), jnp.float32)
    final_state, outputs = lax.scan(block_fn, start, (arrange(scaled), arrange(keys_in), arrange(values), arrange(beta_rate), arrange(keep_flag)))
    outputs = outputs.reshape((length,) + outputs.shape[2:])
    return jnp.moveaxis(outputs, 0, 1)

def forward(params, hidden_f, segments):
    attn_gain, query_key_value_weight, conv_weight, write_strength_weight, onorm_gain, output_projection_weight, mlp_gain, gate_up_projection_weight, down_projection_weight = params
    seq_count = hidden_f.shape[0]
    length = hidden_f.shape[1]
    normalized_input = low(hidden_f * rms_scale(hidden_f) * attn_gain)
    projected_rows = low_back(jnp.einsum('gqu,tum->tgqm', normalized_input, query_key_value_weight, precision=HIGH_ACCURACY))
    output_logits = low_back(jnp.einsum('tue,er->tur', normalized_input, write_strength_weight, precision=HIGH_ACCURACY))
    beta_rate = jax.nn.sigmoid(output_logits)
    act = jax.nn.silu(short_conv(projected_rows, segments, conv_weight))
    shaped = act.reshape(3, seq_count, length, H, HEAD_DIM)
    queries = low(unit_length(shaped[0]))
    keys_in = low(unit_length(shaped[1]))
    values = low(shaped[2])
    mixed = delta_rule(queries, keys_in, values, beta_rate, segments)
    normalized_output = low(mixed * rms_scale(mixed) * onorm_gain).reshape(seq_count, length, KD)
    attention_output = low_back(jnp.einsum('jxv,vr->jxr', normalized_output, output_projection_weight, precision=HIGH_ACCURACY))
    middle = hidden_f + attention_output
    normalized_middle = low(middle * rms_scale(middle) * mlp_gain)
    gate_up_product = low_back(jnp.einsum('tik,jkx->jtix', normalized_middle, gate_up_projection_weight, precision=HIGH_ACCURACY))
    hidden_activation = low(jax.nn.silu(gate_up_product[0]) * gate_up_product[1])
    feedforward_output = low_back(jnp.einsum('yhe,eg->yhg', hidden_activation, down_projection_weight, precision=HIGH_ACCURACY))
    return middle + feedforward_output

def reference(hidden_in, seg_ids, attn_gain, query_key_value_weight, conv_weight, write_strength_weight, onorm_gain, output_projection_weight, mlp_gain, gate_up_projection_weight, down_projection_weight, cotangent):
    params = tuple((param.astype(jnp.float32) for param in (attn_gain, query_key_value_weight, conv_weight, write_strength_weight, onorm_gain, output_projection_weight, mlp_gain, gate_up_projection_weight, down_projection_weight)))
    grouped_in = hidden_in.reshape(N_DP, SEQS, SEQ_LEN, D)
    grouped_seg = seg_ids.reshape(N_DP, SEQS, SEQ_LEN)
    grouped_cot = cotangent.reshape(N_DP, SEQS, SEQ_LEN, D)

    def group_step(totals, inputs):
        block_in, block_seg, block_cot = inputs

        def local_fn(hidden_f, *weights):
            return forward(weights, hidden_f, block_seg)
        result, pullback = jax.vjp(local_fn, block_in.astype(jnp.float32), *params)
        grads = pullback(block_cot.astype(jnp.float32))
        totals = tuple((total + piece for total, piece in zip(totals, grads[1:])))
        return (totals, (result.astype(jnp.bfloat16), grads[0].astype(jnp.bfloat16)))
    zeros = tuple((jnp.zeros_like(param) for param in params))
    totals, (outputs, grads_in) = lax.scan(group_step, zeros, (grouped_in, grouped_seg, grouped_cot))
    return (outputs.reshape(-1, D), grads_in.reshape(-1, D), totals[0], totals[1], totals[2], totals[3], totals[4], totals[5], totals[6], totals[7], totals[8])
```

```python
import jax
import jax.numpy as jnp
from jax import lax
from jax.experimental import pallas as pl
from jax.experimental.pallas import tpu as pltpu
from jax.sharding import PartitionSpec as P

HEAD_DIM = 128
TAPS = 4
CHUNK = 128
HALO = 8
EPS = 1e-06
PAIR = 2
F32 = jnp.float32
BF16 = jnp.bfloat16


def dot_nn(a, b):
    return jnp.dot(a.astype(BF16), b.astype(BF16), preferred_element_type=F32)


def dot_nt(a, b):
    return lax.dot_general(a.astype(BF16), b.astype(BF16), (((1,), (1,)), ((), ())), preferred_element_type=F32)


def dot_tn(a, b):
    return lax.dot_general(a.astype(BF16), b.astype(BF16), (((0,), (0,)), ((), ())), preferred_element_type=F32)


def column(row):
    return jnp.broadcast_to(row, (CHUNK, CHUNK)).T


def load_segments(seg_ref, segcol, length):
    segcol[0:HALO, :] = jnp.full((HALO, CHUNK), -1.0, F32)
    segcol[HALO + length :, :] = jnp.full((HALO, CHUNK), -2.0, F32)
    for n in range(length // CHUNK):
        row = seg_ref[0, :, n * CHUNK : (n + 1) * CHUNK].astype(F32)
        segcol[HALO + n * CHUNK : HALO + (n + 1) * CHUNK, :] = column(row)


def seg_rows(segcol, n, shift):
    base = HALO + n * CHUNK + shift
    return segcol[base : base + CHUNK, :]


def back_masks(segcol, n):
    here = seg_rows(segcol, n, 0)
    return [None] + [(seg_rows(segcol, n, -s) == here).astype(F32) for s in range(1, TAPS)]


def state_masks(seg_ref, segcol, n):
    here = seg_rows(segcol, n, 0)
    row = jnp.broadcast_to(seg_ref[0, :, n * CHUNK : (n + 1) * CHUNK].astype(F32), (CHUNK, CHUNK))
    same = here == row
    before = segcol[HALO + n * CHUNK - 1 : HALO + n * CHUNK, :]
    last = segcol[HALO + (n + 1) * CHUNK - 1 : HALO + (n + 1) * CHUNK, :]
    carry = (here == before).astype(F32)
    tail = (here == last).astype(F32)
    carry_last = (last == before).astype(F32)
    return same, carry, tail, carry_last


def taps_in(proj_ref, c, h, n):
    lanes = slice(h * HEAD_DIM, (h + 1) * HEAD_DIM)
    if n == 0:
        return jnp.concatenate([jnp.zeros((HALO, HEAD_DIM), F32), proj_ref[c, 0:CHUNK, lanes].astype(F32)], axis=0)
    return proj_ref[c, n * CHUNK - HALO : (n + 1) * CHUNK, lanes].astype(F32)


def conv_rows(window, weight_ref, c, h, masks):
    lanes = slice(h * HEAD_DIM, (h + 1) * HEAD_DIM)
    total = weight_ref[c, TAPS - 1 : TAPS, lanes] * window[HALO:]
    for s in range(1, TAPS):
        total = total + weight_ref[c, TAPS - 1 - s : TAPS - s, lanes] * (masks[s] * window[HALO - s : HALO - s + CHUNK])
    return total


def grid_ids():
    rows = lax.broadcasted_iota(jnp.int32, (CHUNK, CHUNK), 0)
    cols = lax.broadcasted_iota(jnp.int32, (CHUNK, CHUNK), 1)
    return rows, cols


def forward_kernel(proj_ref, seg_ref, weight_ref, logit_ref, gain_ref, out_ref, mixed_ref, inv_ref, score_ref, state_ref, delta_ref, err_ref, segcol):
    length = proj_ref.shape[1]
    chunks = length // CHUNK
    load_segments(seg_ref, segcol, length)
    rows, cols = grid_ids()
    apart = rows ^ cols
    lower = rows > cols
    lower_incl = rows >= cols
    scale = HEAD_DIM**-0.5
    pieces, systems, inverses = {}, {}, {}
    for n in range(chunks):
        masks = back_masks(segcol, n)
        same, carry, tail, carry_last = state_masks(seg_ref, segcol, n)
        span = slice(n * CHUNK, (n + 1) * CHUNK)
        for h in range(PAIR):
            acts = []
            for c in range(3):
                conv = conv_rows(taps_in(proj_ref, c, h, n), weight_ref, c, h, masks)
                acts.append(conv * jax.nn.sigmoid(conv))
            q = (acts[0] * lax.rsqrt(jnp.sum(acts[0] * acts[0], axis=-1, keepdims=True) + EPS)).astype(BF16)
            k = (acts[1] * lax.rsqrt(jnp.sum(acts[1] * acts[1], axis=-1, keepdims=True) + EPS)).astype(BF16)
            v = acts[2].astype(BF16).astype(F32)
            rate = jax.nn.sigmoid(column(logit_ref[h, :, span]))
            gram = jnp.where(same & lower, dot_nt(k, k), 0.0)
            scores = (jnp.where(same & lower_incl, dot_nt(q, k), 0.0) * scale).astype(BF16)
            system = rate * gram
            score_ref[h, span, :] = scores
            systems[n, h] = system
            inverses[n, h] = jnp.where(rows == cols, 1.0, 0.0) - jnp.where(apart == 1, system, 0.0)
            pieces[n, h] = (q, k.astype(F32), v, gram, scores, rate, carry, tail, carry_last)
    level = 1
    while (2 << level) <= CHUNK:
        crossed = {}
        for key, inverse in inverses.items():
            crossed[key] = dot_nn(jnp.where((apart >> level) == 1, systems[key], 0.0), inverse)
        for key, inverse in inverses.items():
            inverses[key] = inverse - dot_nn(inverse, crossed[key])
        level += 1
    for n, h in pieces:
        q, kf, v, gram, scores, rate, carry, tail, carry_last = pieces[n, h]
        inverse = inverses[n, h].astype(BF16)
        inv_ref[h, n * CHUNK : (n + 1) * CHUNK, :] = inverse
        base = dot_nn(inverse, rate * v)
        back = dot_nn(inverse, rate * carry * kf)
        pieces[n, h] = (q, kf, v, gram, scores, base, back, carry, tail, carry_last)
    for h in range(PAIR):
        lanes = slice(h * HEAD_DIM, (h + 1) * HEAD_DIM)
        state = None
        for n in range(chunks):
            span = slice(n * CHUNK, (n + 1) * CHUNK)
            q, kf, v, gram, scores, base, back, carry, tail, carry_last = pieces[n, h]
            if n == 0:
                delta = base
                rest = v
                state_ref[h, span, :] = jnp.zeros((CHUNK, CHUNK), BF16)
            else:
                low = state.astype(BF16)
                state_ref[h, span, :] = low
                delta = base - dot_nn(back, low)
                rest = v - carry * dot_nn(kf, low)
            delta_low = delta.astype(BF16)
            moved = dot_tn(tail * kf, delta_low)
            mixed = dot_nn(scores, delta_low)
            if n > 0:
                mixed = mixed + (carry * scale) * dot_nn(q, low)
                moved = moved + carry_last * state
            state = moved
            delta_ref[span, lanes] = delta_low
            err_ref[span, lanes] = (rest - dot_nn(gram, delta_low)).astype(BF16)
            mixed_ref[span, lanes] = mixed
            root = lax.rsqrt(jnp.mean(mixed * mixed, axis=-1, keepdims=True) + EPS)
            out_ref[span, lanes] = (mixed * root * gain_ref[...]).astype(BF16)


def backward_kernel(proj_ref, seg_ref, weight_ref, logit_ref, gain_ref, mixed_ref, inv_ref, score_ref, state_ref, delta_ref, err_ref, nout_ref,
                    gproj_ref, glogit_ref, gconv_ref, gonorm_ref, segcol, gin_ref, act_ref, q_ref, k_ref, head_ref, dq_ref, dk_ref):
    length = proj_ref.shape[1]
    chunks = length // CHUNK
    pair, seq = pl.program_id(0), pl.program_id(1)
    load_segments(seg_ref, segcol, length)
    rows, cols = grid_ids()
    lower = rows > cols
    lower_incl = rows >= cols
    scale = HEAD_DIM**-0.5

    @pl.when((pair == 0) & (seq == 0))
    def _():
        gonorm_ref[...] = jnp.zeros_like(gonorm_ref)

    @pl.when(seq == 0)
    def _():
        gconv_ref[...] = jnp.zeros_like(gconv_ref)

    onorm = jnp.zeros((1, HEAD_DIM), F32)
    pieces = {}
    for n in range(chunks):
        masks = back_masks(segcol, n)
        same, carry, tail, carry_last = state_masks(seg_ref, segcol, n)
        span = slice(n * CHUNK, (n + 1) * CHUNK)
        for h in range(PAIR):
            lanes = slice(h * HEAD_DIM, (h + 1) * HEAD_DIM)
            for c in range(3):
                act_ref[h, c, span, :] = conv_rows(taps_in(proj_ref, c, h, n), weight_ref, c, h, masks)
            conv = act_ref[h, 0, span, :]
            act = conv * jax.nn.sigmoid(conv)
            q = (act * lax.rsqrt(jnp.sum(act * act, axis=-1, keepdims=True) + EPS)).astype(BF16)
            conv = act_ref[h, 1, span, :]
            act = conv * jax.nn.sigmoid(conv)
            k = (act * lax.rsqrt(jnp.sum(act * act, axis=-1, keepdims=True) + EPS)).astype(BF16)
            q_ref[h, span, :] = q
            k_ref[h, span, :] = k
            mixed = mixed_ref[span, lanes]
            root = lax.rsqrt(jnp.mean(mixed * mixed, axis=-1, keepdims=True) + EPS)
            unit = mixed * root
            grad = nout_ref[span, lanes].astype(F32)
            onorm = onorm + jnp.sum(grad * unit, axis=0, keepdims=True)
            scaled = grad * gain_ref[...]
            gmix = root * (scaled - unit * jnp.mean(scaled * unit, axis=-1, keepdims=True))
            glow = gmix.astype(BF16)
            inverse = inv_ref[h, span, :]
            delta = delta_ref[span, lanes]
            gscore = (jnp.where(same & lower_incl, dot_nt(glow, delta), 0.0) * scale).astype(BF16)
            dq = dot_nn(gscore, k)
            held = (scale * carry * gmix).astype(BF16)
            if n > 0:
                dq = dq + dot_nt(held, state_ref[h, span, :])
            dq_ref[h, span, :] = dq
            dk_ref[h, span, :] = dot_tn(gscore, q)
            start = dot_tn(inverse, dot_tn(score_ref[h, span, :], glow))
            kf = k.astype(F32)
            reach = dot_tn(inverse, tail * kf).astype(BF16)
            feed = dot_tn(q, held)
            pieces[n, h] = (start, reach, feed)
    gonorm_ref[...] += onorm
    for h in range(PAIR):
        lanes = slice(h * HEAD_DIM, (h + 1) * HEAD_DIM)
        flow = None
        for n in reversed(range(chunks)):
            span = slice(n * CHUNK, (n + 1) * CHUNK)
            same, carry, tail, carry_last = state_masks(seg_ref, segcol, n)
            rate = jax.nn.sigmoid(column(logit_ref[h, :, span]))
            start, reach, feed = pieces[n, h]
            k = k_ref[h, span, :]
            delta = delta_ref[span, lanes]
            gtarget = start
            if flow is not None:
                low = flow.astype(BF16)
                gtarget = gtarget + dot_nn(reach, low)
            gval = rate * gtarget
            head_ref[h, span, :] = gval
            grecall = (carry * gval).astype(BF16)
            dk = dk_ref[h, span, :]
            if flow is not None:
                dk = dk + tail * dot_nt(delta, low)
            if n > 0:
                dk = dk - dot_nt(grecall, state_ref[h, span, :])
                nxt = feed - dot_tn(k, grecall)
                if flow is not None:
                    nxt = nxt + carry_last * flow
                flow = nxt
            ggram = jnp.where(same & lower, dot_nt(gval, delta), 0.0)
            dk_ref[h, span, :] = dk - dot_nn(ggram + ggram.T, k)
            grate = jnp.sum(err_ref[span, lanes].astype(F32) * gtarget, axis=-1, keepdims=True)
            glogit = jnp.broadcast_to(grate, (CHUNK, CHUNK)) * rate * (1.0 - rate)
            glogit_ref[h, :, span] = glogit.T[0:1, :].astype(BF16)
    for h in range(PAIR):
        lanes = slice(h * HEAD_DIM, (h + 1) * HEAD_DIM)
        for c in range(3):
            gin_ref[h, c, length:, :] = jnp.zeros((HALO, HEAD_DIM), F32)
        taps = [[jnp.zeros((1, HEAD_DIM), F32)] * TAPS for _ in range(3)]
        for n in range(chunks):
            masks = back_masks(segcol, n)
            span = slice(n * CHUNK, (n + 1) * CHUNK)
            for c in range(3):
                conv = act_ref[h, c, span, :]
                gate = jax.nn.sigmoid(conv)
                act = conv * gate
                if c == 2:
                    gact = head_ref[h, span, :]
                else:
                    gunit = (dq_ref if c == 0 else dk_ref)[h, span, :]
                    inv = lax.rsqrt(jnp.sum(act * act, axis=-1, keepdims=True) + EPS)
                    unit = act * inv
                    gact = inv * (gunit - unit * jnp.sum(gunit * unit, axis=-1, keepdims=True))
                gin = gact * (gate + act * (1.0 - gate))
                gin_ref[h, c, span, :] = gin
                window = taps_in(proj_ref, c, h, n)
                taps[c][TAPS - 1] = taps[c][TAPS - 1] + jnp.sum(gin * window[HALO:], axis=0, keepdims=True)
                for s in range(1, TAPS):
                    part = jnp.sum(gin * masks[s] * window[HALO - s : HALO - s + CHUNK], axis=0, keepdims=True)
                    taps[c][TAPS - 1 - s] = taps[c][TAPS - 1 - s] + part
        for c in range(3):
            gconv_ref[c, :, lanes] += jnp.concatenate(taps[c], axis=0)
        for n in range(chunks):
            span = slice(n * CHUNK, (n + 1) * CHUNK)
            here = seg_rows(segcol, n, 0)
            ahead = [None] + [(seg_rows(segcol, n, s) == here).astype(F32) for s in range(1, TAPS)]
            for c in range(3):
                total = weight_ref[c, TAPS - 1 : TAPS, lanes] * gin_ref[h, c, span, :]
                for s in range(1, TAPS):
                    later = gin_ref[h, c, n * CHUNK + s : (n + 1) * CHUNK + s, :]
                    total = total + weight_ref[c, TAPS - 1 - s : TAPS - s, lanes] * (ahead[s] * later)
                gproj_ref[c, span, lanes] = total.astype(BF16)


def mixer_shapes(proj, seg):
    seqs, length = seg.shape
    return seqs, length, proj.shape[2] // HEAD_DIM


def mixer_forward(proj, seg, weight, logits, gain):
    seqs, length, heads = mixer_shapes(proj, seg)
    tokens = seqs * length
    wide = PAIR * HEAD_DIM
    flat = pl.BlockSpec((length, wide), lambda s, p: (s, p))
    square = pl.BlockSpec((PAIR, length, CHUNK), lambda s, p: (p, s, 0))
    return pl.pallas_call(
        forward_kernel,
        grid=(seqs, heads // PAIR),
        in_specs=[
            pl.BlockSpec((3, length, wide), lambda s, p: (0, s, p)),
            pl.BlockSpec((1, 1, length), lambda s, p: (s, 0, 0)),
            pl.BlockSpec((3, TAPS, wide), lambda s, p: (0, 0, p)),
            pl.BlockSpec((PAIR, 1, length), lambda s, p: (p, 0, s)),
            pl.BlockSpec((1, HEAD_DIM), lambda s, p: (0, 0)),
        ],
        out_specs=[flat, flat, square, square, square, flat, flat],
        out_shape=[
            jax.ShapeDtypeStruct((tokens, heads * HEAD_DIM), BF16),
            jax.ShapeDtypeStruct((tokens, heads * HEAD_DIM), F32),
            jax.ShapeDtypeStruct((heads, tokens, CHUNK), BF16),
            jax.ShapeDtypeStruct((heads, tokens, CHUNK), BF16),
            jax.ShapeDtypeStruct((heads, tokens, CHUNK), BF16),
            jax.ShapeDtypeStruct((tokens, heads * HEAD_DIM), BF16),
            jax.ShapeDtypeStruct((tokens, heads * HEAD_DIM), BF16),
        ],
        scratch_shapes=[pltpu.VMEM((length + 2 * HALO, CHUNK), F32)],
        compiler_params=pltpu.CompilerParams(vmem_limit_bytes=48 << 20),
        name="mixer_forward",
    )(proj, seg.reshape(seqs, 1, length), weight, logits, gain.reshape(1, HEAD_DIM))


def mixer_backward(proj, seg, weight, logits, gain, kept, grad_nout):
    seqs, length, heads = mixer_shapes(proj, seg)
    tokens = seqs * length
    wide = PAIR * HEAD_DIM
    mixed, inverse, scores, states, delta, err = kept
    flat = pl.BlockSpec((length, wide), lambda p, s: (s, p))
    square = pl.BlockSpec((PAIR, length, CHUNK), lambda p, s: (p, s, 0))
    cube = pl.BlockSpec((3, length, wide), lambda p, s: (0, s, p))
    taps = pl.BlockSpec((3, TAPS, wide), lambda p, s: (0, 0, p))
    line = pl.BlockSpec((PAIR, 1, length), lambda p, s: (p, 0, s))
    vector = pl.BlockSpec((1, HEAD_DIM), lambda p, s: (0, 0))
    return pl.pallas_call(
        backward_kernel,
        grid=(heads // PAIR, seqs),
        in_specs=[cube, pl.BlockSpec((1, 1, length), lambda p, s: (s, 0, 0)), taps, line, vector, flat, square, square, square, flat, flat, flat],
        out_specs=[cube, line, taps, vector],
        out_shape=[
            jax.ShapeDtypeStruct(proj.shape, BF16),
            jax.ShapeDtypeStruct((heads, 1, tokens), BF16),
            jax.ShapeDtypeStruct(weight.shape, F32),
            jax.ShapeDtypeStruct((1, HEAD_DIM), F32),
        ],
        scratch_shapes=[
            pltpu.VMEM((length + 2 * HALO, CHUNK), F32),
            pltpu.VMEM((PAIR, 3, length + HALO, HEAD_DIM), F32),
            pltpu.VMEM((PAIR, 3, length, HEAD_DIM), F32),
            pltpu.VMEM((PAIR, length, HEAD_DIM), BF16),
            pltpu.VMEM((PAIR, length, HEAD_DIM), BF16),
            pltpu.VMEM((PAIR, length, HEAD_DIM), F32),
            pltpu.VMEM((PAIR, length, HEAD_DIM), F32),
            pltpu.VMEM((PAIR, length, HEAD_DIM), F32),
        ],
        compiler_params=pltpu.CompilerParams(vmem_limit_bytes=48 << 20),
        name="mixer_backward",
    )(proj, seg.reshape(seqs, 1, length), weight, logits, gain.reshape(1, HEAD_DIM), mixed, inverse, scores, states, delta, err, grad_nout)


ROWS = (((0,), (0,)), ((), ()))
COLS = (((1,), (1,)), ((), ()))


def rms_scale(values):
    return lax.rsqrt(jnp.mean(values * values, axis=-1, keepdims=True) + EPS)


def norm_back(grad_normed, unit_rows, scale_rows, gain):
    scaled_grad = grad_normed * gain
    grad_rows = scale_rows * (scaled_grad - unit_rows * jnp.mean(scaled_grad * unit_rows, axis=-1, keepdims=True))
    return grad_rows, jnp.sum(grad_normed * unit_rows, axis=0)


def butterfly(values, axis, size):
    step = 1
    while step < size:
        pairs = [(i, i ^ step) for i in range(size)]
        values = values + lax.ppermute(values, axis, pairs)
        step *= 2
    return values


def scatter_sum(values, axis, dim):
    return lax.psum_scatter(values.astype(BF16), axis, scatter_dimension=dim, tiled=True).astype(F32)


def make_body(dp_size, tensor_size):
    def body(hidden_in, seg_ids, attn_gain, wqkv, conv_weight, wrate, onorm_gain, wout, mlp_gain, wgu, wdown, cotangent):
        tokens = hidden_in.shape[0]
        heads = wrate.shape[1]
        dot = lambda a, b, dims: lax.dot_general(a, b, dims, preferred_element_type=F32)
        taps = conv_weight.astype(F32)
        full_in = lax.all_gather(hidden_in, "tensor", axis=1, tiled=True).astype(F32)
        scale_one = rms_scale(full_in)
        unit_one = full_in * scale_one
        normed_one = (unit_one * attn_gain).astype(BF16)
        proj = jnp.einsum("td,cdk->ctk", normed_one, wqkv, preferred_element_type=F32)
        logits = jnp.einsum("td,dh->ht", normed_one, wrate, preferred_element_type=F32).reshape(heads, 1, tokens)
        out_low, *kept = mixer_forward(proj, seg_ids, taps, logits, onorm_gain)
        attn_part = jnp.dot(out_low, wout, preferred_element_type=F32)
        middle = hidden_in.astype(F32) + scatter_sum(attn_part, "tensor", 1)
        full_mid = lax.all_gather(middle.astype(BF16), "tensor", axis=1, tiled=True).astype(F32)
        full_cot = lax.all_gather(cotangent, "tensor", axis=1, tiled=True)
        scale_two = rms_scale(full_mid)
        unit_two = full_mid * scale_two
        normed_two = (unit_two * mlp_gain).astype(BF16)
        gate_up = jnp.einsum("td,cdf->ctf", normed_two, wgu, preferred_element_type=F32)
        gate_pre, up_pre = gate_up[0], gate_up[1]
        gate_sig = jax.nn.sigmoid(gate_pre)
        hidden = (gate_pre * gate_sig * up_pre).astype(BF16)
        grad_hidden = dot(full_cot, wdown, COLS)
        grad_up = grad_hidden * gate_pre * gate_sig
        grad_gate = grad_hidden * up_pre * gate_sig * (1.0 + gate_pre * (1.0 - gate_sig))
        grad_pair = jnp.stack([grad_gate, grad_up]).astype(BF16)
        grad_nmid = jnp.einsum("ctf,cdf->td", grad_pair, wgu, preferred_element_type=F32)
        part_two, gain_two = norm_back(grad_nmid, unit_two, scale_two, mlp_gain)
        grad_middle = cotangent.astype(F32) + scatter_sum(part_two, "tensor", 1)
        full_grad_mid = lax.all_gather(grad_middle.astype(BF16), "tensor", axis=1, tiled=True)
        grad_down = dot(hidden, full_cot, ROWS)
        grad_gate_up = jnp.einsum("td,ctf->cdf", normed_two, grad_pair, preferred_element_type=F32)
        ffn_part = jnp.dot(hidden, wdown, preferred_element_type=F32)
        layer_out = (middle + scatter_sum(ffn_part, "tensor", 1)).astype(BF16)
        grad_nout = dot(full_grad_mid, wout, COLS)
        grad_out = dot(out_low, full_grad_mid, ROWS)
        grad_proj, grad_logits, grad_conv, gain_onorm = mixer_backward(proj, seg_ids, taps, logits, onorm_gain, kept, grad_nout)
        grad_logits = grad_logits.reshape(heads, tokens)
        grad_nin = jnp.einsum("ctk,cdk->td", grad_proj, wqkv, preferred_element_type=F32)
        grad_nin = grad_nin + jnp.einsum("ht,dh->td", grad_logits, wrate, preferred_element_type=F32)
        grad_qkv = jnp.einsum("td,ctk->cdk", normed_one, grad_proj, preferred_element_type=F32)
        grad_beta = jnp.einsum("td,ht->dh", normed_one, grad_logits, preferred_element_type=F32)
        part_one, gain_one = norm_back(grad_nin, unit_one, scale_one, attn_gain)
        grad_in = (grad_middle + scatter_sum(part_one, "tensor", 1)).astype(BF16)
        width = gain_one.shape[0]
        flat = jnp.concatenate([gain_one, gain_two, gain_onorm.reshape(-1), grad_conv.reshape(-1), grad_beta.reshape(-1)])
        shared = 2 * width + HEAD_DIM
        flat = butterfly(flat, "dp", dp_size)
        gains = butterfly(flat[:shared], "tensor", tensor_size)
        grad_conv = flat[shared : shared + grad_conv.size].reshape(grad_conv.shape)
        mine = grad_beta.shape[0] // dp_size
        grad_beta = flat[shared + grad_conv.size :].reshape(grad_beta.shape)
        grad_beta = lax.dynamic_slice_in_dim(grad_beta, lax.axis_index("dp") * mine, mine, 0)
        return (
            layer_out,
            grad_in,
            gains[:width],
            scatter_sum(grad_qkv, "dp", 1),
            grad_conv,
            grad_beta,
            gains[2 * width :],
            scatter_sum(grad_out, "dp", 1),
            gains[width : 2 * width],
            scatter_sum(grad_gate_up, "dp", 1),
            scatter_sum(grad_down, "dp", 1),
        )

    return body


def solution(mesh):
    return jax.shard_map(
        make_body(mesh.shape["dp"], mesh.shape["tensor"]),
        mesh=mesh,
        in_specs=(
            P("dp", "tensor"),
            P("dp", None),
            P(),
            P(None, None, "tensor"),
            P(None, None, "tensor"),
            P(None, "tensor"),
            P(),
            P("tensor", None),
            P(),
            P(None, None, "tensor"),
            P("tensor", None),
            P("dp", "tensor"),
        ),
        out_specs=(
            P("dp", "tensor"),
            P("dp", "tensor"),
            P(),
            P(None, "dp", "tensor"),
            P(None, None, "tensor"),
            P("dp", "tensor"),
            P(),
            P("tensor", "dp"),
            P(),
            P(None, "dp", "tensor"),
            P("tensor", "dp"),
        ),
        check_vma=False,
    )
```

```python
import jax
import jax.numpy as jnp
from jax import lax
from jax.experimental import pallas as pl
from jax.experimental.pallas import tpu as pltpu
from jax.experimental.layout import Layout, with_layout_constraint
from jax.sharding import PartitionSpec as P

HEAD_DIM = 128
TAPS = 4
CHUNK = 128
HALO = 8
EPS = 1e-06
PAIR = 2
F32 = jnp.float32
BF16 = jnp.bfloat16


def dot_nn(a, b):
    return jnp.dot(a.astype(BF16), b.astype(BF16), preferred_element_type=F32)


def dot_nt(a, b):
    return lax.dot_general(a.astype(BF16), b.astype(BF16), (((1,), (1,)), ((), ())), preferred_element_type=F32)


def dot_tn(a, b):
    return lax.dot_general(a.astype(BF16), b.astype(BF16), (((0,), (0,)), ((), ())), preferred_element_type=F32)


def column(row):
    return jnp.broadcast_to(row, (CHUNK, CHUNK)).T


def logit_row(logit_ref, head, span):
    values = logit_ref[:, span]
    return jnp.sum(jnp.where(lax.broadcasted_iota(jnp.int32, values.shape, 0) == head, values, 0.0), axis=0, keepdims=True)


def load_segments(seg_ref, segcol, length):
    segcol[0:HALO, :] = jnp.full((HALO, CHUNK), -1.0, F32)
    segcol[HALO + length :, :] = jnp.full((HALO, CHUNK), -2.0, F32)
    for n in range(length // CHUNK):
        row = seg_ref[0, :, n * CHUNK : (n + 1) * CHUNK].astype(F32)
        segcol[HALO + n * CHUNK : HALO + (n + 1) * CHUNK, :] = column(row)


def seg_rows(segcol, n, shift):
    base = HALO + n * CHUNK + shift
    return segcol[base : base + CHUNK, :]


def back_masks(segcol, n):
    here = seg_rows(segcol, n, 0)
    return [None] + [(seg_rows(segcol, n, -s) == here).astype(F32) for s in range(1, TAPS)]


def state_masks(seg_ref, segcol, n):
    here = seg_rows(segcol, n, 0)
    row = jnp.broadcast_to(seg_ref[0, :, n * CHUNK : (n + 1) * CHUNK].astype(F32), (CHUNK, CHUNK))
    same = here == row
    before = segcol[HALO + n * CHUNK - 1 : HALO + n * CHUNK, :]
    last = segcol[HALO + (n + 1) * CHUNK - 1 : HALO + (n + 1) * CHUNK, :]
    carry = (here == before).astype(F32)
    tail = (here == last).astype(F32)
    carry_last = (last == before).astype(F32)
    return same, carry, tail, carry_last


def taps_in(proj_ref, c, h, n):
    lanes = slice(h * HEAD_DIM, (h + 1) * HEAD_DIM)
    if n == 0:
        return jnp.concatenate([jnp.zeros((HALO, HEAD_DIM), F32), proj_ref[c, 0:CHUNK, lanes].astype(F32)], axis=0)
    return proj_ref[c, n * CHUNK - HALO : (n + 1) * CHUNK, lanes].astype(F32)


def conv_rows(window, weight_ref, c, h, masks):
    lanes = slice(h * HEAD_DIM, (h + 1) * HEAD_DIM)
    total = weight_ref[c, TAPS - 1 : TAPS, lanes] * window[HALO:]
    for s in range(1, TAPS):
        total = total + weight_ref[c, TAPS - 1 - s : TAPS - s, lanes] * (masks[s] * window[HALO - s : HALO - s + CHUNK])
    return total


def grid_ids():
    rows = lax.broadcasted_iota(jnp.int32, (CHUNK, CHUNK), 0)
    cols = lax.broadcasted_iota(jnp.int32, (CHUNK, CHUNK), 1)
    return rows, cols


def forward_kernel(proj_ref, seg_ref, weight_ref, logit_ref, gain_ref, out_ref, mixed_ref, inv_ref, score_ref, state_ref, delta_ref, err_ref, segcol):
    length = proj_ref.shape[1]
    chunks = length // CHUNK
    load_segments(seg_ref, segcol, length)
    rows, cols = grid_ids()
    apart = rows ^ cols
    lower = rows > cols
    lower_incl = rows >= cols
    scale = HEAD_DIM**-0.5
    pieces, systems, inverses = {}, {}, {}
    for n in range(chunks):
        masks = back_masks(segcol, n)
        same, carry, tail, carry_last = state_masks(seg_ref, segcol, n)
        span = slice(n * CHUNK, (n + 1) * CHUNK)
        for h in range(PAIR):
            acts = []
            for c in range(3):
                conv = conv_rows(taps_in(proj_ref, c, h, n), weight_ref, c, h, masks)
                acts.append(conv * jax.nn.sigmoid(conv))
            q = (acts[0] * lax.rsqrt(jnp.sum(acts[0] * acts[0], axis=-1, keepdims=True) + EPS)).astype(BF16)
            k = (acts[1] * lax.rsqrt(jnp.sum(acts[1] * acts[1], axis=-1, keepdims=True) + EPS)).astype(BF16)
            v = acts[2].astype(BF16).astype(F32)
            rate = jax.nn.sigmoid(column(logit_row(logit_ref, PAIR * pl.program_id(1) + h, span)))
            gram = jnp.where(same & lower, dot_nt(k, k), 0.0)
            scores = (jnp.where(same & lower_incl, dot_nt(q, k), 0.0) * scale).astype(BF16)
            system = rate * gram
            score_ref[h, span, :] = scores
            systems[n, h] = system
            inverses[n, h] = jnp.where(rows == cols, 1.0, 0.0) - jnp.where(apart == 1, system, 0.0)
            pieces[n, h] = (q, k.astype(F32), v, gram, scores, rate, carry, tail, carry_last)
    level = 1
    while (2 << level) <= CHUNK:
        crossed = {}
        for key, inverse in inverses.items():
            crossed[key] = dot_nn(jnp.where((apart >> level) == 1, systems[key], 0.0), inverse)
        for key, inverse in inverses.items():
            inverses[key] = inverse - dot_nn(inverse, crossed[key])
        level += 1
    for n, h in pieces:
        q, kf, v, gram, scores, rate, carry, tail, carry_last = pieces[n, h]
        inverse = inverses[n, h].astype(BF16)
        inv_ref[h, n * CHUNK : (n + 1) * CHUNK, :] = inverse
        base = dot_nn(inverse, rate * v)
        back = dot_nn(inverse, rate * carry * kf)
        pieces[n, h] = (q, kf, v, gram, scores, base, back, carry, tail, carry_last)
    for h in range(PAIR):
        lanes = slice(h * HEAD_DIM, (h + 1) * HEAD_DIM)
        state = None
        for n in range(chunks):
            span = slice(n * CHUNK, (n + 1) * CHUNK)
            q, kf, v, gram, scores, base, back, carry, tail, carry_last = pieces[n, h]
            if n == 0:
                delta = base
                rest = v
                state_ref[h, span, :] = jnp.zeros((CHUNK, CHUNK), BF16)
            else:
                low = state.astype(BF16)
                state_ref[h, span, :] = low
                delta = base - dot_nn(back, low)
                rest = v - carry * dot_nn(kf, low)
            delta_low = delta.astype(BF16)
            moved = dot_tn(tail * kf, delta_low)
            mixed = dot_nn(scores, delta_low)
            if n > 0:
                mixed = mixed + (carry * scale) * dot_nn(q, low)
                moved = moved + carry_last * state
            state = moved
            delta_ref[span, lanes] = delta_low
            err_ref[span, lanes] = (rest - dot_nn(gram, delta_low)).astype(BF16)
            mixed_ref[span, lanes] = mixed
            root = lax.rsqrt(jnp.mean(mixed * mixed, axis=-1, keepdims=True) + EPS)
            out_ref[span, lanes] = (mixed * root * gain_ref[...]).astype(BF16)


def backward_kernel(proj_ref, seg_ref, weight_ref, logit_ref, gain_ref, mixed_ref, inv_ref, score_ref, state_ref, delta_ref, err_ref, nout_ref,
                    gproj_ref, glogit_ref, gconv_ref, gonorm_ref, segcol, gin_ref, act_ref, q_ref, k_ref, head_ref, dq_ref, dk_ref):
    length = proj_ref.shape[1]
    chunks = length // CHUNK
    pair, seq = pl.program_id(0), pl.program_id(1)
    load_segments(seg_ref, segcol, length)
    rows, cols = grid_ids()
    lower = rows > cols
    lower_incl = rows >= cols
    scale = HEAD_DIM**-0.5

    @pl.when((pair == 0) & (seq == 0))
    def _():
        gonorm_ref[...] = jnp.zeros_like(gonorm_ref)

    @pl.when(seq == 0)
    def _():
        gconv_ref[...] = jnp.zeros_like(gconv_ref)

    onorm = jnp.zeros((1, HEAD_DIM), F32)
    pieces = {}
    for n in range(chunks):
        masks = back_masks(segcol, n)
        same, carry, tail, carry_last = state_masks(seg_ref, segcol, n)
        span = slice(n * CHUNK, (n + 1) * CHUNK)
        for h in range(PAIR):
            lanes = slice(h * HEAD_DIM, (h + 1) * HEAD_DIM)
            for c in range(3):
                act_ref[h, c, span, :] = conv_rows(taps_in(proj_ref, c, h, n), weight_ref, c, h, masks)
            conv = act_ref[h, 0, span, :]
            act = conv * jax.nn.sigmoid(conv)
            q = (act * lax.rsqrt(jnp.sum(act * act, axis=-1, keepdims=True) + EPS)).astype(BF16)
            conv = act_ref[h, 1, span, :]
            act = conv * jax.nn.sigmoid(conv)
            k = (act * lax.rsqrt(jnp.sum(act * act, axis=-1, keepdims=True) + EPS)).astype(BF16)
            q_ref[h, span, :] = q
            k_ref[h, span, :] = k
            mixed = mixed_ref[span, lanes]
            root = lax.rsqrt(jnp.mean(mixed * mixed, axis=-1, keepdims=True) + EPS)
            unit = mixed * root
            grad = nout_ref[span, lanes].astype(F32)
            onorm = onorm + jnp.sum(grad * unit, axis=0, keepdims=True)
            scaled = grad * gain_ref[...]
            gmix = root * (scaled - unit * jnp.mean(scaled * unit, axis=-1, keepdims=True))
            glow = gmix.astype(BF16)
            inverse = inv_ref[h, span, :]
            delta = delta_ref[span, lanes]
            gscore = (jnp.where(same & lower_incl, dot_nt(glow, delta), 0.0) * scale).astype(BF16)
            dq = dot_nn(gscore, k)
            held = (scale * carry * gmix).astype(BF16)
            if n > 0:
                dq = dq + dot_nt(held, state_ref[h, span, :])
            dq_ref[h, span, :] = dq
            dk_ref[h, span, :] = dot_tn(gscore, q)
            start = dot_tn(inverse, dot_tn(score_ref[h, span, :], glow))
            kf = k.astype(F32)
            reach = dot_tn(inverse, tail * kf).astype(BF16)
            feed = dot_tn(q, held)
            pieces[n, h] = (start, reach, feed)
    gonorm_ref[...] += onorm
    for h in range(PAIR):
        lanes = slice(h * HEAD_DIM, (h + 1) * HEAD_DIM)
        flow = None
        for n in reversed(range(chunks)):
            span = slice(n * CHUNK, (n + 1) * CHUNK)
            same, carry, tail, carry_last = state_masks(seg_ref, segcol, n)
            rate = jax.nn.sigmoid(column(logit_row(logit_ref, PAIR * pair + h, span)))
            start, reach, feed = pieces[n, h]
            k = k_ref[h, span, :]
            delta = delta_ref[span, lanes]
            gtarget = start
            if flow is not None:
                low = flow.astype(BF16)
                gtarget = gtarget + dot_nn(reach, low)
            gval = rate * gtarget
            head_ref[h, span, :] = gval
            grecall = (carry * gval).astype(BF16)
            dk = dk_ref[h, span, :]
            if flow is not None:
                dk = dk + tail * dot_nt(delta, low)
            if n > 0:
                dk = dk - dot_nt(grecall, state_ref[h, span, :])
                nxt = feed - dot_tn(k, grecall)
                if flow is not None:
                    nxt = nxt + carry_last * flow
                flow = nxt
            ggram = jnp.where(same & lower, dot_nt(gval, delta), 0.0)
            dk_ref[h, span, :] = dk - dot_nn(ggram + ggram.T, k)
            grate = jnp.sum(err_ref[span, lanes].astype(F32) * gtarget, axis=-1, keepdims=True)
            glogit = jnp.broadcast_to(grate, (CHUNK, CHUNK)) * rate * (1.0 - rate)
            glogit_ref[h, :, span] = glogit.T[0:1, :].astype(BF16)
    for h in range(PAIR):
        lanes = slice(h * HEAD_DIM, (h + 1) * HEAD_DIM)
        for c in range(3):
            gin_ref[h, c, length:, :] = jnp.zeros((HALO, HEAD_DIM), F32)
        taps = [[jnp.zeros((1, HEAD_DIM), F32)] * TAPS for _ in range(3)]
        for n in range(chunks):
            masks = back_masks(segcol, n)
            span = slice(n * CHUNK, (n + 1) * CHUNK)
            for c in range(3):
                conv = act_ref[h, c, span, :]
                gate = jax.nn.sigmoid(conv)
                act = conv * gate
                if c == 2:
                    gact = head_ref[h, span, :]
                else:
                    gunit = (dq_ref if c == 0 else dk_ref)[h, span, :]
                    inv = lax.rsqrt(jnp.sum(act * act, axis=-1, keepdims=True) + EPS)
                    unit = act * inv
                    gact = inv * (gunit - unit * jnp.sum(gunit * unit, axis=-1, keepdims=True))
                gin = gact * (gate + act * (1.0 - gate))
                gin_ref[h, c, span, :] = gin
                window = taps_in(proj_ref, c, h, n)
                taps[c][TAPS - 1] = taps[c][TAPS - 1] + jnp.sum(gin * window[HALO:], axis=0, keepdims=True)
                for s in range(1, TAPS):
                    part = jnp.sum(gin * masks[s] * window[HALO - s : HALO - s + CHUNK], axis=0, keepdims=True)
                    taps[c][TAPS - 1 - s] = taps[c][TAPS - 1 - s] + part
        for c in range(3):
            gconv_ref[c, :, lanes] += jnp.concatenate(taps[c], axis=0)
        for n in range(chunks):
            span = slice(n * CHUNK, (n + 1) * CHUNK)
            here = seg_rows(segcol, n, 0)
            ahead = [None] + [(seg_rows(segcol, n, s) == here).astype(F32) for s in range(1, TAPS)]
            for c in range(3):
                total = weight_ref[c, TAPS - 1 : TAPS, lanes] * gin_ref[h, c, span, :]
                for s in range(1, TAPS):
                    later = gin_ref[h, c, n * CHUNK + s : (n + 1) * CHUNK + s, :]
                    total = total + weight_ref[c, TAPS - 1 - s : TAPS - s, lanes] * (ahead[s] * later)
                gproj_ref[c, span, lanes] = total.astype(BF16)


def mixer_shapes(proj, seg):
    seqs, length = seg.shape
    return seqs, length, proj.shape[2] // HEAD_DIM


def mixer_forward(proj, seg, weight, logits, gain):
    seqs, length, heads = mixer_shapes(proj, seg)
    tokens = seqs * length
    wide = PAIR * HEAD_DIM
    flat = pl.BlockSpec((length, wide), lambda s, p: (s, p))
    square = pl.BlockSpec((PAIR, length, CHUNK), lambda s, p: (p, s, 0))
    return pl.pallas_call(
        forward_kernel,
        grid=(seqs, heads // PAIR),
        in_specs=[
            pl.BlockSpec((3, length, wide), lambda s, p: (0, s, p)),
            pl.BlockSpec((1, 1, length), lambda s, p: (s, 0, 0)),
            pl.BlockSpec((3, TAPS, wide), lambda s, p: (0, 0, p)),
            pl.BlockSpec((logits.shape[0], length), lambda s, p: (0, s)),
            pl.BlockSpec((1, HEAD_DIM), lambda s, p: (0, 0)),
        ],
        out_specs=[flat, flat, square, square, square, flat, flat],
        out_shape=[
            jax.ShapeDtypeStruct((tokens, heads * HEAD_DIM), BF16),
            jax.ShapeDtypeStruct((tokens, heads * HEAD_DIM), F32),
            jax.ShapeDtypeStruct((heads, tokens, CHUNK), BF16),
            jax.ShapeDtypeStruct((heads, tokens, CHUNK), BF16),
            jax.ShapeDtypeStruct((heads, tokens, CHUNK), BF16),
            jax.ShapeDtypeStruct((tokens, heads * HEAD_DIM), BF16),
            jax.ShapeDtypeStruct((tokens, heads * HEAD_DIM), BF16),
        ],
        scratch_shapes=[pltpu.VMEM((length + 2 * HALO, CHUNK), F32)],
        compiler_params=pltpu.CompilerParams(vmem_limit_bytes=48 << 20),
        name="mixer_forward",
    )(proj, seg.reshape(seqs, 1, length), weight, logits, gain.reshape(1, HEAD_DIM))


def mixer_backward(proj, seg, weight, logits, gain, kept, grad_nout):
    seqs, length, heads = mixer_shapes(proj, seg)
    tokens = seqs * length
    wide = PAIR * HEAD_DIM
    mixed, inverse, scores, states, delta, err = kept
    flat = pl.BlockSpec((length, wide), lambda p, s: (s, p))
    square = pl.BlockSpec((PAIR, length, CHUNK), lambda p, s: (p, s, 0))
    cube = pl.BlockSpec((3, length, wide), lambda p, s: (0, s, p))
    taps = pl.BlockSpec((3, TAPS, wide), lambda p, s: (0, 0, p))
    line = pl.BlockSpec((PAIR, 1, length), lambda p, s: (p, 0, s))
    vector = pl.BlockSpec((1, HEAD_DIM), lambda p, s: (0, 0))
    return pl.pallas_call(
        backward_kernel,
        grid=(heads // PAIR, seqs),
        in_specs=[cube, pl.BlockSpec((1, 1, length), lambda p, s: (s, 0, 0)), taps, pl.BlockSpec((logits.shape[0], length), lambda p, s: (0, s)), vector, flat, square, square, square, flat, flat, flat],
        out_specs=[cube, line, taps, vector],
        out_shape=[
            jax.ShapeDtypeStruct(proj.shape, BF16),
            jax.ShapeDtypeStruct((heads, 1, tokens), BF16),
            jax.ShapeDtypeStruct(weight.shape, F32),
            jax.ShapeDtypeStruct((1, HEAD_DIM), F32),
        ],
        scratch_shapes=[
            pltpu.VMEM((length + 2 * HALO, CHUNK), F32),
            pltpu.VMEM((PAIR, 3, length + HALO, HEAD_DIM), F32),
            pltpu.VMEM((PAIR, 3, length, HEAD_DIM), F32),
            pltpu.VMEM((PAIR, length, HEAD_DIM), BF16),
            pltpu.VMEM((PAIR, length, HEAD_DIM), BF16),
            pltpu.VMEM((PAIR, length, HEAD_DIM), F32),
            pltpu.VMEM((PAIR, length, HEAD_DIM), F32),
            pltpu.VMEM((PAIR, length, HEAD_DIM), F32),
        ],
        compiler_params=pltpu.CompilerParams(vmem_limit_bytes=48 << 20),
        name="mixer_backward",
    )(proj, seg.reshape(seqs, 1, length), weight, logits, gain.reshape(1, HEAD_DIM), mixed, inverse, scores, states, delta, err, grad_nout)


MESH = pl.DeviceIdType.MESH
ROWS_PER = 128


def partners():
    me = lax.axis_index("tensor")
    near = me + 1 - 2 * lax.rem(me, 2)
    far = lax.rem(me + 2, 4)
    return me, near, far


def greet(near, far):
    barrier = pltpu.get_barrier_semaphore()
    for other in (near, far):
        pl.semaphore_signal(barrier, inc=1, device_id={"tensor": other}, device_id_type=MESH)
    pl.semaphore_wait(barrier, 2)


def push(src, dst, send, recv, other):
    return pltpu.make_async_remote_copy(src_ref=src, dst_ref=dst, send_sem=send, recv_sem=recv, device_id={"tensor": other}, device_id_type=MESH)


def band(m):
    return pl.ds(pl.multiple_of(m * ROWS_PER, ROWS_PER), ROWS_PER)


def part_of(q, width):
    return pl.ds(pl.multiple_of(q * width, width), width)


def loop(start, stop, body):
    lax.fori_loop(start, stop, lambda m, carry: (body(m), carry)[1], 0)


def project_kernel(x_ref, gain_ref, rate_ref, weight_ref, full_out, normed_out, proj_out, logit_ref,
                   full, weight, normed, proj, weight_sem, far_send, far_recv, near_send, near_recv, pass_send, pass_recv, full_sem, normed_sem, proj_sem):
    me, near, far = partners()
    width = x_ref.shape[1]
    chunks = x_ref.shape[0] // ROWS_PER
    mine, theirs = part_of(me, width), part_of(far, width)
    load = pltpu.make_async_copy(weight_ref, weight, weight_sem)
    load.start()
    greet(near, far)

    def to_far(m):
        return push(x_ref.at[band(m)], full.at[band(m), mine], far_send.at[m], far_recv.at[m], far)

    def to_near(m):
        return push(x_ref.at[band(m)], full.at[band(m), mine], near_send.at[m], near_recv.at[m], near)

    def onward(m):
        return push(full.at[band(m), theirs], full.at[band(m), theirs], pass_send.at[m], pass_recv.at[m], near)

    def out_full(m):
        return pltpu.make_async_copy(full.at[band(m)], full_out.at[band(m)], full_sem.at[m])

    def out_normed(m):
        return pltpu.make_async_copy(normed.at[band(m)], normed_out.at[band(m)], normed_sem.at[m])

    def out_proj(m):
        return pltpu.make_async_copy(proj.at[:, band(m)], proj_out.at[:, band(m)], proj_sem.at[m])

    def begin(m):
        to_far(m).start()
        to_near(m).start()
        full[band(m), mine] = x_ref[band(m), :]

    def compute(m):
        to_near(m).wait_recv()
        onward(m).wait_recv()
        values = full[band(m), :].astype(F32)
        low = (values * lax.rsqrt(jnp.mean(values * values, axis=-1, keepdims=True) + EPS) * gain_ref[...]).astype(BF16)
        normed[band(m), :] = low
        for c in range(3):
            proj[c, band(m), :] = jnp.dot(low, weight[c], preferred_element_type=F32)
        logit_ref[:, band(m)] = lax.dot_general(rate_ref[...], low, (((1,), (1,)), ((), ())), preferred_element_type=F32)
        out_full(m).start()
        out_normed(m).start()
        out_proj(m).start()

    def relay(m):
        to_far(m).wait_recv()
        onward(m).start()

    def both(m):
        relay(m)
        compute(m - 1)

    def finish(m):
        to_far(m).wait_send()
        to_near(m).wait_send()
        onward(m).wait_send()
        out_full(m).wait()
        out_normed(m).wait()
        out_proj(m).wait()

    loop(0, chunks, begin)
    relay(0)
    load.wait()
    loop(1, chunks, both)
    compute(chunks - 1)
    loop(0, chunks, finish)


def in_vmem():
    return pl.BlockSpec(memory_space=pltpu.VMEM)


def in_hbm():
    return pl.BlockSpec(memory_space=pl.ANY)


def project(hidden_in, gain, rate, weight):
    tokens, _ = hidden_in.shape
    wide = weight.shape[1]
    chunks = tokens // ROWS_PER
    sems = pltpu.SemaphoreType.DMA((chunks,))
    return pl.pallas_call(
        project_kernel,
        in_specs=[in_vmem(), in_vmem(), in_vmem(), in_hbm()],
        out_specs=[in_hbm(), in_hbm(), in_hbm(), in_vmem()],
        out_shape=[
            jax.ShapeDtypeStruct((tokens, wide), BF16),
            jax.ShapeDtypeStruct((tokens, wide), BF16),
            jax.ShapeDtypeStruct((3, tokens, weight.shape[2]), F32),
            jax.ShapeDtypeStruct((rate.shape[0], tokens), F32),
        ],
        scratch_shapes=[
            pltpu.VMEM((tokens, wide), BF16),
            pltpu.VMEM(weight.shape, BF16),
            pltpu.VMEM((tokens, wide), BF16),
            pltpu.VMEM((3, tokens, weight.shape[2]), F32),
            pltpu.SemaphoreType.DMA,
        ] + [sems] * 9,
        compiler_params=pltpu.CompilerParams(collective_id=0, has_side_effects=True, vmem_limit_bytes=56 << 20),
        name="project",
    )(hidden_in, gain.reshape(1, wide), rate, weight)


def middle_kernel(low_ref, wout_ref, gain_ref, own_ref, other_ref, x_ref, wdown_ref, wgu_ref,
                  middle_out, mid_out, normed_out, hidden_out, gate_out, up_out, cot_out,
                  x_full, cot, wdown, wgu, keep, first, got_first, second, got_second, mid, middle, ghid, normed, acts,
                  load_sem, cot_send, cot_recv, a_send, a_recv, b_send, b_recv, c_send, c_recv, middle_sem, mid_sem, normed_sem, act_sem, cot_sem):
    me, near, far = partners()
    width = own_ref.shape[1]
    chunks = low_ref.shape[0] // ROWS_PER
    side, spot = lax.rem(me, 2), lax.div(me, 2)
    mine, theirs = part_of(me, width), part_of(far, width)
    loads = [
        pltpu.make_async_copy(own_ref, cot.at[:, mine], load_sem.at[0]),
        pltpu.make_async_copy(other_ref, cot.at[:, theirs], load_sem.at[1]),
        pltpu.make_async_copy(wdown_ref, wdown, load_sem.at[2]),
        pltpu.make_async_copy(x_ref, x_full, load_sem.at[3]),
        pltpu.make_async_copy(wgu_ref, wgu, load_sem.at[4]),
    ]
    for load in loads:
        load.start()
    greet(near, far)

    def send_first(m):
        return push(first.at[band(m)], got_first.at[band(m)], a_send.at[m], a_recv.at[m], near)

    def send_second(m):
        return push(second.at[band(m)], got_second.at[band(m)], b_send.at[m], b_recv.at[m], far)

    def share(m, which):
        at = (mine, theirs)[which]
        return push(mid.at[band(m), at], mid.at[band(m), at], c_send.at[m, which], c_recv.at[m, which], near)

    def out_middle(m):
        return pltpu.make_async_copy(middle.at[band(m)], middle_out.at[band(m)], middle_sem.at[m])

    def out_mid(m):
        return pltpu.make_async_copy(mid.at[band(m)], mid_out.at[band(m)], mid_sem.at[m])

    def out_normed(m):
        slot = lax.rem(m, 2)
        return pltpu.make_async_copy(normed.at[slot], normed_out.at[band(m)], normed_sem.at[slot])

    def out_act(m, which):
        slot = lax.rem(m, 2)
        return pltpu.make_async_copy(acts.at[slot, which], (hidden_out, gate_out, up_out)[which].at[band(m)], act_sem.at[slot, which])

    def project_out(m):
        rows = low_ref[band(m), :]
        for j in range(2):
            slot = slice(j * width, (j + 1) * width)
            first[band(m), slot] = jnp.dot(rows, wout_ref[:, part_of(2 * j + 1 - side, width)], preferred_element_type=F32).astype(BF16)
        send_first(m).start()
        for j in range(2):
            slot = slice(j * width, (j + 1) * width)
            keep[band(m), slot] = jnp.dot(rows, wout_ref[:, part_of(2 * j + side, width)], preferred_element_type=F32)

    def pair_sum(m):
        send_first(m).wait_recv()
        second[band(m), :] = (keep[band(m), :] + got_first[band(m), :].astype(F32)).astype(BF16)
        send_second(m).start()

    def feed(m):
        project_out(m)
        pair_sum(m - 1)

    def grad_hidden(m):
        ghid[band(m), :] = lax.dot_general(cot[band(m), :], wdown[...], (((1,), (1,)), ((), ())), preferred_element_type=F32)

    def total(m):
        send_second(m).wait_recv()
        for which, at, slot in ((0, mine, spot), (1, theirs, 1 - spot)):
            piece = part_of(slot, width)
            value = x_full[band(m), at].astype(F32) + (second[band(m), piece].astype(F32) + got_second[band(m), piece].astype(F32))
            if which == 0:
                middle[band(m), :] = value
            mid[band(m), at] = value.astype(BF16)
            share(m, which).start()
        out_middle(m).start()

    def compute(m):
        share(m, 0).wait_recv()
        share(m, 1).wait_recv()
        out_mid(m).start()
        slot = lax.rem(m, 2)

        @pl.when(m >= 2)
        def _():
            out_normed(m - 2).wait()
            for which in range(3):
                out_act(m - 2, which).wait()

        values = mid[band(m), :].astype(F32)
        low = (values * lax.rsqrt(jnp.mean(values * values, axis=-1, keepdims=True) + EPS) * gain_ref[...]).astype(BF16)
        normed[slot] = low
        out_normed(m).start()
        gate_pre = jnp.dot(low, wgu[0], preferred_element_type=F32)
        up_pre = jnp.dot(low, wgu[1], preferred_element_type=F32)
        gate = jax.nn.sigmoid(gate_pre)
        silu = gate_pre * gate
        grad = ghid[band(m), :]
        acts[slot, 0] = (silu * up_pre).astype(BF16)
        acts[slot, 1] = (grad * up_pre * (gate + silu * (1.0 - gate))).astype(BF16)
        acts[slot, 2] = (grad * silu).astype(BF16)
        for which in range(3):
            out_act(m, which).start()

    def both(m):
        total(m)
        compute(m - 1)

    loads[0].wait()
    loads[1].wait()
    shares = [push(cot.at[:, at], cot.at[:, at], cot_send.at[i], cot_recv.at[i], near) for i, at in enumerate((mine, theirs))]
    project_out(0)
    loop(1, chunks, feed)
    pair_sum(chunks - 1)
    for copy in shares:
        copy.start()
    loads[2].wait()
    loads[3].wait()
    for copy in shares:
        copy.wait_recv()
    save = pltpu.make_async_copy(cot, cot_out, cot_sem)
    save.start()
    loop(0, chunks, grad_hidden)
    loads[4].wait()
    total(0)
    loop(1, chunks, both)
    compute(chunks - 1)

    def finish(m):
        send_first(m).wait_send()
        send_second(m).wait_send()
        share(m, 0).wait_send()
        share(m, 1).wait_send()
        out_middle(m).wait()
        out_mid(m).wait()

    for m in (chunks - 2, chunks - 1):
        out_normed(m).wait()
        for which in range(3):
            out_act(m, which).wait()
    for copy in shares:
        copy.wait_send()
    save.wait()
    loop(0, chunks, finish)


def middle_step(out_low, wout, gain, cot_own, cot_far, full_in, wdown, wgu):
    tokens, width = cot_own.shape
    wide, units = wgu.shape[1], wgu.shape[2]
    chunks = tokens // ROWS_PER
    dma = pltpu.SemaphoreType.DMA
    half = (tokens, wide // 2)
    return pl.pallas_call(
        middle_kernel,
        in_specs=[in_vmem(), in_vmem(), in_vmem()] + [in_hbm()] * 5,
        out_specs=[in_hbm()] * 7,
        out_shape=[
            jax.ShapeDtypeStruct((tokens, width), F32),
            jax.ShapeDtypeStruct((tokens, wide), BF16),
            jax.ShapeDtypeStruct((tokens, wide), BF16),
            jax.ShapeDtypeStruct((tokens, units), BF16),
            jax.ShapeDtypeStruct((tokens, units), BF16),
            jax.ShapeDtypeStruct((tokens, units), BF16),
            jax.ShapeDtypeStruct((tokens, wide), BF16),
        ],
        scratch_shapes=[
            pltpu.VMEM((tokens, wide), BF16),
            pltpu.VMEM((tokens, wide), BF16),
            pltpu.VMEM(wdown.shape, BF16),
            pltpu.VMEM(wgu.shape, BF16),
            pltpu.VMEM(half, F32),
            pltpu.VMEM(half, BF16),
            pltpu.VMEM(half, BF16),
            pltpu.VMEM(half, BF16),
            pltpu.VMEM(half, BF16),
            pltpu.VMEM((tokens, wide), BF16),
            pltpu.VMEM((tokens, width), F32),
            pltpu.VMEM((tokens, units), F32),
            pltpu.VMEM((2, ROWS_PER, wide), BF16),
            pltpu.VMEM((2, 3, ROWS_PER, units), BF16),
            dma((5,)), dma((2,)), dma((2,)),
            dma((chunks,)), dma((chunks,)), dma((chunks,)), dma((chunks,)),
            dma((chunks, 2)), dma((chunks, 2)),
            dma((chunks,)), dma((chunks,)), dma((2,)), dma((2, 3)), dma,
        ],
        compiler_params=pltpu.CompilerParams(collective_id=1, has_side_effects=True, vmem_limit_bytes=62 << 20),
        name="middle_step",
    )(out_low, wout, gain.reshape(1, wide), cot_own, cot_far, full_in, wdown, wgu)


def return_kernel(wout_ref, gain_ref, gate_ref, up_ref, mid_ref, cot_ref, wgu_ref,
                  gmid_out, full_out, nout_out, sum_ref,
                  gate, up, mid, cot, wgu, piece, keep, first, got_first, second, got_second, full, gmid, nout,
                  load_sem, a_send, a_recv, b_send, b_recv, c_send, c_recv, gmid_sem, full_sem, nout_sem):
    me, near, far = partners()
    width = gmid.shape[1]
    chunks = gmid.shape[0] // ROWS_PER
    side, spot = lax.rem(me, 2), lax.div(me, 2)
    mine, theirs = part_of(me, width), part_of(far, width)
    loads = [
        pltpu.make_async_copy(gate_ref, gate, load_sem.at[0]),
        pltpu.make_async_copy(wgu_ref.at[0], wgu.at[0], load_sem.at[1]),
        pltpu.make_async_copy(up_ref, up, load_sem.at[2]),
        pltpu.make_async_copy(wgu_ref.at[1], wgu.at[1], load_sem.at[3]),
        pltpu.make_async_copy(mid_ref, mid, load_sem.at[4]),
        pltpu.make_async_copy(cot_ref, cot, load_sem.at[5]),
    ]
    for load in loads:
        load.start()
    greet(near, far)
    sum_ref[...] = jnp.zeros_like(sum_ref)

    def send_first(m):
        return push(first.at[band(m)], got_first.at[band(m)], a_send.at[m], a_recv.at[m], near)

    def send_second(m):
        return push(second.at[band(m)], got_second.at[band(m)], b_send.at[m], b_recv.at[m], far)

    def share(m, which):
        at = (mine, theirs)[which]
        return push(full.at[band(m), at], full.at[band(m), at], c_send.at[m, which], c_recv.at[m, which], near)

    def outs(m):
        return [
            pltpu.make_async_copy(gmid.at[band(m)], gmid_out.at[band(m)], gmid_sem.at[m]),
            pltpu.make_async_copy(full.at[band(m)], full_out.at[band(m)], full_sem.at[m]),
            pltpu.make_async_copy(nout.at[band(m)], nout_out.at[band(m)], nout_sem.at[m]),
        ]

    def partial(m):
        dims = (((1,), (1,)), ((), ()))
        grad = lax.dot_general(gate[band(m), :], wgu[0], dims, preferred_element_type=F32)
        grad = grad + lax.dot_general(up[band(m), :], wgu[1], dims, preferred_element_type=F32)
        values = mid[band(m), :].astype(F32)
        scale = lax.rsqrt(jnp.mean(values * values, axis=-1, keepdims=True) + EPS)
        unit = values * scale
        sum_ref[...] += jnp.sum(grad * unit, axis=0, keepdims=True)
        scaled = grad * gain_ref[...]
        piece[...] = scale * (scaled - unit * jnp.mean(scaled * unit, axis=-1, keepdims=True))
        for j in range(2):
            slot = slice(j * width, (j + 1) * width)
            first[band(m), slot] = piece[:, part_of(2 * j + 1 - side, width)].astype(BF16)
            keep[band(m), slot] = piece[:, part_of(2 * j + side, width)]
        send_first(m).start()

    def pair_sum(m):
        send_first(m).wait_recv()
        second[band(m), :] = (keep[band(m), :] + got_first[band(m), :].astype(F32)).astype(BF16)
        send_second(m).start()

    def feed(m):
        partial(m)
        pair_sum(m - 1)

    def total(m):
        send_second(m).wait_recv()
        for which, at, slot in ((0, mine, spot), (1, theirs, 1 - spot)):
            part = part_of(slot, width)
            value = cot[band(m), at].astype(F32) + (second[band(m), part].astype(F32) + got_second[band(m), part].astype(F32))
            if which == 0:
                gmid[band(m), :] = value
            full[band(m), at] = value.astype(BF16)
            share(m, which).start()
        outs(m)[0].start()

    def compute(m):
        share(m, 0).wait_recv()
        share(m, 1).wait_recv()
        outs(m)[1].start()
        nout[band(m), :] = lax.dot_general(full[band(m), :], wout_ref[...], (((1,), (1,)), ((), ())), preferred_element_type=F32)
        outs(m)[2].start()

    def both(m):
        total(m)
        compute(m - 1)

    def finish(m):
        send_first(m).wait_send()
        send_second(m).wait_send()
        share(m, 0).wait_send()
        share(m, 1).wait_send()
        for copy in outs(m):
            copy.wait()

    for load in loads[:5]:
        load.wait()
    partial(0)
    loop(1, chunks, feed)
    pair_sum(chunks - 1)
    loads[5].wait()
    total(0)
    loop(1, chunks, both)
    compute(chunks - 1)
    loop(0, chunks, finish)


def return_step(wout, gain, grad_gate, grad_up, full_mid, full_cot, wgu):
    tokens, wide = full_mid.shape
    units = wgu.shape[2]
    width = wide // 4
    chunks = tokens // ROWS_PER
    dma = pltpu.SemaphoreType.DMA
    half = (tokens, wide // 2)
    return pl.pallas_call(
        return_kernel,
        in_specs=[in_vmem(), in_vmem()] + [in_hbm()] * 5,
        out_specs=[in_hbm()] * 3 + [in_vmem()],
        out_shape=[
            jax.ShapeDtypeStruct((tokens, width), F32),
            jax.ShapeDtypeStruct((tokens, wide), BF16),
            jax.ShapeDtypeStruct((tokens, wout.shape[0]), F32),
            jax.ShapeDtypeStruct((1, wide), F32),
        ],
        scratch_shapes=[
            pltpu.VMEM((tokens, units), BF16),
            pltpu.VMEM((tokens, units), BF16),
            pltpu.VMEM((tokens, wide), BF16),
            pltpu.VMEM((tokens, wide), BF16),
            pltpu.VMEM(wgu.shape, BF16),
            pltpu.VMEM((ROWS_PER, wide), F32),
            pltpu.VMEM(half, F32),
            pltpu.VMEM(half, BF16),
            pltpu.VMEM(half, BF16),
            pltpu.VMEM(half, BF16),
            pltpu.VMEM(half, BF16),
            pltpu.VMEM((tokens, wide), BF16),
            pltpu.VMEM((tokens, width), F32),
            pltpu.VMEM((tokens, wout.shape[0]), F32),
            dma((6,)),
            dma((chunks,)), dma((chunks,)), dma((chunks,)), dma((chunks,)),
            dma((chunks, 2)), dma((chunks, 2)),
            dma((chunks,)), dma((chunks,)), dma((chunks,)),
        ],
        compiler_params=pltpu.CompilerParams(collective_id=2, has_side_effects=True, vmem_limit_bytes=62 << 20),
        name="return_step",
    )(wout, gain.reshape(1, wide), grad_gate, grad_up, full_mid, full_cot, wgu)


PLAIN = (((1,), (0,)), ((), ()))
ROWS = (((0,), (0,)), ((), ()))


def rms_scale(values):
    return lax.rsqrt(jnp.mean(values * values, axis=-1, keepdims=True) + EPS)


def norm_back(grad_normed, unit_rows, scale_rows, gain):
    scaled_grad = grad_normed * gain
    grad_rows = scale_rows * (scaled_grad - unit_rows * jnp.mean(scaled_grad * unit_rows, axis=-1, keepdims=True))
    return grad_rows, jnp.sum(grad_normed * unit_rows, axis=0)


def butterfly(values, axis, size):
    step = 1
    while step < size:
        pairs = [(i, i ^ step) for i in range(size)]
        values = values + lax.ppermute(values, axis, pairs)
        step *= 2
    return values


def row_major(values):
    return with_layout_constraint(values, Layout(tuple(range(values.ndim))))


def tie(value, token):
    return value if token is None else lax.optimization_barrier((value, token))[0]


class Timeline:
    def __init__(self, size):
        self.size = size
        self.bits = size.bit_length() - 1
        self.token = None
        self.open = {}

    def after(self, value):
        return tie(value, self.token)

    def swap(self, values, bit):
        return lax.ppermute(values, "dp", [(i, i ^ (1 << bit)) for i in range(self.size)])

    def scatter(self, name, grad, order=()):
        order = list(order) + [bit for bit in range(self.bits) if bit not in order]
        blocks = row_major(grad.astype(BF16)).reshape((2,) * self.bits + (grad.shape[0] // self.size, grad.shape[1]))
        self.open[name] = ([blocks], list(range(self.bits))[::-1], order, 0)
        self.move(name)

    def move(self, name):
        terms, axes, order, stage = self.open[name]
        bit = order[stage]
        own = lax.rem(lax.div(lax.axis_index("dp"), 1 << bit), 2)
        axis = axes.index(bit)
        if stage:
            terms = terms[:-1] + [self.after(terms[-1])]

        def pick(value, at):
            return lax.dynamic_index_in_dim(value, at, axis, keepdims=False)

        away = pick(terms[0], 1 - own) if stage == 0 else sum(pick(t, 1 - own).astype(F32) for t in terms).astype(BF16)
        away = row_major(away)
        self.token = away
        came = self.swap(away, bit)
        self.open[name] = ([pick(t, own) for t in terms] + [came], axes[:axis] + axes[axis + 1 :], order, stage + 1)

    def close(self, name):
        while self.open[name][3] < self.bits:
            self.move(name)
        terms = self.open.pop(name)[0]
        terms = terms[:-1] + [self.after(terms[-1])]
        return row_major(sum(t.astype(F32) for t in terms))


def make_body(dp_size, tensor_size):
    def body(hidden_in, seg_ids, attn_gain, wqkv, conv_weight, wrate, onorm_gain, wout, mlp_gain, wgu, wdown, cotangent):
        return step(hidden_in, seg_ids, attn_gain, wqkv, conv_weight, wrate, onorm_gain, wout, mlp_gain, wgu, wdown, cotangent)

    def step(hidden_in, seg_ids, attn_gain, wqkv, conv_weight, wrate, onorm_gain, wout, mlp_gain, wgu, wdown, cotangent):
        tokens, width = hidden_in.shape
        heads = wrate.shape[1]
        me = lax.axis_index("tensor")
        side, spot = lax.rem(me, 2), lax.div(me, 2)

        def dot(a, b, dims):
            return lax.dot_general(a, b, dims, preferred_element_type=F32)

        def swap(values, step):
            return lax.ppermute(values, "tensor", [(i, i ^ step) for i in range(tensor_size)])

        def columns(values, q):
            return lax.dynamic_slice_in_dim(values, q * width, width, 1)

        def quarter_sum(pick):
            away = jnp.concatenate([pick(2 * j + 1 - side).astype(BF16) for j in range(2)], axis=1)
            came = swap(away, 1)
            other = (pick(lax.rem(me + 2, 4)) + columns(came, 1 - spot).astype(F32)).astype(BF16)
            far = swap(other, 2)
            return pick(me) + columns(came, spot).astype(F32), far

        taps = conv_weight.astype(F32)
        rates = jnp.zeros((8, wrate.shape[0]), BF16).at[:heads].set(wrate.T)
        full_low, normed_one, proj, logits = project(hidden_in, attn_gain, rates, wqkv)
        cot_own, _ = lax.optimization_barrier((cotangent, logits))
        cot_far = swap(cot_own, 2)
        out_low, *kept = mixer_forward(proj, seg_ids, taps, logits, onorm_gain)
        middle, mid_low, normed_two, hidden, grad_gate, grad_up, full_cot = middle_step(out_low, wout, mlp_gain, cotangent, cot_far, full_low, wdown, wgu)
        line = Timeline(dp_size)
        line.scatter("down", dot(full_cot, hidden, ROWS))
        line.scatter("gate", dot(normed_two, line.after(grad_gate), ROWS), (1,))
        line.scatter("up", dot(normed_two, line.after(grad_up), ROWS))
        late_gate = line.after(grad_gate)
        grad_middle, full_grad_mid, grad_nout, gain_two = return_step(wout, mlp_gain, late_gate, grad_up, mid_low, full_cot, wgu)
        line.scatter("out", dot(full_grad_mid, out_low, ROWS))
        line.move("gate")
        line.move("down")
        grad_proj, grad_logits, grad_conv, gain_onorm = mixer_backward(proj, seg_ids, taps, logits, onorm_gain, kept, line.after(grad_nout))
        line.token = grad_logits
        grad_logits = grad_logits.reshape(heads, tokens)
        line.move("up")
        line.move("down")
        late_low, late_proj = line.after((full_low, grad_proj))
        grad_nin = jnp.einsum("ctk,cdk->td", late_proj, wqkv, preferred_element_type=F32)
        grad_nin = grad_nin + jnp.einsum("ht,dh->td", grad_logits, wrate, preferred_element_type=F32)
        full_in = late_low.astype(F32)
        scale_one = rms_scale(full_in)
        part_one, gain_one = norm_back(grad_nin, full_in * scale_one, scale_one, attn_gain)
        part_one = part_one.astype(BF16)
        line.token = (part_one, gain_one)
        wide = gain_one.shape[0]
        grad_beta = jnp.einsum("td,ht->dh", normed_one, line.after(grad_logits), preferred_element_type=F32)
        gains = butterfly(jnp.concatenate([gain_one, gain_two.reshape(-1), gain_onorm.reshape(-1)]), "tensor", tensor_size)
        shared = gains.shape[0]
        line.move("gate")
        line.scatter("k", dot(normed_one, line.after(grad_proj[1]), ROWS), (1,))
        small = jnp.concatenate([gains, grad_conv.reshape(-1), grad_beta.reshape(-1)])
        small_came = line.swap(small, 0)
        line.scatter("v", dot(normed_one, line.after(grad_proj[2]), ROWS))
        line.scatter("q", dot(normed_one, line.after(grad_proj[0]), ROWS))
        one, one_far = quarter_sum(lambda q: columns(part_one, q).astype(F32))
        line.move("up")
        late_hidden = line.after(hidden)
        ffn, ffn_far = quarter_sum(lambda q: dot(late_hidden, columns(wdown, q), PLAIN))
        line.move("out")
        grad_down = line.close("down").T
        small = small + line.after(small_came)
        small_came = line.swap(small, 1 % line.bits)
        line.move("k")
        line.move("out")
        grad_gate_w = line.close("gate")
        line.move("v")
        grad_up_w = line.close("up")
        small = small + line.after(small_came)
        small_came = line.swap(small, 2 % line.bits)
        grad_in = (grad_middle + one + line.after(one_far).astype(F32)).astype(BF16)
        layer_out = (middle + ffn + line.after(ffn_far).astype(F32)).astype(BF16)
        line.move("q")
        line.move("v")
        line.move("k")
        line.move("q")
        small = small + line.after(small_came)
        for bit in range(3, line.bits):
            small = small + line.swap(small, bit)
        grad_out = line.close("out").T
        grad_qkv = [line.close(n) for n in "qkv"]
        gains = small[:shared]
        grad_conv = small[shared : shared + grad_conv.size].reshape(grad_conv.shape)
        mine = grad_beta.shape[0] // dp_size
        grad_beta = small[shared + grad_conv.size :].reshape(grad_beta.shape)
        grad_beta = lax.dynamic_slice_in_dim(grad_beta, lax.axis_index("dp") * mine, mine, 0)
        return (
            layer_out,
            grad_in,
            gains[:wide],
            jnp.stack(grad_qkv),
            grad_conv,
            grad_beta,
            gains[2 * wide :],
            grad_out,
            gains[wide : 2 * wide],
            jnp.stack([grad_gate_w, grad_up_w]),
            grad_down,
        )

    return body


def solution(mesh):
    return jax.shard_map(
        make_body(mesh.shape["dp"], mesh.shape["tensor"]),
        mesh=mesh,
        in_specs=(
            P("dp", "tensor"),
            P("dp", None),
            P(),
            P(None, None, "tensor"),
            P(None, None, "tensor"),
            P(None, "tensor"),
            P(),
            P("tensor", None),
            P(),
            P(None, None, "tensor"),
            P("tensor", None),
            P("dp", "tensor"),
        ),
        out_specs=(
            P("dp", "tensor"),
            P("dp", "tensor"),
            P(),
            P(None, "dp", "tensor"),
            P(None, None, "tensor"),
            P("dp", "tensor"),
            P(),
            P("tensor", "dp"),
            P(),
            P(None, "dp", "tensor"),
            P("tensor", "dp"),
        ),
        check_vma=False,
    )
```

```python
import jax
import jax.numpy as jnp
from jax import lax
from jax.experimental import pallas as pl
from jax.experimental.pallas import tpu as pltpu
from jax.experimental.layout import Layout, with_layout_constraint
from jax.sharding import PartitionSpec as P

HEAD_DIM = 128
TAPS = 4
CHUNK = 128
HALO = 8
EPS = 1e-06
PAIR = 2
F32 = jnp.float32
BF16 = jnp.bfloat16


def dot_nn(a, b):
    return jnp.dot(a.astype(BF16), b.astype(BF16), preferred_element_type=F32)


def dot_nt(a, b):
    return lax.dot_general(a.astype(BF16), b.astype(BF16), (((1,), (1,)), ((), ())), preferred_element_type=F32)


def dot_tn(a, b):
    return lax.dot_general(a.astype(BF16), b.astype(BF16), (((0,), (0,)), ((), ())), preferred_element_type=F32)


def column(row):
    return jnp.broadcast_to(row, (CHUNK, CHUNK)).T


def logit_row(logit_ref, head, span):
    values = logit_ref[:, span]
    return jnp.sum(jnp.where(lax.broadcasted_iota(jnp.int32, values.shape, 0) == head, values, 0.0), axis=0, keepdims=True)


def load_segments(seg_ref, segcol, length):
    segcol[0:HALO, :] = jnp.full((HALO, CHUNK), -1.0, F32)
    segcol[HALO + length :, :] = jnp.full((HALO, CHUNK), -2.0, F32)
    for n in range(length // CHUNK):
        row = seg_ref[0, :, n * CHUNK : (n + 1) * CHUNK].astype(F32)
        segcol[HALO + n * CHUNK : HALO + (n + 1) * CHUNK, :] = column(row)


def seg_rows(segcol, n, shift):
    base = HALO + n * CHUNK + shift
    return segcol[base : base + CHUNK, :]


def back_masks(segcol, n):
    here = seg_rows(segcol, n, 0)
    return [None] + [(seg_rows(segcol, n, -s) == here).astype(F32) for s in range(1, TAPS)]


def state_masks(seg_ref, segcol, n):
    here = seg_rows(segcol, n, 0)
    row = jnp.broadcast_to(seg_ref[0, :, n * CHUNK : (n + 1) * CHUNK].astype(F32), (CHUNK, CHUNK))
    same = here == row
    before = segcol[HALO + n * CHUNK - 1 : HALO + n * CHUNK, :]
    last = segcol[HALO + (n + 1) * CHUNK - 1 : HALO + (n + 1) * CHUNK, :]
    carry = (here == before).astype(F32)
    tail = (here == last).astype(F32)
    carry_last = (last == before).astype(F32)
    return same, carry, tail, carry_last


def taps_in(proj_ref, c, h, n):
    lanes = slice(h * HEAD_DIM, (h + 1) * HEAD_DIM)
    if n == 0:
        return jnp.concatenate([jnp.zeros((HALO, HEAD_DIM), F32), proj_ref[c, 0:CHUNK, lanes].astype(F32)], axis=0)
    return proj_ref[c, n * CHUNK - HALO : (n + 1) * CHUNK, lanes].astype(F32)


def conv_rows(window, weight_ref, c, h, masks):
    lanes = slice(h * HEAD_DIM, (h + 1) * HEAD_DIM)
    total = weight_ref[c, TAPS - 1 : TAPS, lanes] * window[HALO:]
    for s in range(1, TAPS):
        total = total + weight_ref[c, TAPS - 1 - s : TAPS - s, lanes] * (masks[s] * window[HALO - s : HALO - s + CHUNK])
    return total


def grid_ids():
    rows = lax.broadcasted_iota(jnp.int32, (CHUNK, CHUNK), 0)
    cols = lax.broadcasted_iota(jnp.int32, (CHUNK, CHUNK), 1)
    return rows, cols


def forward_kernel(proj_ref, seg_ref, weight_ref, logit_ref, gain_ref, out_ref, mixed_ref, inv_ref, score_ref, state_ref, delta_ref, err_ref, segcol):
    length = proj_ref.shape[1]
    chunks = length // CHUNK
    load_segments(seg_ref, segcol, length)
    rows, cols = grid_ids()
    apart = rows ^ cols
    lower = rows > cols
    lower_incl = rows >= cols
    scale = HEAD_DIM**-0.5
    pieces, systems, inverses = {}, {}, {}
    for n in range(chunks):
        masks = back_masks(segcol, n)
        same, carry, tail, carry_last = state_masks(seg_ref, segcol, n)
        span = slice(n * CHUNK, (n + 1) * CHUNK)
        for h in range(PAIR):
            acts = []
            for c in range(3):
                conv = conv_rows(taps_in(proj_ref, c, h, n), weight_ref, c, h, masks)
                acts.append(conv * jax.nn.sigmoid(conv))
            q = (acts[0] * lax.rsqrt(jnp.sum(acts[0] * acts[0], axis=-1, keepdims=True) + EPS)).astype(BF16)
            k = (acts[1] * lax.rsqrt(jnp.sum(acts[1] * acts[1], axis=-1, keepdims=True) + EPS)).astype(BF16)
            v = acts[2].astype(BF16).astype(F32)
            rate = jax.nn.sigmoid(column(logit_row(logit_ref, PAIR * pl.program_id(1) + h, span)))
            gram = jnp.where(same & lower, dot_nt(k, k), 0.0)
            scores = (jnp.where(same & lower_incl, dot_nt(q, k), 0.0) * scale).astype(BF16)
            system = rate * gram
            score_ref[h, span, :] = scores
            systems[n, h] = system
            inverses[n, h] = jnp.where(rows == cols, 1.0, 0.0) - jnp.where(apart == 1, system, 0.0)
            pieces[n, h] = (q, k.astype(F32), v, gram, scores, rate, carry, tail, carry_last)
    level = 1
    while (2 << level) <= CHUNK:
        crossed = {}
        for key, inverse in inverses.items():
            crossed[key] = dot_nn(jnp.where((apart >> level) == 1, systems[key], 0.0), inverse)
        for key, inverse in inverses.items():
            inverses[key] = inverse - dot_nn(inverse, crossed[key])
        level += 1
    for n, h in pieces:
        q, kf, v, gram, scores, rate, carry, tail, carry_last = pieces[n, h]
        inverse = inverses[n, h].astype(BF16)
        inv_ref[h, n * CHUNK : (n + 1) * CHUNK, :] = inverse
        base = dot_nn(inverse, rate * v)
        back = dot_nn(inverse, rate * carry * kf)
        pieces[n, h] = (q, kf, v, gram, scores, base, back, carry, tail, carry_last)
    for h in range(PAIR):
        lanes = slice(h * HEAD_DIM, (h + 1) * HEAD_DIM)
        state = None
        for n in range(chunks):
            span = slice(n * CHUNK, (n + 1) * CHUNK)
            q, kf, v, gram, scores, base, back, carry, tail, carry_last = pieces[n, h]
            if n == 0:
                delta = base
                rest = v
                state_ref[h, span, :] = jnp.zeros((CHUNK, CHUNK), BF16)
            else:
                low = state.astype(BF16)
                state_ref[h, span, :] = low
                delta = base - dot_nn(back, low)
                rest = v - carry * dot_nn(kf, low)
            delta_low = delta.astype(BF16)
            moved = dot_tn(tail * kf, delta_low)
            mixed = dot_nn(scores, delta_low)
            if n > 0:
                mixed = mixed + (carry * scale) * dot_nn(q, low)
                moved = moved + carry_last * state
            state = moved
            delta_ref[span, lanes] = delta_low
            err_ref[span, lanes] = (rest - dot_nn(gram, delta_low)).astype(BF16)
            mixed_ref[span, lanes] = mixed
            root = lax.rsqrt(jnp.mean(mixed * mixed, axis=-1, keepdims=True) + EPS)
            out_ref[span, lanes] = (mixed * root * gain_ref[...]).astype(BF16)


def backward_kernel(proj_ref, seg_ref, weight_ref, logit_ref, gain_ref, mixed_ref, inv_ref, score_ref, state_ref, delta_ref, err_ref, nout_ref,
                    gproj_ref, glogit_ref, gconv_ref, gonorm_ref, segcol, gin_ref, act_ref, q_ref, k_ref, head_ref, dq_ref, dk_ref):
    length = proj_ref.shape[1]
    chunks = length // CHUNK
    pair, seq = pl.program_id(0), pl.program_id(1)
    load_segments(seg_ref, segcol, length)
    rows, cols = grid_ids()
    lower = rows > cols
    lower_incl = rows >= cols
    scale = HEAD_DIM**-0.5

    @pl.when((pair == 0) & (seq == 0))
    def _():
        gonorm_ref[...] = jnp.zeros_like(gonorm_ref)

    @pl.when(seq == 0)
    def _():
        gconv_ref[...] = jnp.zeros_like(gconv_ref)

    onorm = jnp.zeros((1, HEAD_DIM), F32)
    pieces = {}
    for n in range(chunks):
        masks = back_masks(segcol, n)
        same, carry, tail, carry_last = state_masks(seg_ref, segcol, n)
        span = slice(n * CHUNK, (n + 1) * CHUNK)
        for h in range(PAIR):
            lanes = slice(h * HEAD_DIM, (h + 1) * HEAD_DIM)
            for c in range(3):
                act_ref[h, c, span, :] = conv_rows(taps_in(proj_ref, c, h, n), weight_ref, c, h, masks)
            conv = act_ref[h, 0, span, :]
            act = conv * jax.nn.sigmoid(conv)
            q = (act * lax.rsqrt(jnp.sum(act * act, axis=-1, keepdims=True) + EPS)).astype(BF16)
            conv = act_ref[h, 1, span, :]
            act = conv * jax.nn.sigmoid(conv)
            k = (act * lax.rsqrt(jnp.sum(act * act, axis=-1, keepdims=True) + EPS)).astype(BF16)
            q_ref[h, span, :] = q
            k_ref[h, span, :] = k
            mixed = mixed_ref[span, lanes]
            root = lax.rsqrt(jnp.mean(mixed * mixed, axis=-1, keepdims=True) + EPS)
            unit = mixed * root
            grad = nout_ref[span, lanes].astype(F32)
            onorm = onorm + jnp.sum(grad * unit, axis=0, keepdims=True)
            scaled = grad * gain_ref[...]
            gmix = root * (scaled - unit * jnp.mean(scaled * unit, axis=-1, keepdims=True))
            glow = gmix.astype(BF16)
            inverse = inv_ref[h, span, :]
            delta = delta_ref[span, lanes]
            gscore = (jnp.where(same & lower_incl, dot_nt(glow, delta), 0.0) * scale).astype(BF16)
            dq = dot_nn(gscore, k)
            held = (scale * carry * gmix).astype(BF16)
            if n > 0:
                dq = dq + dot_nt(held, state_ref[h, span, :])
            dq_ref[h, span, :] = dq
            dk_ref[h, span, :] = dot_tn(gscore, q)
            start = dot_tn(inverse, dot_tn(score_ref[h, span, :], glow))
            kf = k.astype(F32)
            reach = dot_tn(inverse, tail * kf).astype(BF16)
            feed = dot_tn(q, held)
            pieces[n, h] = (start, reach, feed)
    gonorm_ref[...] += onorm
    for h in range(PAIR):
        lanes = slice(h * HEAD_DIM, (h + 1) * HEAD_DIM)
        flow = None
        for n in reversed(range(chunks)):
            span = slice(n * CHUNK, (n + 1) * CHUNK)
            same, carry, tail, carry_last = state_masks(seg_ref, segcol, n)
            rate = jax.nn.sigmoid(column(logit_row(logit_ref, PAIR * pair + h, span)))
            start, reach, feed = pieces[n, h]
            k = k_ref[h, span, :]
            delta = delta_ref[span, lanes]
            gtarget = start
            if flow is not None:
                low = flow.astype(BF16)
                gtarget = gtarget + dot_nn(reach, low)
            gval = rate * gtarget
            head_ref[h, span, :] = gval
            grecall = (carry * gval).astype(BF16)
            dk = dk_ref[h, span, :]
            if flow is not None:
                dk = dk + tail * dot_nt(delta, low)
            if n > 0:
                dk = dk - dot_nt(grecall, state_ref[h, span, :])
                nxt = feed - dot_tn(k, grecall)
                if flow is not None:
                    nxt = nxt + carry_last * flow
                flow = nxt
            ggram = jnp.where(same & lower, dot_nt(gval, delta), 0.0)
            dk_ref[h, span, :] = dk - dot_nn(ggram + ggram.T, k)
            grate = jnp.sum(err_ref[span, lanes].astype(F32) * gtarget, axis=-1, keepdims=True)
            glogit = jnp.broadcast_to(grate, (CHUNK, CHUNK)) * rate * (1.0 - rate)
            glogit_ref[h, :, span] = glogit.T[0:1, :].astype(BF16)
    for h in range(PAIR):
        lanes = slice(h * HEAD_DIM, (h + 1) * HEAD_DIM)
        for c in range(3):
            gin_ref[h, c, length:, :] = jnp.zeros((HALO, HEAD_DIM), F32)
        taps = [[jnp.zeros((1, HEAD_DIM), F32)] * TAPS for _ in range(3)]
        for n in range(chunks):
            masks = back_masks(segcol, n)
            span = slice(n * CHUNK, (n + 1) * CHUNK)
            for c in range(3):
                conv = act_ref[h, c, span, :]
                gate = jax.nn.sigmoid(conv)
                act = conv * gate
                if c == 2:
                    gact = head_ref[h, span, :]
                else:
                    gunit = (dq_ref if c == 0 else dk_ref)[h, span, :]
                    inv = lax.rsqrt(jnp.sum(act * act, axis=-1, keepdims=True) + EPS)
                    unit = act * inv
                    gact = inv * (gunit - unit * jnp.sum(gunit * unit, axis=-1, keepdims=True))
                gin = gact * (gate + act * (1.0 - gate))
                gin_ref[h, c, span, :] = gin
                window = taps_in(proj_ref, c, h, n)
                taps[c][TAPS - 1] = taps[c][TAPS - 1] + jnp.sum(gin * window[HALO:], axis=0, keepdims=True)
                for s in range(1, TAPS):
                    part = jnp.sum(gin * masks[s] * window[HALO - s : HALO - s + CHUNK], axis=0, keepdims=True)
                    taps[c][TAPS - 1 - s] = taps[c][TAPS - 1 - s] + part
        for c in range(3):
            gconv_ref[c, :, lanes] += jnp.concatenate(taps[c], axis=0)
        for n in range(chunks):
            span = slice(n * CHUNK, (n + 1) * CHUNK)
            here = seg_rows(segcol, n, 0)
            ahead = [None] + [(seg_rows(segcol, n, s) == here).astype(F32) for s in range(1, TAPS)]
            for c in range(3):
                total = weight_ref[c, TAPS - 1 : TAPS, lanes] * gin_ref[h, c, span, :]
                for s in range(1, TAPS):
                    later = gin_ref[h, c, n * CHUNK + s : (n + 1) * CHUNK + s, :]
                    total = total + weight_ref[c, TAPS - 1 - s : TAPS - s, lanes] * (ahead[s] * later)
                gproj_ref[c, span, lanes] = total.astype(BF16)


def mixer_shapes(proj, seg):
    seqs, length = seg.shape
    return seqs, length, proj.shape[2] // HEAD_DIM


def mixer_forward(proj, seg, weight, logits, gain):
    seqs, length, heads = mixer_shapes(proj, seg)
    tokens = seqs * length
    wide = PAIR * HEAD_DIM
    flat = pl.BlockSpec((length, wide), lambda s, p: (s, p))
    square = pl.BlockSpec((PAIR, length, CHUNK), lambda s, p: (p, s, 0))
    return pl.pallas_call(
        forward_kernel,
        grid=(seqs, heads // PAIR),
        in_specs=[
            pl.BlockSpec((3, length, wide), lambda s, p: (0, s, p)),
            pl.BlockSpec((1, 1, length), lambda s, p: (s, 0, 0)),
            pl.BlockSpec((3, TAPS, wide), lambda s, p: (0, 0, p)),
            pl.BlockSpec((logits.shape[0], length), lambda s, p: (0, s)),
            pl.BlockSpec((1, HEAD_DIM), lambda s, p: (0, 0)),
        ],
        out_specs=[flat, flat, square, square, square, flat, flat],
        out_shape=[
            jax.ShapeDtypeStruct((tokens, heads * HEAD_DIM), BF16),
            jax.ShapeDtypeStruct((tokens, heads * HEAD_DIM), F32),
            jax.ShapeDtypeStruct((heads, tokens, CHUNK), BF16),
            jax.ShapeDtypeStruct((heads, tokens, CHUNK), BF16),
            jax.ShapeDtypeStruct((heads, tokens, CHUNK), BF16),
            jax.ShapeDtypeStruct((tokens, heads * HEAD_DIM), BF16),
            jax.ShapeDtypeStruct((tokens, heads * HEAD_DIM), BF16),
        ],
        scratch_shapes=[pltpu.VMEM((length + 2 * HALO, CHUNK), F32)],
        compiler_params=pltpu.CompilerParams(vmem_limit_bytes=48 << 20),
        name="mixer_forward",
    )(proj, seg.reshape(seqs, 1, length), weight, logits, gain.reshape(1, HEAD_DIM))


def mixer_backward(proj, seg, weight, logits, gain, kept, grad_nout):
    seqs, length, heads = mixer_shapes(proj, seg)
    tokens = seqs * length
    wide = PAIR * HEAD_DIM
    mixed, inverse, scores, states, delta, err = kept
    flat = pl.BlockSpec((length, wide), lambda p, s: (s, p))
    square = pl.BlockSpec((PAIR, length, CHUNK), lambda p, s: (p, s, 0))
    cube = pl.BlockSpec((3, length, wide), lambda p, s: (0, s, p))
    taps = pl.BlockSpec((3, TAPS, wide), lambda p, s: (0, 0, p))
    line = pl.BlockSpec((PAIR, 1, length), lambda p, s: (p, 0, s))
    vector = pl.BlockSpec((1, HEAD_DIM), lambda p, s: (0, 0))
    return pl.pallas_call(
        backward_kernel,
        grid=(heads // PAIR, seqs),
        in_specs=[cube, pl.BlockSpec((1, 1, length), lambda p, s: (s, 0, 0)), taps, pl.BlockSpec((logits.shape[0], length), lambda p, s: (0, s)), vector, flat, square, square, square, flat, flat, flat],
        out_specs=[cube, line, taps, vector],
        out_shape=[
            jax.ShapeDtypeStruct(proj.shape, BF16),
            jax.ShapeDtypeStruct((heads, 1, tokens), BF16),
            jax.ShapeDtypeStruct(weight.shape, F32),
            jax.ShapeDtypeStruct((1, HEAD_DIM), F32),
        ],
        scratch_shapes=[
            pltpu.VMEM((length + 2 * HALO, CHUNK), F32),
            pltpu.VMEM((PAIR, 3, length + HALO, HEAD_DIM), F32),
            pltpu.VMEM((PAIR, 3, length, HEAD_DIM), F32),
            pltpu.VMEM((PAIR, length, HEAD_DIM), BF16),
            pltpu.VMEM((PAIR, length, HEAD_DIM), BF16),
            pltpu.VMEM((PAIR, length, HEAD_DIM), F32),
            pltpu.VMEM((PAIR, length, HEAD_DIM), F32),
            pltpu.VMEM((PAIR, length, HEAD_DIM), F32),
        ],
        compiler_params=pltpu.CompilerParams(vmem_limit_bytes=48 << 20),
        name="mixer_backward",
    )(proj, seg.reshape(seqs, 1, length), weight, logits, gain.reshape(1, HEAD_DIM), mixed, inverse, scores, states, delta, err, grad_nout)


MESH = pl.DeviceIdType.MESH
ROWS_PER = 128


def partners():
    me = lax.axis_index("tensor")
    near = me + 1 - 2 * lax.rem(me, 2)
    far = lax.rem(me + 2, 4)
    return me, near, far


def greet(near, far):
    barrier = pltpu.get_barrier_semaphore()
    for other in (near, far):
        pl.semaphore_signal(barrier, inc=1, device_id={"tensor": other}, device_id_type=MESH)
    pl.semaphore_wait(barrier, 2)


def push(src, dst, send, recv, other):
    return pltpu.make_async_remote_copy(src_ref=src, dst_ref=dst, send_sem=send, recv_sem=recv, device_id={"tensor": other}, device_id_type=MESH)


def band(m):
    return pl.ds(pl.multiple_of(m * ROWS_PER, ROWS_PER), ROWS_PER)


def part_of(q, width):
    return pl.ds(pl.multiple_of(q * width, width), width)


def loop(start, stop, body):
    lax.fori_loop(start, stop, lambda m, carry: (body(m), carry)[1], 0)


def project_kernel(x_ref, gain_ref, rate_ref, weight_ref, full_out, normed_out, proj_out, logit_ref,
                   full, weight, normed, proj, weight_sem, far_send, far_recv, near_send, near_recv, pass_send, pass_recv, full_sem, normed_sem, proj_sem):
    me, near, far = partners()
    width = x_ref.shape[1]
    chunks = x_ref.shape[0] // ROWS_PER
    mine, theirs = part_of(me, width), part_of(far, width)
    load = pltpu.make_async_copy(weight_ref, weight, weight_sem)
    load.start()
    greet(near, far)

    def to_far(m):
        return push(x_ref.at[band(m)], full.at[band(m), mine], far_send.at[m], far_recv.at[m], far)

    def to_near(m):
        return push(x_ref.at[band(m)], full.at[band(m), mine], near_send.at[m], near_recv.at[m], near)

    def onward(m):
        return push(full.at[band(m), theirs], full.at[band(m), theirs], pass_send.at[m], pass_recv.at[m], near)

    def out_full(m):
        return pltpu.make_async_copy(full.at[band(m)], full_out.at[band(m)], full_sem.at[m])

    def out_normed(m):
        return pltpu.make_async_copy(normed.at[band(m)], normed_out.at[band(m)], normed_sem.at[m])

    def out_proj(m):
        return pltpu.make_async_copy(proj.at[:, band(m)], proj_out.at[:, band(m)], proj_sem.at[m])

    def begin(m):
        to_far(m).start()
        to_near(m).start()
        full[band(m), mine] = x_ref[band(m), :]

    def compute(m):
        to_near(m).wait_recv()
        onward(m).wait_recv()
        values = full[band(m), :].astype(F32)
        low = (values * lax.rsqrt(jnp.mean(values * values, axis=-1, keepdims=True) + EPS) * gain_ref[...]).astype(BF16)
        normed[band(m), :] = low
        for c in range(3):
            proj[c, band(m), :] = jnp.dot(low, weight[c], preferred_element_type=F32)
        logit_ref[:, band(m)] = lax.dot_general(rate_ref[...], low, (((1,), (1,)), ((), ())), preferred_element_type=F32)
        out_full(m).start()
        out_normed(m).start()
        out_proj(m).start()

    def relay(m):
        to_far(m).wait_recv()
        onward(m).start()

    def both(m):
        relay(m)
        compute(m - 1)

    def finish(m):
        to_far(m).wait_send()
        to_near(m).wait_send()
        onward(m).wait_send()
        out_full(m).wait()
        out_normed(m).wait()
        out_proj(m).wait()

    loop(0, chunks, begin)
    relay(0)
    load.wait()
    loop(1, chunks, both)
    compute(chunks - 1)
    loop(0, chunks, finish)


def in_vmem():
    return pl.BlockSpec(memory_space=pltpu.VMEM)


def in_hbm():
    return pl.BlockSpec(memory_space=pl.ANY)


def project(hidden_in, gain, rate, weight):
    tokens, _ = hidden_in.shape
    wide = weight.shape[1]
    chunks = tokens // ROWS_PER
    sems = pltpu.SemaphoreType.DMA((chunks,))
    return pl.pallas_call(
        project_kernel,
        in_specs=[in_vmem(), in_vmem(), in_vmem(), in_hbm()],
        out_specs=[in_hbm(), in_hbm(), in_hbm(), in_vmem()],
        out_shape=[
            jax.ShapeDtypeStruct((tokens, wide), BF16),
            jax.ShapeDtypeStruct((tokens, wide), BF16),
            jax.ShapeDtypeStruct((3, tokens, weight.shape[2]), F32),
            jax.ShapeDtypeStruct((rate.shape[0], tokens), F32),
        ],
        scratch_shapes=[
            pltpu.VMEM((tokens, wide), BF16),
            pltpu.VMEM(weight.shape, BF16),
            pltpu.VMEM((tokens, wide), BF16),
            pltpu.VMEM((3, tokens, weight.shape[2]), F32),
            pltpu.SemaphoreType.DMA,
        ] + [sems] * 9,
        compiler_params=pltpu.CompilerParams(collective_id=0, has_side_effects=True, vmem_limit_bytes=56 << 20),
        name="project",
    )(hidden_in, gain.reshape(1, wide), rate, weight)


def middle_kernel(low_ref, wout_ref, gain_ref, own_ref, other_ref, x_ref, wdown_ref, wgu_ref,
                  middle_out, mid_out, normed_out, hidden_out, gate_out, up_out, cot_out, ffn_out,
                  x_full, cot, wdown, wgu, keep, first, got_first, second, got_second, mid, middle, ghid, normed, acts, ffn,
                  load_sem, cot_send, cot_recv, a_send, a_recv, b_send, b_recv, c_send, c_recv, middle_sem, mid_sem, normed_sem, act_sem, cot_sem, ffn_sem):
    me, near, far = partners()
    width = own_ref.shape[1]
    chunks = low_ref.shape[0] // ROWS_PER
    side, spot = lax.rem(me, 2), lax.div(me, 2)
    mine, theirs = part_of(me, width), part_of(far, width)
    loads = [
        pltpu.make_async_copy(own_ref, cot.at[:, mine], load_sem.at[0]),
        pltpu.make_async_copy(other_ref, cot.at[:, theirs], load_sem.at[1]),
        pltpu.make_async_copy(wdown_ref, wdown, load_sem.at[2]),
        pltpu.make_async_copy(x_ref, x_full, load_sem.at[3]),
        pltpu.make_async_copy(wgu_ref, wgu, load_sem.at[4]),
    ]
    for load in loads:
        load.start()
    greet(near, far)

    def send_first(m):
        return push(first.at[band(m)], got_first.at[band(m)], a_send.at[m], a_recv.at[m], near)

    def send_second(m):
        return push(second.at[band(m)], got_second.at[band(m)], b_send.at[m], b_recv.at[m], far)

    def share(m, which):
        at = (mine, theirs)[which]
        return push(mid.at[band(m), at], mid.at[band(m), at], c_send.at[m, which], c_recv.at[m, which], near)

    def out_middle(m):
        return pltpu.make_async_copy(middle.at[band(m)], middle_out.at[band(m)], middle_sem.at[m])

    def out_mid(m):
        return pltpu.make_async_copy(mid.at[band(m)], mid_out.at[band(m)], mid_sem.at[m])

    def out_normed(m):
        slot = lax.rem(m, 2)
        return pltpu.make_async_copy(normed.at[slot], normed_out.at[band(m)], normed_sem.at[slot])

    def out_ffn(m):
        slot = lax.rem(m, 2)
        return pltpu.make_async_copy(ffn.at[slot], ffn_out.at[band(m)], ffn_sem.at[slot])

    def out_act(m, which):
        slot = lax.rem(m, 2)
        return pltpu.make_async_copy(acts.at[slot, which], (hidden_out, gate_out, up_out)[which].at[band(m)], act_sem.at[slot, which])

    def project_out(m):
        rows = low_ref[band(m), :]
        for j in range(2):
            slot = slice(j * width, (j + 1) * width)
            first[band(m), slot] = jnp.dot(rows, wout_ref[:, part_of(2 * j + 1 - side, width)], preferred_element_type=F32).astype(BF16)
        send_first(m).start()
        for j in range(2):
            slot = slice(j * width, (j + 1) * width)
            keep[band(m), slot] = jnp.dot(rows, wout_ref[:, part_of(2 * j + side, width)], preferred_element_type=F32)

    def pair_sum(m):
        send_first(m).wait_recv()
        second[band(m), :] = (keep[band(m), :] + got_first[band(m), :].astype(F32)).astype(BF16)
        send_second(m).start()

    def feed(m):
        project_out(m)
        pair_sum(m - 1)

    def grad_hidden(m):
        ghid[band(m), :] = lax.dot_general(cot[band(m), :], wdown[...], (((1,), (1,)), ((), ())), preferred_element_type=F32)

    def total(m):
        send_second(m).wait_recv()
        for which, at, slot in ((0, mine, spot), (1, theirs, 1 - spot)):
            piece = part_of(slot, width)
            value = x_full[band(m), at].astype(F32) + (second[band(m), piece].astype(F32) + got_second[band(m), piece].astype(F32))
            if which == 0:
                middle[band(m), :] = value
            mid[band(m), at] = value.astype(BF16)
            share(m, which).start()
        out_middle(m).start()

    def compute(m):
        share(m, 0).wait_recv()
        share(m, 1).wait_recv()
        out_mid(m).start()
        slot = lax.rem(m, 2)

        @pl.when(m >= 2)
        def _():
            out_normed(m - 2).wait()
            out_ffn(m - 2).wait()
            for which in range(3):
                out_act(m - 2, which).wait()

        values = mid[band(m), :].astype(F32)
        low = (values * lax.rsqrt(jnp.mean(values * values, axis=-1, keepdims=True) + EPS) * gain_ref[...]).astype(BF16)
        normed[slot] = low
        out_normed(m).start()
        gate_pre = jnp.dot(low, wgu[0], preferred_element_type=F32)
        up_pre = jnp.dot(low, wgu[1], preferred_element_type=F32)
        gate = jax.nn.sigmoid(gate_pre)
        silu = gate_pre * gate
        grad = ghid[band(m), :]
        acts[slot, 0] = (silu * up_pre).astype(BF16)
        acts[slot, 1] = (grad * up_pre * (gate + silu * (1.0 - gate))).astype(BF16)
        acts[slot, 2] = (grad * silu).astype(BF16)
        for which in range(3):
            out_act(m, which).start()
        ffn[slot] = jnp.dot(acts[slot, 0], wdown[...], preferred_element_type=F32).astype(BF16)
        out_ffn(m).start()

    def both(m):
        total(m)
        compute(m - 1)

    loads[0].wait()
    loads[1].wait()
    shares = [push(cot.at[:, at], cot.at[:, at], cot_send.at[i], cot_recv.at[i], near) for i, at in enumerate((mine, theirs))]
    project_out(0)
    loop(1, chunks, feed)
    pair_sum(chunks - 1)
    for copy in shares:
        copy.start()
    loads[2].wait()
    loads[3].wait()
    for copy in shares:
        copy.wait_recv()
    save = pltpu.make_async_copy(cot, cot_out, cot_sem)
    save.start()
    loop(0, chunks, grad_hidden)
    loads[4].wait()
    total(0)
    loop(1, chunks, both)
    compute(chunks - 1)

    def finish(m):
        send_first(m).wait_send()
        send_second(m).wait_send()
        share(m, 0).wait_send()
        share(m, 1).wait_send()
        out_middle(m).wait()
        out_mid(m).wait()

    for m in (chunks - 2, chunks - 1):
        out_normed(m).wait()
        out_ffn(m).wait()
        for which in range(3):
            out_act(m, which).wait()
    for copy in shares:
        copy.wait_send()
    save.wait()
    loop(0, chunks, finish)


def middle_step(out_low, wout, gain, cot_own, cot_far, full_in, wdown, wgu):
    tokens, width = cot_own.shape
    wide, units = wgu.shape[1], wgu.shape[2]
    chunks = tokens // ROWS_PER
    dma = pltpu.SemaphoreType.DMA
    half = (tokens, wide // 2)
    return pl.pallas_call(
        middle_kernel,
        in_specs=[in_vmem(), in_vmem(), in_vmem()] + [in_hbm()] * 5,
        out_specs=[in_hbm()] * 8,
        out_shape=[
            jax.ShapeDtypeStruct((tokens, width), F32),
            jax.ShapeDtypeStruct((tokens, wide), BF16),
            jax.ShapeDtypeStruct((tokens, wide), BF16),
            jax.ShapeDtypeStruct((tokens, units), BF16),
            jax.ShapeDtypeStruct((tokens, units), BF16),
            jax.ShapeDtypeStruct((tokens, units), BF16),
            jax.ShapeDtypeStruct((tokens, wide), BF16),
            jax.ShapeDtypeStruct((tokens, wide), BF16),
        ],
        scratch_shapes=[
            pltpu.VMEM((tokens, wide), BF16),
            pltpu.VMEM((tokens, wide), BF16),
            pltpu.VMEM(wdown.shape, BF16),
            pltpu.VMEM(wgu.shape, BF16),
            pltpu.VMEM(half, F32),
            pltpu.VMEM(half, BF16),
            pltpu.VMEM(half, BF16),
            pltpu.VMEM(half, BF16),
            pltpu.VMEM(half, BF16),
            pltpu.VMEM((tokens, wide), BF16),
            pltpu.VMEM((tokens, width), F32),
            pltpu.VMEM((tokens, units), F32),
            pltpu.VMEM((2, ROWS_PER, wide), BF16),
            pltpu.VMEM((2, 3, ROWS_PER, units), BF16),
            pltpu.VMEM((2, ROWS_PER, wide), BF16),
            dma((5,)), dma((2,)), dma((2,)),
            dma((chunks,)), dma((chunks,)), dma((chunks,)), dma((chunks,)),
            dma((chunks, 2)), dma((chunks, 2)),
            dma((chunks,)), dma((chunks,)), dma((2,)), dma((2, 3)), dma, dma((2,)),
        ],
        compiler_params=pltpu.CompilerParams(collective_id=1, has_side_effects=True, vmem_limit_bytes=62 << 20),
        name="middle_step",
    )(out_low, wout, gain.reshape(1, wide), cot_own, cot_far, full_in, wdown, wgu)


def return_kernel(wout_ref, gain_ref, gate_ref, up_ref, mid_ref, cot_ref, wgu_ref,
                  gmid_out, full_out, nout_out, sum_ref,
                  gate, up, mid, cot, wgu, piece, keep, first, got_first, second, got_second, full, gmid, nout,
                  load_sem, a_send, a_recv, b_send, b_recv, c_send, c_recv, gmid_sem, full_sem, nout_sem):
    me, near, far = partners()
    width = gmid.shape[1]
    chunks = gmid.shape[0] // ROWS_PER
    side, spot = lax.rem(me, 2), lax.div(me, 2)
    mine, theirs = part_of(me, width), part_of(far, width)
    loads = [
        pltpu.make_async_copy(gate_ref, gate, load_sem.at[0]),
        pltpu.make_async_copy(wgu_ref.at[0], wgu.at[0], load_sem.at[1]),
        pltpu.make_async_copy(up_ref, up, load_sem.at[2]),
        pltpu.make_async_copy(wgu_ref.at[1], wgu.at[1], load_sem.at[3]),
        pltpu.make_async_copy(mid_ref, mid, load_sem.at[4]),
        pltpu.make_async_copy(cot_ref, cot, load_sem.at[5]),
    ]
    for load in loads:
        load.start()
    greet(near, far)
    sum_ref[...] = jnp.zeros_like(sum_ref)

    def send_first(m):
        return push(first.at[band(m)], got_first.at[band(m)], a_send.at[m], a_recv.at[m], near)

    def send_second(m):
        return push(second.at[band(m)], got_second.at[band(m)], b_send.at[m], b_recv.at[m], far)

    def share(m, which):
        at = (mine, theirs)[which]
        return push(full.at[band(m), at], full.at[band(m), at], c_send.at[m, which], c_recv.at[m, which], near)

    def outs(m):
        return [
            pltpu.make_async_copy(gmid.at[band(m)], gmid_out.at[band(m)], gmid_sem.at[m]),
            pltpu.make_async_copy(full.at[band(m)], full_out.at[band(m)], full_sem.at[m]),
            pltpu.make_async_copy(nout.at[band(m)], nout_out.at[band(m)], nout_sem.at[m]),
        ]

    def partial(m):
        dims = (((1,), (1,)), ((), ()))
        grad = lax.dot_general(gate[band(m), :], wgu[0], dims, preferred_element_type=F32)
        grad = grad + lax.dot_general(up[band(m), :], wgu[1], dims, preferred_element_type=F32)
        values = mid[band(m), :].astype(F32)
        scale = lax.rsqrt(jnp.mean(values * values, axis=-1, keepdims=True) + EPS)
        unit = values * scale
        sum_ref[...] += jnp.sum(grad * unit, axis=0, keepdims=True)
        scaled = grad * gain_ref[...]
        piece[...] = scale * (scaled - unit * jnp.mean(scaled * unit, axis=-1, keepdims=True))
        for j in range(2):
            slot = slice(j * width, (j + 1) * width)
            first[band(m), slot] = piece[:, part_of(2 * j + 1 - side, width)].astype(BF16)
            keep[band(m), slot] = piece[:, part_of(2 * j + side, width)]
        send_first(m).start()

    def pair_sum(m):
        send_first(m).wait_recv()
        second[band(m), :] = (keep[band(m), :] + got_first[band(m), :].astype(F32)).astype(BF16)
        send_second(m).start()

    def feed(m):
        partial(m)
        pair_sum(m - 1)

    def total(m):
        send_second(m).wait_recv()
        for which, at, slot in ((0, mine, spot), (1, theirs, 1 - spot)):
            part = part_of(slot, width)
            value = cot[band(m), at].astype(F32) + (second[band(m), part].astype(F32) + got_second[band(m), part].astype(F32))
            if which == 0:
                gmid[band(m), :] = value
            full[band(m), at] = value.astype(BF16)
            share(m, which).start()
        outs(m)[0].start()

    def compute(m):
        share(m, 0).wait_recv()
        share(m, 1).wait_recv()
        outs(m)[1].start()
        nout[band(m), :] = lax.dot_general(full[band(m), :], wout_ref[...], (((1,), (1,)), ((), ())), preferred_element_type=F32)
        outs(m)[2].start()

    def both(m):
        total(m)
        compute(m - 1)

    def finish(m):
        send_first(m).wait_send()
        send_second(m).wait_send()
        share(m, 0).wait_send()
        share(m, 1).wait_send()
        for copy in outs(m):
            copy.wait()

    for load in loads[:5]:
        load.wait()
    partial(0)
    loop(1, chunks, feed)
    pair_sum(chunks - 1)
    loads[5].wait()
    total(0)
    loop(1, chunks, both)
    compute(chunks - 1)
    loop(0, chunks, finish)


def return_step(wout, gain, grad_gate, grad_up, full_mid, full_cot, wgu):
    tokens, wide = full_mid.shape
    units = wgu.shape[2]
    width = wide // 4
    chunks = tokens // ROWS_PER
    dma = pltpu.SemaphoreType.DMA
    half = (tokens, wide // 2)
    return pl.pallas_call(
        return_kernel,
        in_specs=[in_vmem(), in_vmem()] + [in_hbm()] * 5,
        out_specs=[in_hbm()] * 3 + [in_vmem()],
        out_shape=[
            jax.ShapeDtypeStruct((tokens, width), F32),
            jax.ShapeDtypeStruct((tokens, wide), BF16),
            jax.ShapeDtypeStruct((tokens, wout.shape[0]), F32),
            jax.ShapeDtypeStruct((1, wide), F32),
        ],
        scratch_shapes=[
            pltpu.VMEM((tokens, units), BF16),
            pltpu.VMEM((tokens, units), BF16),
            pltpu.VMEM((tokens, wide), BF16),
            pltpu.VMEM((tokens, wide), BF16),
            pltpu.VMEM(wgu.shape, BF16),
            pltpu.VMEM((ROWS_PER, wide), F32),
            pltpu.VMEM(half, F32),
            pltpu.VMEM(half, BF16),
            pltpu.VMEM(half, BF16),
            pltpu.VMEM(half, BF16),
            pltpu.VMEM(half, BF16),
            pltpu.VMEM((tokens, wide), BF16),
            pltpu.VMEM((tokens, width), F32),
            pltpu.VMEM((tokens, wout.shape[0]), F32),
            dma((6,)),
            dma((chunks,)), dma((chunks,)), dma((chunks,)), dma((chunks,)),
            dma((chunks, 2)), dma((chunks, 2)),
            dma((chunks,)), dma((chunks,)), dma((chunks,)),
        ],
        compiler_params=pltpu.CompilerParams(collective_id=2, has_side_effects=True, vmem_limit_bytes=62 << 20),
        name="return_step",
    )(wout, gain.reshape(1, wide), grad_gate, grad_up, full_mid, full_cot, wgu)


ROWS = (((0,), (0,)), ((), ()))


def rms_scale(values):
    return lax.rsqrt(jnp.mean(values * values, axis=-1, keepdims=True) + EPS)


def norm_back(grad_normed, unit_rows, scale_rows, gain):
    scaled_grad = grad_normed * gain
    grad_rows = scale_rows * (scaled_grad - unit_rows * jnp.mean(scaled_grad * unit_rows, axis=-1, keepdims=True))
    return grad_rows, jnp.sum(grad_normed * unit_rows, axis=0)


def butterfly(values, axis, size):
    step = 1
    while step < size:
        pairs = [(i, i ^ step) for i in range(size)]
        values = values + lax.ppermute(values, axis, pairs)
        step *= 2
    return values


def row_major(values):
    return with_layout_constraint(values, Layout(tuple(range(values.ndim))))


def tie(value, token):
    return value if token is None else lax.optimization_barrier((value, token))[0]


class Timeline:
    def __init__(self, size):
        self.size = size
        self.bits = size.bit_length() - 1
        self.token = None
        self.open = {}
        self.later = {}
        self.rider = None
        self.rides = {}

    def after(self, value):
        return tie(value, self.token)

    def swap(self, values, bit):
        return lax.ppermute(values, "dp", [(i, i ^ (1 << bit)) for i in range(self.size)])

    def send(self, away, bit, ride):
        if not ride:
            return self.swap(away, bit)
        flat = away.reshape(-1, away.shape[-1])
        rider = lax.reduce_precision(self.rider, 8, 7)
        self.token = row_major(jnp.concatenate([flat, rider.astype(BF16)]))
        came = self.swap(self.token, bit)
        self.rider = rider + came[flat.shape[0] :].astype(F32)
        return came[: flat.shape[0]].reshape(away.shape)

    def half(self, values, bit, other):
        own = lax.rem(lax.div(lax.axis_index("dp"), 1 << bit), 2)
        side = 1 - own if other else own
        run = values.shape[1] // self.size << bit
        pieces = [lax.dynamic_slice_in_dim(values, (2 * i + side) * run, run, 1) for i in range(self.size // 2 >> bit)]
        return pieces[0] if len(pieces) == 1 else jnp.concatenate(pieces, axis=1)

    def product(self, rows, values):
        grad = lax.dot_general(rows, values, ROWS, preferred_element_type=F32).astype(BF16)
        return row_major(grad).reshape((2,) * (self.bits - 1) + (2 * rows.shape[1] // self.size, values.shape[1]))

    def scatter(self, name, rows, values, bit, ride=False):
        away = self.product(self.half(rows, bit, True), self.after(values))
        self.token = away
        came = self.send(away, bit, ride)
        self.rides[name] = ride
        order = [bit] + [i for i in range(self.bits) if i != bit]
        axes = [i for i in range(self.bits)[::-1] if i != bit]
        self.open[name] = ([came], axes, order, 1)
        self.later[name] = (rows, values, bit)

    def keep(self, name):
        rows, values, bit = self.later.pop(name)
        own = self.product(self.half(self.after(rows), bit, False), values)
        self.token = own
        terms, axes, order, stage = self.open[name]
        self.open[name] = ([own] + terms, axes, order, stage)

    def move(self, name):
        if name in self.later:
            self.keep(name)
        terms, axes, order, stage = self.open[name]
        bit = order[stage]
        own = lax.rem(lax.div(lax.axis_index("dp"), 1 << bit), 2)
        axis = axes.index(bit)
        terms = terms[:-1] + [self.after(terms[-1])]

        def pick(value, at):
            return lax.dynamic_index_in_dim(value, at, axis, keepdims=False)

        away = row_major(sum(pick(t, 1 - own).astype(F32) for t in terms).astype(BF16))
        self.token = away
        came = self.send(away, bit, self.rides[name])
        self.open[name] = ([pick(t, own) for t in terms] + [came], axes[:axis] + axes[axis + 1 :], order, stage + 1)

    def close(self, name):
        while self.open[name][3] < self.bits:
            self.move(name)
        terms = self.open.pop(name)[0]
        terms = terms[:-1] + [self.after(terms[-1])]
        return row_major(sum(t.astype(F32) for t in terms))


def make_body(dp_size, tensor_size):
    def body(hidden_in, seg_ids, attn_gain, wqkv, conv_weight, wrate, onorm_gain, wout, mlp_gain, wgu, wdown, cotangent):
        return step(hidden_in, seg_ids, attn_gain, wqkv, conv_weight, wrate, onorm_gain, wout, mlp_gain, wgu, wdown, cotangent)

    def step(hidden_in, seg_ids, attn_gain, wqkv, conv_weight, wrate, onorm_gain, wout, mlp_gain, wgu, wdown, cotangent):
        tokens, width = hidden_in.shape
        heads = wrate.shape[1]
        me = lax.axis_index("tensor")
        side, spot = lax.rem(me, 2), lax.div(me, 2)

        def swap(values, step):
            return lax.ppermute(values, "tensor", [(i, i ^ step) for i in range(tensor_size)])

        def columns(values, q):
            return lax.dynamic_slice_in_dim(values, q * width, width, 1)

        def quarter_sum(pick):
            away = jnp.concatenate([pick(2 * j + 1 - side).astype(BF16) for j in range(2)], axis=1)
            came = swap(away, 1)
            other = (pick(lax.rem(me + 2, 4)) + columns(came, 1 - spot).astype(F32)).astype(BF16)
            far = swap(other, 2)
            return pick(me) + columns(came, spot).astype(F32), far

        taps = conv_weight.astype(F32)
        rates = jnp.zeros((8, wrate.shape[0]), BF16).at[:heads].set(wrate.T)
        full_low, normed_one, proj, logits = project(hidden_in, attn_gain, rates, wqkv)
        cot_own, _ = lax.optimization_barrier((cotangent, logits))
        cot_far = swap(cot_own, 2)
        out_low, *kept = mixer_forward(proj, seg_ids, taps, logits, onorm_gain)
        middle, mid_low, normed_two, hidden, grad_gate, grad_up, full_cot, ffn_part = middle_step(out_low, wout, mlp_gain, cotangent, cot_far, full_low, wdown, wgu)
        line = Timeline(dp_size)
        cut = grad_up.shape[1] // 11 * 4
        line.scatter("down", full_cot, hidden, 0)
        line.scatter("gate", normed_two, grad_gate, 1)
        line.scatter("upx", normed_two, grad_up[:, cut:], 0)
        line.scatter("upz", normed_two, grad_up[:, :cut], 1)
        late_gate = line.after(grad_gate)
        grad_middle, full_grad_mid, grad_nout, gain_two = return_step(wout, mlp_gain, late_gate, grad_up, mid_low, full_cot, wgu)
        line.token = grad_nout
        line.move("down")
        line.scatter("out", full_grad_mid, out_low, 0)
        line.move("gate")
        line.move("upx")
        grad_proj, grad_logits, grad_conv, gain_onorm = mixer_backward(proj, seg_ids, taps, logits, onorm_gain, kept, line.after(grad_nout))
        line.token = grad_logits
        grad_logits = grad_logits.reshape(heads, tokens)
        line.move("down")
        line.move("upz")
        line.scatter("k", normed_one, grad_proj[1], 0)
        late_low, late_proj = line.after((full_low, grad_proj))
        grad_nin = jnp.einsum("ctk,cdk->td", late_proj, wqkv, preferred_element_type=F32)
        grad_nin = grad_nin + jnp.einsum("ht,dh->td", grad_logits, wrate, preferred_element_type=F32)
        full_in = late_low.astype(F32)
        scale_one = rms_scale(full_in)
        part_one, gain_one = norm_back(grad_nin, full_in * scale_one, scale_one, attn_gain)
        part_one = part_one.astype(BF16)
        line.token = (part_one, gain_one)
        wide = gain_one.shape[0]
        gains = butterfly(jnp.concatenate([gain_one, gain_two.reshape(-1), gain_onorm.reshape(-1)]), "tensor", tensor_size)
        shared = gains.shape[0]
        line.move("gate")
        grad_beta = jnp.einsum("td,ht->dh", normed_one, line.after(grad_logits), preferred_element_type=F32)
        line.move("out")
        small = jnp.concatenate([gains, grad_conv.reshape(-1), grad_beta.reshape(-1)])
        lanes = grad_proj.shape[2]
        extra = -small.shape[0] % (16 * lanes)
        line.rider = jnp.pad(small, (0, extra)).reshape(-1, lanes)
        line.scatter("v", normed_one, grad_proj[2], 0, ride=True)
        line.scatter("q", normed_one, grad_proj[0], 0)
        line.move("upx")
        line.move("k")
        line.move("upz")
        line.move("out")
        one, one_far = quarter_sum(lambda q: columns(part_one, q).astype(F32))
        line.keep("v")
        line.move("v")
        late_ffn = line.after(ffn_part)
        ffn, ffn_far = quarter_sum(lambda q: columns(late_ffn, q).astype(F32))
        line.keep("q")
        grad_down = line.close("down").T
        line.token = grad_down
        line.move("k")
        line.move("q")
        line.move("v")
        grad_gate_w = line.close("gate")
        grad_in = (grad_middle + one + line.after(one_far).astype(F32)).astype(BF16)
        line.token = (grad_gate_w, grad_in)
        grad_up_w = jnp.concatenate([line.close("upz"), line.close("upx")], axis=1)
        grad_gate_up = jnp.stack([grad_gate_w, grad_up_w])
        grad_out = line.close("out").T
        layer_out = (middle + ffn + line.after(ffn_far).astype(F32)).astype(BF16)
        line.token = (grad_gate_up, grad_out, layer_out)
        line.move("q")
        grad_k, grad_v = line.close("k"), line.close("v")
        small = line.rider.reshape(-1)
        grad_qkv = jnp.stack([grad_k, grad_k, grad_v])
        line.token = (grad_qkv, small)
        grad_qkv = lax.dynamic_update_slice(grad_qkv, line.close("q")[None], (0, 0, 0))
        gains = small[:shared]
        mine = grad_beta.shape[0] // dp_size
        rest = small[shared + grad_conv.size :]
        grad_conv = small[shared : shared + grad_conv.size].reshape(grad_conv.shape)
        grad_beta = rest[: grad_beta.size].reshape(grad_beta.shape)
        grad_beta = lax.dynamic_slice_in_dim(grad_beta, lax.axis_index("dp") * mine, mine, 0)
        return (
            layer_out,
            grad_in,
            gains[:wide],
            grad_qkv,
            grad_conv,
            grad_beta,
            gains[2 * wide :],
            grad_out,
            gains[wide : 2 * wide],
            grad_gate_up,
            grad_down,
        )

    return body


def solution(mesh):
    return jax.shard_map(
        make_body(mesh.shape["dp"], mesh.shape["tensor"]),
        mesh=mesh,
        in_specs=(
            P("dp", "tensor"),
            P("dp", None),
            P(),
            P(None, None, "tensor"),
            P(None, None, "tensor"),
            P(None, "tensor"),
            P(),
            P("tensor", None),
            P(),
            P(None, None, "tensor"),
            P("tensor", None),
            P("dp", "tensor"),
        ),
        out_specs=(
            P("dp", "tensor"),
            P("dp", "tensor"),
            P(),
            P(None, "dp", "tensor"),
            P(None, None, "tensor"),
            P("dp", "tensor"),
            P(),
            P("tensor", "dp"),
            P(),
            P(None, "dp", "tensor"),
            P("tensor", "dp"),
        ),
        check_vma=False,
    )
```

```python
import jax
import jax.numpy as jnp
from jax import lax
from jax.experimental import pallas as pl
from jax.experimental.pallas import tpu as pltpu
from jax.experimental.layout import Layout, with_layout_constraint
from jax.sharding import PartitionSpec as P

HEAD_DIM = 128
TAPS = 4
CHUNK = 128
HALO = 8
EPS = 1e-06
PAIR = 2
F32 = jnp.float32
BF16 = jnp.bfloat16


def dot_nn(a, b):
    return jnp.dot(a.astype(BF16), b.astype(BF16), preferred_element_type=F32)


def dot_nt(a, b):
    return lax.dot_general(a.astype(BF16), b.astype(BF16), (((1,), (1,)), ((), ())), preferred_element_type=F32)


def dot_tn(a, b):
    return lax.dot_general(a.astype(BF16), b.astype(BF16), (((0,), (0,)), ((), ())), preferred_element_type=F32)


def column(row):
    return jnp.broadcast_to(row, (CHUNK, CHUNK)).T


def logit_row(logit_ref, head, span):
    values = logit_ref[:, span]
    return jnp.sum(jnp.where(lax.broadcasted_iota(jnp.int32, values.shape, 0) == head, values, 0.0), axis=0, keepdims=True)


def load_segments(seg_ref, segcol, length):
    segcol[0:HALO, :] = jnp.full((HALO, CHUNK), -1.0, F32)
    segcol[HALO + length :, :] = jnp.full((HALO, CHUNK), -2.0, F32)
    for n in range(length // CHUNK):
        row = seg_ref[0, :, n * CHUNK : (n + 1) * CHUNK].astype(F32)
        segcol[HALO + n * CHUNK : HALO + (n + 1) * CHUNK, :] = column(row)


def seg_rows(segcol, n, shift):
    base = HALO + n * CHUNK + shift
    return segcol[base : base + CHUNK, :]


def back_masks(segcol, n):
    here = seg_rows(segcol, n, 0)
    return [None] + [(seg_rows(segcol, n, -s) == here).astype(F32) for s in range(1, TAPS)]


def state_masks(seg_ref, segcol, n):
    here = seg_rows(segcol, n, 0)
    row = jnp.broadcast_to(seg_ref[0, :, n * CHUNK : (n + 1) * CHUNK].astype(F32), (CHUNK, CHUNK))
    same = here == row
    before = segcol[HALO + n * CHUNK - 1 : HALO + n * CHUNK, :]
    last = segcol[HALO + (n + 1) * CHUNK - 1 : HALO + (n + 1) * CHUNK, :]
    carry = (here == before).astype(F32)
    tail = (here == last).astype(F32)
    carry_last = (last == before).astype(F32)
    return same, carry, tail, carry_last


def taps_in(proj_ref, c, h, n):
    lanes = slice(h * HEAD_DIM, (h + 1) * HEAD_DIM)
    if n == 0:
        return jnp.concatenate([jnp.zeros((HALO, HEAD_DIM), F32), proj_ref[c, 0:CHUNK, lanes].astype(F32)], axis=0)
    return proj_ref[c, n * CHUNK - HALO : (n + 1) * CHUNK, lanes].astype(F32)


def conv_rows(window, weight_ref, c, h, masks):
    lanes = slice(h * HEAD_DIM, (h + 1) * HEAD_DIM)
    total = weight_ref[c, TAPS - 1 : TAPS, lanes] * window[HALO:]
    for s in range(1, TAPS):
        total = total + weight_ref[c, TAPS - 1 - s : TAPS - s, lanes] * (masks[s] * window[HALO - s : HALO - s + CHUNK])
    return total


def grid_ids():
    rows = lax.broadcasted_iota(jnp.int32, (CHUNK, CHUNK), 0)
    cols = lax.broadcasted_iota(jnp.int32, (CHUNK, CHUNK), 1)
    return rows, cols


def forward_kernel(proj_ref, seg_ref, weight_ref, logit_ref, gain_ref, out_ref, mixed_ref, inv_ref, score_ref, state_ref, delta_ref, err_ref, segcol):
    length = proj_ref.shape[1]
    chunks = length // CHUNK
    load_segments(seg_ref, segcol, length)
    rows, cols = grid_ids()
    apart = rows ^ cols
    lower = rows > cols
    lower_incl = rows >= cols
    scale = HEAD_DIM**-0.5
    pieces, systems, inverses = {}, {}, {}
    for n in range(chunks):
        masks = back_masks(segcol, n)
        same, carry, tail, carry_last = state_masks(seg_ref, segcol, n)
        span = slice(n * CHUNK, (n + 1) * CHUNK)
        for h in range(PAIR):
            acts = []
            for c in range(3):
                conv = conv_rows(taps_in(proj_ref, c, h, n), weight_ref, c, h, masks)
                acts.append(conv * jax.nn.sigmoid(conv))
            q = (acts[0] * lax.rsqrt(jnp.sum(acts[0] * acts[0], axis=-1, keepdims=True) + EPS)).astype(BF16)
            k = (acts[1] * lax.rsqrt(jnp.sum(acts[1] * acts[1], axis=-1, keepdims=True) + EPS)).astype(BF16)
            v = acts[2].astype(BF16).astype(F32)
            rate = jax.nn.sigmoid(column(logit_row(logit_ref, PAIR * pl.program_id(1) + h, span)))
            gram = jnp.where(same & lower, dot_nt(k, k), 0.0)
            scores = (jnp.where(same & lower_incl, dot_nt(q, k), 0.0) * scale).astype(BF16)
            system = rate * gram
            score_ref[h, span, :] = scores
            systems[n, h] = system
            inverses[n, h] = jnp.where(rows == cols, 1.0, 0.0) - jnp.where(apart == 1, system, 0.0)
            pieces[n, h] = (q, k.astype(F32), v, gram, scores, rate, carry, tail, carry_last)
    level = 1
    while (2 << level) <= CHUNK:
        crossed = {}
        for key, inverse in inverses.items():
            crossed[key] = dot_nn(jnp.where((apart >> level) == 1, systems[key], 0.0), inverse)
        for key, inverse in inverses.items():
            inverses[key] = inverse - dot_nn(inverse, crossed[key])
        level += 1
    for n, h in pieces:
        q, kf, v, gram, scores, rate, carry, tail, carry_last = pieces[n, h]
        inverse = inverses[n, h].astype(BF16)
        inv_ref[h, n * CHUNK : (n + 1) * CHUNK, :] = inverse
        base = dot_nn(inverse, rate * v)
        back = dot_nn(inverse, rate * carry * kf)
        pieces[n, h] = (q, kf, v, gram, scores, base, back, carry, tail, carry_last)
    for h in range(PAIR):
        lanes = slice(h * HEAD_DIM, (h + 1) * HEAD_DIM)
        state = None
        for n in range(chunks):
            span = slice(n * CHUNK, (n + 1) * CHUNK)
            q, kf, v, gram, scores, base, back, carry, tail, carry_last = pieces[n, h]
            if n == 0:
                delta = base
                rest = v
                state_ref[h, span, :] = jnp.zeros((CHUNK, CHUNK), BF16)
            else:
                low = state.astype(BF16)
                state_ref[h, span, :] = low
                delta = base - dot_nn(back, low)
                rest = v - carry * dot_nn(kf, low)
            delta_low = delta.astype(BF16)
            moved = dot_tn(tail * kf, delta_low)
            mixed = dot_nn(scores, delta_low)
            if n > 0:
                mixed = mixed + (carry * scale) * dot_nn(q, low)
                moved = moved + carry_last * state
            state = moved
            delta_ref[span, lanes] = delta_low
            err_ref[span, lanes] = (rest - dot_nn(gram, delta_low)).astype(BF16)
            mixed_ref[span, lanes] = mixed
            root = lax.rsqrt(jnp.mean(mixed * mixed, axis=-1, keepdims=True) + EPS)
            out_ref[span, lanes] = (mixed * root * gain_ref[...]).astype(BF16)


def backward_kernel(proj_ref, seg_ref, weight_ref, logit_ref, gain_ref, mixed_ref, inv_ref, score_ref, state_ref, delta_ref, err_ref, nout_ref,
                    gproj_ref, glogit_ref, gconv_ref, gonorm_ref, segcol, gin_ref, act_ref, q_ref, k_ref, head_ref, dq_ref, dk_ref):
    length = proj_ref.shape[1]
    chunks = length // CHUNK
    pair, seq = pl.program_id(0), pl.program_id(1)
    load_segments(seg_ref, segcol, length)
    rows, cols = grid_ids()
    lower = rows > cols
    lower_incl = rows >= cols
    scale = HEAD_DIM**-0.5

    @pl.when((pair == 0) & (seq == 0))
    def _():
        gonorm_ref[...] = jnp.zeros_like(gonorm_ref)

    @pl.when(seq == 0)
    def _():
        gconv_ref[...] = jnp.zeros_like(gconv_ref)

    onorm = jnp.zeros((1, HEAD_DIM), F32)
    pieces = {}
    for n in range(chunks):
        masks = back_masks(segcol, n)
        same, carry, tail, carry_last = state_masks(seg_ref, segcol, n)
        span = slice(n * CHUNK, (n + 1) * CHUNK)
        for h in range(PAIR):
            lanes = slice(h * HEAD_DIM, (h + 1) * HEAD_DIM)
            for c in range(3):
                act_ref[h, c, span, :] = conv_rows(taps_in(proj_ref, c, h, n), weight_ref, c, h, masks)
            conv = act_ref[h, 0, span, :]
            act = conv * jax.nn.sigmoid(conv)
            q = (act * lax.rsqrt(jnp.sum(act * act, axis=-1, keepdims=True) + EPS)).astype(BF16)
            conv = act_ref[h, 1, span, :]
            act = conv * jax.nn.sigmoid(conv)
            k = (act * lax.rsqrt(jnp.sum(act * act, axis=-1, keepdims=True) + EPS)).astype(BF16)
            q_ref[h, span, :] = q
            k_ref[h, span, :] = k
            mixed = mixed_ref[span, lanes]
            root = lax.rsqrt(jnp.mean(mixed * mixed, axis=-1, keepdims=True) + EPS)
            unit = mixed * root
            grad = nout_ref[span, lanes].astype(F32)
            onorm = onorm + jnp.sum(grad * unit, axis=0, keepdims=True)
            scaled = grad * gain_ref[...]
            gmix = root * (scaled - unit * jnp.mean(scaled * unit, axis=-1, keepdims=True))
            glow = gmix.astype(BF16)
            inverse = inv_ref[h, span, :]
            delta = delta_ref[span, lanes]
            gscore = (jnp.where(same & lower_incl, dot_nt(glow, delta), 0.0) * scale).astype(BF16)
            dq = dot_nn(gscore, k)
            held = (scale * carry * gmix).astype(BF16)
            if n > 0:
                dq = dq + dot_nt(held, state_ref[h, span, :])
            dq_ref[h, span, :] = dq
            dk_ref[h, span, :] = dot_tn(gscore, q)
            start = dot_tn(inverse, dot_tn(score_ref[h, span, :], glow))
            kf = k.astype(F32)
            reach = dot_tn(inverse, tail * kf).astype(BF16)
            feed = dot_tn(q, held)
            pieces[n, h] = (start, reach, feed)
    gonorm_ref[...] += onorm
    for h in range(PAIR):
        lanes = slice(h * HEAD_DIM, (h + 1) * HEAD_DIM)
        flow = None
        for n in reversed(range(chunks)):
            span = slice(n * CHUNK, (n + 1) * CHUNK)
            same, carry, tail, carry_last = state_masks(seg_ref, segcol, n)
            rate = jax.nn.sigmoid(column(logit_row(logit_ref, PAIR * pair + h, span)))
            start, reach, feed = pieces[n, h]
            k = k_ref[h, span, :]
            delta = delta_ref[span, lanes]
            gtarget = start
            if flow is not None:
                low = flow.astype(BF16)
                gtarget = gtarget + dot_nn(reach, low)
            gval = rate * gtarget
            head_ref[h, span, :] = gval
            grecall = (carry * gval).astype(BF16)
            dk = dk_ref[h, span, :]
            if flow is not None:
                dk = dk + tail * dot_nt(delta, low)
            if n > 0:
                dk = dk - dot_nt(grecall, state_ref[h, span, :])
                nxt = feed - dot_tn(k, grecall)
                if flow is not None:
                    nxt = nxt + carry_last * flow
                flow = nxt
            ggram = jnp.where(same & lower, dot_nt(gval, delta), 0.0)
            dk_ref[h, span, :] = dk - dot_nn(ggram + ggram.T, k)
            grate = jnp.sum(err_ref[span, lanes].astype(F32) * gtarget, axis=-1, keepdims=True)
            glogit = jnp.broadcast_to(grate, (CHUNK, CHUNK)) * rate * (1.0 - rate)
            glogit_ref[h, :, span] = glogit.T[0:1, :].astype(BF16)
    for h in range(PAIR):
        lanes = slice(h * HEAD_DIM, (h + 1) * HEAD_DIM)
        for c in range(3):
            gin_ref[h, c, length:, :] = jnp.zeros((HALO, HEAD_DIM), F32)
        taps = [[jnp.zeros((1, HEAD_DIM), F32)] * TAPS for _ in range(3)]
        for n in range(chunks):
            masks = back_masks(segcol, n)
            span = slice(n * CHUNK, (n + 1) * CHUNK)
            for c in range(3):
                conv = act_ref[h, c, span, :]
                gate = jax.nn.sigmoid(conv)
                act = conv * gate
                if c == 2:
                    gact = head_ref[h, span, :]
                else:
                    gunit = (dq_ref if c == 0 else dk_ref)[h, span, :]
                    inv = lax.rsqrt(jnp.sum(act * act, axis=-1, keepdims=True) + EPS)
                    unit = act * inv
                    gact = inv * (gunit - unit * jnp.sum(gunit * unit, axis=-1, keepdims=True))
                gin = gact * (gate + act * (1.0 - gate))
                gin_ref[h, c, span, :] = gin
                window = taps_in(proj_ref, c, h, n)
                taps[c][TAPS - 1] = taps[c][TAPS - 1] + jnp.sum(gin * window[HALO:], axis=0, keepdims=True)
                for s in range(1, TAPS):
                    part = jnp.sum(gin * masks[s] * window[HALO - s : HALO - s + CHUNK], axis=0, keepdims=True)
                    taps[c][TAPS - 1 - s] = taps[c][TAPS - 1 - s] + part
        for c in range(3):
            gconv_ref[c, :, lanes] += jnp.concatenate(taps[c], axis=0)
        for n in range(chunks):
            span = slice(n * CHUNK, (n + 1) * CHUNK)
            here = seg_rows(segcol, n, 0)
            ahead = [None] + [(seg_rows(segcol, n, s) == here).astype(F32) for s in range(1, TAPS)]
            for c in range(3):
                total = weight_ref[c, TAPS - 1 : TAPS, lanes] * gin_ref[h, c, span, :]
                for s in range(1, TAPS):
                    later = gin_ref[h, c, n * CHUNK + s : (n + 1) * CHUNK + s, :]
                    total = total + weight_ref[c, TAPS - 1 - s : TAPS - s, lanes] * (ahead[s] * later)
                gproj_ref[c, span, lanes] = total.astype(BF16)


def mixer_shapes(proj, seg):
    seqs, length = seg.shape
    return seqs, length, proj.shape[2] // HEAD_DIM


def mixer_forward(proj, seg, weight, logits, gain):
    seqs, length, heads = mixer_shapes(proj, seg)
    tokens = seqs * length
    wide = PAIR * HEAD_DIM
    flat = pl.BlockSpec((length, wide), lambda s, p: (s, p))
    square = pl.BlockSpec((PAIR, length, CHUNK), lambda s, p: (p, s, 0))
    return pl.pallas_call(
        forward_kernel,
        grid=(seqs, heads // PAIR),
        in_specs=[
            pl.BlockSpec((3, length, wide), lambda s, p: (0, s, p)),
            pl.BlockSpec((1, 1, length), lambda s, p: (s, 0, 0)),
            pl.BlockSpec((3, TAPS, wide), lambda s, p: (0, 0, p)),
            pl.BlockSpec((logits.shape[0], length), lambda s, p: (0, s)),
            pl.BlockSpec((1, HEAD_DIM), lambda s, p: (0, 0)),
        ],
        out_specs=[flat, flat, square, square, square, flat, flat],
        out_shape=[
            jax.ShapeDtypeStruct((tokens, heads * HEAD_DIM), BF16),
            jax.ShapeDtypeStruct((tokens, heads * HEAD_DIM), F32),
            jax.ShapeDtypeStruct((heads, tokens, CHUNK), BF16),
            jax.ShapeDtypeStruct((heads, tokens, CHUNK), BF16),
            jax.ShapeDtypeStruct((heads, tokens, CHUNK), BF16),
            jax.ShapeDtypeStruct((tokens, heads * HEAD_DIM), BF16),
            jax.ShapeDtypeStruct((tokens, heads * HEAD_DIM), BF16),
        ],
        scratch_shapes=[pltpu.VMEM((length + 2 * HALO, CHUNK), F32)],
        compiler_params=pltpu.CompilerParams(vmem_limit_bytes=48 << 20),
        name="mixer_forward",
    )(proj, seg.reshape(seqs, 1, length), weight, logits, gain.reshape(1, HEAD_DIM))


def mixer_backward(proj, seg, weight, logits, gain, kept, grad_nout):
    seqs, length, heads = mixer_shapes(proj, seg)
    tokens = seqs * length
    wide = PAIR * HEAD_DIM
    mixed, inverse, scores, states, delta, err = kept
    flat = pl.BlockSpec((length, wide), lambda p, s: (s, p))
    square = pl.BlockSpec((PAIR, length, CHUNK), lambda p, s: (p, s, 0))
    cube = pl.BlockSpec((3, length, wide), lambda p, s: (0, s, p))
    taps = pl.BlockSpec((3, TAPS, wide), lambda p, s: (0, 0, p))
    line = pl.BlockSpec((PAIR, 1, length), lambda p, s: (p, 0, s))
    vector = pl.BlockSpec((1, HEAD_DIM), lambda p, s: (0, 0))
    return pl.pallas_call(
        backward_kernel,
        grid=(heads // PAIR, seqs),
        in_specs=[cube, pl.BlockSpec((1, 1, length), lambda p, s: (s, 0, 0)), taps, pl.BlockSpec((logits.shape[0], length), lambda p, s: (0, s)), vector, flat, square, square, square, flat, flat, flat],
        out_specs=[cube, line, taps, vector],
        out_shape=[
            jax.ShapeDtypeStruct(proj.shape, BF16),
            jax.ShapeDtypeStruct((heads, 1, tokens), BF16),
            jax.ShapeDtypeStruct(weight.shape, F32),
            jax.ShapeDtypeStruct((1, HEAD_DIM), F32),
        ],
        scratch_shapes=[
            pltpu.VMEM((length + 2 * HALO, CHUNK), F32),
            pltpu.VMEM((PAIR, 3, length + HALO, HEAD_DIM), F32),
            pltpu.VMEM((PAIR, 3, length, HEAD_DIM), F32),
            pltpu.VMEM((PAIR, length, HEAD_DIM), BF16),
            pltpu.VMEM((PAIR, length, HEAD_DIM), BF16),
            pltpu.VMEM((PAIR, length, HEAD_DIM), F32),
            pltpu.VMEM((PAIR, length, HEAD_DIM), F32),
            pltpu.VMEM((PAIR, length, HEAD_DIM), F32),
        ],
        compiler_params=pltpu.CompilerParams(vmem_limit_bytes=48 << 20),
        name="mixer_backward",
    )(proj, seg.reshape(seqs, 1, length), weight, logits, gain.reshape(1, HEAD_DIM), mixed, inverse, scores, states, delta, err, grad_nout)


MESH = pl.DeviceIdType.MESH
ROWS_PER = 128


def partners():
    me = lax.axis_index("tensor")
    near = me + 1 - 2 * lax.rem(me, 2)
    far = lax.rem(me + 2, 4)
    return me, near, far


def greet(near, far):
    barrier = pltpu.get_barrier_semaphore()
    for other in (near, far):
        pl.semaphore_signal(barrier, inc=1, device_id={"tensor": other}, device_id_type=MESH)
    pl.semaphore_wait(barrier, 2)


def push(src, dst, send, recv, other):
    return pltpu.make_async_remote_copy(src_ref=src, dst_ref=dst, send_sem=send, recv_sem=recv, device_id={"tensor": other}, device_id_type=MESH)


def band(m):
    return pl.ds(pl.multiple_of(m * ROWS_PER, ROWS_PER), ROWS_PER)


def part_of(q, width):
    return pl.ds(pl.multiple_of(q * width, width), width)


def loop(start, stop, body):
    lax.fori_loop(start, stop, lambda m, carry: (body(m), carry)[1], 0)


def project_kernel(x_ref, gain_ref, rate_ref, weight_ref, full_out, normed_out, proj_out, logit_ref,
                   full, weight, normed, proj, weight_sem, far_send, far_recv, near_send, near_recv, pass_send, pass_recv, full_sem, normed_sem, proj_sem):
    me, near, far = partners()
    width = x_ref.shape[1]
    chunks = x_ref.shape[0] // ROWS_PER
    mine, theirs = part_of(me, width), part_of(far, width)
    load = pltpu.make_async_copy(weight_ref, weight, weight_sem)
    load.start()
    greet(near, far)

    def to_far(m):
        return push(x_ref.at[band(m)], full.at[band(m), mine], far_send.at[m], far_recv.at[m], far)

    def to_near(m):
        return push(x_ref.at[band(m)], full.at[band(m), mine], near_send.at[m], near_recv.at[m], near)

    def onward(m):
        return push(full.at[band(m), theirs], full.at[band(m), theirs], pass_send.at[m], pass_recv.at[m], near)

    def out_full(m):
        return pltpu.make_async_copy(full.at[band(m)], full_out.at[band(m)], full_sem.at[m])

    def out_normed(m):
        return pltpu.make_async_copy(normed.at[band(m)], normed_out.at[band(m)], normed_sem.at[m])

    def out_proj(m):
        return pltpu.make_async_copy(proj.at[:, band(m)], proj_out.at[:, band(m)], proj_sem.at[m])

    def begin(m):
        to_far(m).start()
        to_near(m).start()
        full[band(m), mine] = x_ref[band(m), :]

    def compute(m):
        to_near(m).wait_recv()
        onward(m).wait_recv()
        values = full[band(m), :].astype(F32)
        low = (values * lax.rsqrt(jnp.mean(values * values, axis=-1, keepdims=True) + EPS) * gain_ref[...]).astype(BF16)
        normed[band(m), :] = low
        for c in range(3):
            proj[c, band(m), :] = jnp.dot(low, weight[c], preferred_element_type=F32)
        logit_ref[:, band(m)] = lax.dot_general(rate_ref[...], low, (((1,), (1,)), ((), ())), preferred_element_type=F32)
        out_full(m).start()
        out_normed(m).start()
        out_proj(m).start()

    def relay(m):
        to_far(m).wait_recv()
        onward(m).start()

    def both(m):
        pl.when(m < chunks)(lambda: relay(m))
        pl.when(m > 0)(lambda: compute(m - 1))

    def finish(m):
        to_far(m).wait_send()
        to_near(m).wait_send()
        onward(m).wait_send()
        out_full(m).wait()
        out_normed(m).wait()
        out_proj(m).wait()

    loop(0, chunks, begin)
    load.wait()
    loop(0, chunks + 1, both)
    loop(0, chunks, finish)


def in_vmem():
    return pl.BlockSpec(memory_space=pltpu.VMEM)


def in_hbm():
    return pl.BlockSpec(memory_space=pl.ANY)


def project(hidden_in, gain, rate, weight):
    tokens, _ = hidden_in.shape
    wide = weight.shape[1]
    chunks = tokens // ROWS_PER
    sems = pltpu.SemaphoreType.DMA((chunks,))
    return pl.pallas_call(
        project_kernel,
        in_specs=[in_vmem(), in_vmem(), in_vmem(), in_hbm()],
        out_specs=[in_hbm(), in_hbm(), in_hbm(), in_vmem()],
        out_shape=[
            jax.ShapeDtypeStruct((tokens, wide), BF16),
            jax.ShapeDtypeStruct((tokens, wide), BF16),
            jax.ShapeDtypeStruct((3, tokens, weight.shape[2]), F32),
            jax.ShapeDtypeStruct((rate.shape[0], tokens), F32),
        ],
        scratch_shapes=[
            pltpu.VMEM((tokens, wide), BF16),
            pltpu.VMEM(weight.shape, BF16),
            pltpu.VMEM((tokens, wide), BF16),
            pltpu.VMEM((3, tokens, weight.shape[2]), F32),
            pltpu.SemaphoreType.DMA,
        ] + [sems] * 9,
        compiler_params=pltpu.CompilerParams(collective_id=0, has_side_effects=True, vmem_limit_bytes=56 << 20),
        name="project",
    )(hidden_in, gain.reshape(1, wide), rate, weight)


def middle_kernel(low_ref, wout_ref, gain_ref, own_ref, other_ref, x_ref, wdown_ref, wgu_ref,
                  middle_out, mid_out, normed_out, hidden_out, gate_out, up_out, cot_out, ffn_out,
                  x_full, cot, wdown, wgu, keep, first, got_first, second, got_second, mid, middle, ghid, normed, acts, ffn,
                  load_sem, cot_send, cot_recv, a_send, a_recv, b_send, b_recv, c_send, c_recv, middle_sem, mid_sem, normed_sem, act_sem, cot_sem, ffn_sem):
    me, near, far = partners()
    width = own_ref.shape[1]
    chunks = low_ref.shape[0] // ROWS_PER
    side, spot = lax.rem(me, 2), lax.div(me, 2)
    mine, theirs = part_of(me, width), part_of(far, width)
    loads = [
        pltpu.make_async_copy(own_ref, cot.at[:, mine], load_sem.at[0]),
        pltpu.make_async_copy(other_ref, cot.at[:, theirs], load_sem.at[1]),
        pltpu.make_async_copy(wdown_ref, wdown, load_sem.at[2]),
        pltpu.make_async_copy(x_ref, x_full, load_sem.at[3]),
        pltpu.make_async_copy(wgu_ref, wgu, load_sem.at[4]),
    ]
    for load in loads:
        load.start()
    greet(near, far)

    def send_first(m):
        return push(first.at[band(m)], got_first.at[band(m)], a_send.at[m], a_recv.at[m], near)

    def send_second(m):
        return push(second.at[band(m)], got_second.at[band(m)], b_send.at[m], b_recv.at[m], far)

    def share(m, which):
        at = (mine, theirs)[which]
        return push(mid.at[band(m), at], mid.at[band(m), at], c_send.at[m, which], c_recv.at[m, which], near)

    def out_middle(m):
        return pltpu.make_async_copy(middle.at[band(m)], middle_out.at[band(m)], middle_sem.at[m])

    def out_mid(m):
        return pltpu.make_async_copy(mid.at[band(m)], mid_out.at[band(m)], mid_sem.at[m])

    def out_normed(m):
        slot = lax.rem(m, 2)
        return pltpu.make_async_copy(normed.at[slot], normed_out.at[band(m)], normed_sem.at[slot])

    def out_ffn(m):
        slot = lax.rem(m, 2)
        return pltpu.make_async_copy(ffn.at[slot], ffn_out.at[band(m)], ffn_sem.at[slot])

    def out_act(m, which):
        slot = lax.rem(m, 2)
        return pltpu.make_async_copy(acts.at[slot, which], (hidden_out, gate_out, up_out)[which].at[band(m)], act_sem.at[slot, which])

    def project_out(m):
        rows = low_ref[band(m), :]
        for j in range(2):
            slot = slice(j * width, (j + 1) * width)
            first[band(m), slot] = jnp.dot(rows, wout_ref[:, part_of(2 * j + 1 - side, width)], preferred_element_type=F32).astype(BF16)
        send_first(m).start()
        for j in range(2):
            slot = slice(j * width, (j + 1) * width)
            keep[band(m), slot] = jnp.dot(rows, wout_ref[:, part_of(2 * j + side, width)], preferred_element_type=F32)

    def pair_sum(m):
        send_first(m).wait_recv()
        second[band(m), :] = (keep[band(m), :] + got_first[band(m), :].astype(F32)).astype(BF16)
        send_second(m).start()

    def feed(m):
        pl.when(m < chunks)(lambda: project_out(m))
        pl.when(m > 0)(lambda: pair_sum(m - 1))

    def grad_hidden(m):
        ghid[band(m), :] = lax.dot_general(cot[band(m), :], wdown[...], (((1,), (1,)), ((), ())), preferred_element_type=F32)

    def total(m):
        send_second(m).wait_recv()
        for which, at, slot in ((0, mine, spot), (1, theirs, 1 - spot)):
            piece = part_of(slot, width)
            value = x_full[band(m), at].astype(F32) + (second[band(m), piece].astype(F32) + got_second[band(m), piece].astype(F32))
            if which == 0:
                middle[band(m), :] = value
            mid[band(m), at] = value.astype(BF16)
            share(m, which).start()
        out_middle(m).start()

    def compute(m):
        share(m, 0).wait_recv()
        share(m, 1).wait_recv()
        out_mid(m).start()
        slot = lax.rem(m, 2)

        @pl.when(m >= 2)
        def _():
            out_normed(m - 2).wait()
            out_ffn(m - 2).wait()
            for which in range(3):
                out_act(m - 2, which).wait()

        values = mid[band(m), :].astype(F32)
        low = (values * lax.rsqrt(jnp.mean(values * values, axis=-1, keepdims=True) + EPS) * gain_ref[...]).astype(BF16)
        normed[slot] = low
        out_normed(m).start()
        gate_pre = jnp.dot(low, wgu[0], preferred_element_type=F32)
        up_pre = jnp.dot(low, wgu[1], preferred_element_type=F32)
        gate = jax.nn.sigmoid(gate_pre)
        silu = gate_pre * gate
        grad = ghid[band(m), :]
        acts[slot, 0] = (silu * up_pre).astype(BF16)
        acts[slot, 1] = (grad * up_pre * (gate + silu * (1.0 - gate))).astype(BF16)
        acts[slot, 2] = (grad * silu).astype(BF16)
        for which in range(3):
            out_act(m, which).start()
        ffn[slot] = jnp.dot(acts[slot, 0], wdown[...], preferred_element_type=F32).astype(BF16)
        out_ffn(m).start()

    def both(m):
        pl.when(m < chunks)(lambda: total(m))
        pl.when(m > 0)(lambda: compute(m - 1))

    shares = [push(cot.at[:, at], cot.at[:, at], cot_send.at[i], cot_recv.at[i], near) for i, at in enumerate((mine, theirs))]
    loop(0, chunks + 1, feed)
    loads[0].wait()
    loads[1].wait()
    for copy in shares:
        copy.start()
    loads[2].wait()
    loads[3].wait()
    for copy in shares:
        copy.wait_recv()
    save = pltpu.make_async_copy(cot, cot_out, cot_sem)
    save.start()
    loop(0, chunks, grad_hidden)
    loads[4].wait()
    loop(0, chunks + 1, both)

    def finish(m):
        send_first(m).wait_send()
        send_second(m).wait_send()
        share(m, 0).wait_send()
        share(m, 1).wait_send()
        out_middle(m).wait()
        out_mid(m).wait()

    for m in (chunks - 2, chunks - 1):
        out_normed(m).wait()
        out_ffn(m).wait()
        for which in range(3):
            out_act(m, which).wait()
    for copy in shares:
        copy.wait_send()
    save.wait()
    loop(0, chunks, finish)


def middle_step(out_low, wout, gain, cot_own, cot_far, full_in, wdown, wgu):
    tokens, width = cot_own.shape
    wide, units = wgu.shape[1], wgu.shape[2]
    chunks = tokens // ROWS_PER
    dma = pltpu.SemaphoreType.DMA
    half = (tokens, wide // 2)
    return pl.pallas_call(
        middle_kernel,
        in_specs=[in_vmem(), in_vmem(), in_vmem()] + [in_hbm()] * 5,
        out_specs=[in_hbm()] * 8,
        out_shape=[
            jax.ShapeDtypeStruct((tokens, width), F32),
            jax.ShapeDtypeStruct((tokens, wide), BF16),
            jax.ShapeDtypeStruct((tokens, wide), BF16),
            jax.ShapeDtypeStruct((tokens, units), BF16),
            jax.ShapeDtypeStruct((tokens, units), BF16),
            jax.ShapeDtypeStruct((tokens, units), BF16),
            jax.ShapeDtypeStruct((tokens, wide), BF16),
            jax.ShapeDtypeStruct((tokens, wide), BF16),
        ],
        scratch_shapes=[
            pltpu.VMEM((tokens, wide), BF16),
            pltpu.VMEM((tokens, wide), BF16),
            pltpu.VMEM(wdown.shape, BF16),
            pltpu.VMEM(wgu.shape, BF16),
            pltpu.VMEM(half, F32),
            pltpu.VMEM(half, BF16),
            pltpu.VMEM(half, BF16),
            pltpu.VMEM(half, BF16),
            pltpu.VMEM(half, BF16),
            pltpu.VMEM((tokens, wide), BF16),
            pltpu.VMEM((tokens, width), F32),
            pltpu.VMEM((tokens, units), F32),
            pltpu.VMEM((2, ROWS_PER, wide), BF16),
            pltpu.VMEM((2, 3, ROWS_PER, units), BF16),
            pltpu.VMEM((2, ROWS_PER, wide), BF16),
            dma((5,)), dma((2,)), dma((2,)),
            dma((chunks,)), dma((chunks,)), dma((chunks,)), dma((chunks,)),
            dma((chunks, 2)), dma((chunks, 2)),
            dma((chunks,)), dma((chunks,)), dma((2,)), dma((2, 3)), dma, dma((2,)),
        ],
        compiler_params=pltpu.CompilerParams(collective_id=1, has_side_effects=True, vmem_limit_bytes=62 << 20),
        name="middle_step",
    )(out_low, wout, gain.reshape(1, wide), cot_own, cot_far, full_in, wdown, wgu)


def return_kernel(wout_ref, gain_ref, gate_ref, up_ref, mid_ref, cot_ref, wgu_ref,
                  gmid_out, full_out, nout_out, sum_ref,
                  gate, up, mid, cot, wgu, piece, keep, first, got_first, second, got_second, full, gmid, nout,
                  load_sem, a_send, a_recv, b_send, b_recv, c_send, c_recv, gmid_sem, full_sem, nout_sem):
    me, near, far = partners()
    width = gmid.shape[1]
    chunks = gmid.shape[0] // ROWS_PER
    side, spot = lax.rem(me, 2), lax.div(me, 2)
    mine, theirs = part_of(me, width), part_of(far, width)
    loads = [
        pltpu.make_async_copy(gate_ref, gate, load_sem.at[0]),
        pltpu.make_async_copy(wgu_ref.at[0], wgu.at[0], load_sem.at[1]),
        pltpu.make_async_copy(up_ref, up, load_sem.at[2]),
        pltpu.make_async_copy(wgu_ref.at[1], wgu.at[1], load_sem.at[3]),
        pltpu.make_async_copy(mid_ref, mid, load_sem.at[4]),
        pltpu.make_async_copy(cot_ref, cot, load_sem.at[5]),
    ]
    for load in loads:
        load.start()
    greet(near, far)
    sum_ref[...] = jnp.zeros_like(sum_ref)

    def send_first(m):
        return push(first.at[band(m)], got_first.at[band(m)], a_send.at[m], a_recv.at[m], near)

    def send_second(m):
        return push(second.at[band(m)], got_second.at[band(m)], b_send.at[m], b_recv.at[m], far)

    def share(m, which):
        at = (mine, theirs)[which]
        return push(full.at[band(m), at], full.at[band(m), at], c_send.at[m, which], c_recv.at[m, which], near)

    def outs(m):
        return [
            pltpu.make_async_copy(gmid.at[band(m)], gmid_out.at[band(m)], gmid_sem.at[m]),
            pltpu.make_async_copy(full.at[band(m)], full_out.at[band(m)], full_sem.at[m]),
            pltpu.make_async_copy(nout.at[band(m)], nout_out.at[band(m)], nout_sem.at[m]),
        ]

    def partial(m):
        dims = (((1,), (1,)), ((), ()))
        grad = lax.dot_general(gate[band(m), :], wgu[0], dims, preferred_element_type=F32)
        grad = grad + lax.dot_general(up[band(m), :], wgu[1], dims, preferred_element_type=F32)
        values = mid[band(m), :].astype(F32)
        scale = lax.rsqrt(jnp.mean(values * values, axis=-1, keepdims=True) + EPS)
        unit = values * scale
        sum_ref[...] += jnp.sum(grad * unit, axis=0, keepdims=True)
        scaled = grad * gain_ref[...]
        piece[...] = scale * (scaled - unit * jnp.mean(scaled * unit, axis=-1, keepdims=True))
        for j in range(2):
            slot = slice(j * width, (j + 1) * width)
            first[band(m), slot] = piece[:, part_of(2 * j + 1 - side, width)].astype(BF16)
            keep[band(m), slot] = piece[:, part_of(2 * j + side, width)]
        send_first(m).start()

    def pair_sum(m):
        send_first(m).wait_recv()
        second[band(m), :] = (keep[band(m), :] + got_first[band(m), :].astype(F32)).astype(BF16)
        send_second(m).start()

    def feed(m):
        pl.when(m < chunks)(lambda: partial(m))
        pl.when(m > 0)(lambda: pair_sum(m - 1))

    def total(m):
        send_second(m).wait_recv()
        for which, at, slot in ((0, mine, spot), (1, theirs, 1 - spot)):
            part = part_of(slot, width)
            value = cot[band(m), at].astype(F32) + (second[band(m), part].astype(F32) + got_second[band(m), part].astype(F32))
            if which == 0:
                gmid[band(m), :] = value
            full[band(m), at] = value.astype(BF16)
            share(m, which).start()
        outs(m)[0].start()

    def compute(m):
        share(m, 0).wait_recv()
        share(m, 1).wait_recv()
        outs(m)[1].start()
        nout[band(m), :] = lax.dot_general(full[band(m), :], wout_ref[...], (((1,), (1,)), ((), ())), preferred_element_type=F32)
        outs(m)[2].start()

    def both(m):
        pl.when(m < chunks)(lambda: total(m))
        pl.when(m > 0)(lambda: compute(m - 1))

    def finish(m):
        send_first(m).wait_send()
        send_second(m).wait_send()
        share(m, 0).wait_send()
        share(m, 1).wait_send()
        for copy in outs(m):
            copy.wait()

    for load in loads[:5]:
        load.wait()
    loop(0, chunks + 1, feed)
    loads[5].wait()
    loop(0, chunks + 1, both)
    loop(0, chunks, finish)


def return_step(wout, gain, grad_gate, grad_up, full_mid, full_cot, wgu):
    tokens, wide = full_mid.shape
    units = wgu.shape[2]
    width = wide // 4
    chunks = tokens // ROWS_PER
    dma = pltpu.SemaphoreType.DMA
    half = (tokens, wide // 2)
    return pl.pallas_call(
        return_kernel,
        in_specs=[in_vmem(), in_vmem()] + [in_hbm()] * 5,
        out_specs=[in_hbm()] * 3 + [in_vmem()],
        out_shape=[
            jax.ShapeDtypeStruct((tokens, width), F32),
            jax.ShapeDtypeStruct((tokens, wide), BF16),
            jax.ShapeDtypeStruct((tokens, wout.shape[0]), F32),
            jax.ShapeDtypeStruct((1, wide), F32),
        ],
        scratch_shapes=[
            pltpu.VMEM((tokens, units), BF16),
            pltpu.VMEM((tokens, units), BF16),
            pltpu.VMEM((tokens, wide), BF16),
            pltpu.VMEM((tokens, wide), BF16),
            pltpu.VMEM(wgu.shape, BF16),
            pltpu.VMEM((ROWS_PER, wide), F32),
            pltpu.VMEM(half, F32),
            pltpu.VMEM(half, BF16),
            pltpu.VMEM(half, BF16),
            pltpu.VMEM(half, BF16),
            pltpu.VMEM(half, BF16),
            pltpu.VMEM((tokens, wide), BF16),
            pltpu.VMEM((tokens, width), F32),
            pltpu.VMEM((tokens, wout.shape[0]), F32),
            dma((6,)),
            dma((chunks,)), dma((chunks,)), dma((chunks,)), dma((chunks,)),
            dma((chunks, 2)), dma((chunks, 2)),
            dma((chunks,)), dma((chunks,)), dma((chunks,)),
        ],
        compiler_params=pltpu.CompilerParams(collective_id=2, has_side_effects=True, vmem_limit_bytes=62 << 20),
        name="return_step",
    )(wout, gain.reshape(1, wide), grad_gate, grad_up, full_mid, full_cot, wgu)


ROWS = (((0,), (0,)), ((), ()))


def rms_scale(values):
    return lax.rsqrt(jnp.mean(values * values, axis=-1, keepdims=True) + EPS)


def norm_back(grad_normed, unit_rows, scale_rows, gain):
    scaled_grad = grad_normed * gain
    grad_rows = scale_rows * (scaled_grad - unit_rows * jnp.mean(scaled_grad * unit_rows, axis=-1, keepdims=True))
    return grad_rows, jnp.sum(grad_normed * unit_rows, axis=0)


def butterfly(values, axis, size):
    step = 1
    while step < size:
        pairs = [(i, i ^ step) for i in range(size)]
        values = values + lax.ppermute(values, axis, pairs)
        step *= 2
    return values


def row_major(values):
    return with_layout_constraint(values, Layout(tuple(range(values.ndim))))


def tie(value, token):
    return value if token is None else lax.optimization_barrier((value, token))[0]


class Timeline:
    def __init__(self, size):
        self.size = size
        self.bits = size.bit_length() - 1
        self.token = None
        self.open = {}
        self.later = {}
        self.rider = None
        self.rides = {}

    def after(self, value):
        return tie(value, self.token)

    def swap(self, values, bit):
        return lax.ppermute(values, "dp", [(i, i ^ (1 << bit)) for i in range(self.size)])

    def send(self, away, bit, ride):
        if not ride:
            return self.swap(away, bit)
        flat = away.reshape(-1, away.shape[-1])
        rider = lax.reduce_precision(self.rider, 8, 7)
        self.token = row_major(jnp.concatenate([flat, rider.astype(BF16)]))
        came = self.swap(self.token, bit)
        self.rider = rider + came[flat.shape[0] :].astype(F32)
        return came[: flat.shape[0]].reshape(away.shape)

    def half(self, values, bit, other):
        own = lax.rem(lax.div(lax.axis_index("dp"), 1 << bit), 2)
        side = 1 - own if other else own
        run = values.shape[1] // self.size << bit
        pieces = [lax.dynamic_slice_in_dim(values, (2 * i + side) * run, run, 1) for i in range(self.size // 2 >> bit)]
        return pieces[0] if len(pieces) == 1 else jnp.concatenate(pieces, axis=1)

    def product(self, rows, values):
        grad = lax.dot_general(rows, values, ROWS, preferred_element_type=F32).astype(BF16)
        return row_major(grad).reshape((2,) * (self.bits - 1) + (2 * rows.shape[1] // self.size, values.shape[1]))

    def scatter(self, name, rows, values, bit, ride=False):
        whole = bit == 0 and values.shape[1] * 4 <= rows.shape[1]
        if whole:
            own = lax.rem(lax.div(lax.axis_index("dp"), 1 << bit), 2)
            grad = lax.dot_general(rows, self.after(values), ROWS, preferred_element_type=F32).astype(BF16)
            blocks = row_major(grad).reshape((2,) * self.bits + (rows.shape[1] // self.size, values.shape[1]))
            away = row_major(lax.dynamic_index_in_dim(blocks, 1 - own, self.bits - 1 - bit, keepdims=False))
        else:
            away = self.product(self.half(rows, bit, True), self.after(values))
        self.token = away
        came = self.send(away, bit, ride)
        self.rides[name] = ride
        order = [bit] + [i for i in range(self.bits) if i != bit]
        axes = [i for i in range(self.bits)[::-1] if i != bit]
        self.open[name] = ([came], axes, order, 1)
        if whole:
            self.open[name] = ([lax.dynamic_index_in_dim(blocks, own, self.bits - 1 - bit, keepdims=False), came], axes, order, 1)
        else:
            self.later[name] = (rows, values, bit)

    def keep(self, name):
        rows, values, bit = self.later.pop(name)
        own = self.product(self.half(self.after(rows), bit, False), values)
        self.token = own
        terms, axes, order, stage = self.open[name]
        self.open[name] = ([own] + terms, axes, order, stage)

    def move(self, name):
        if name in self.later:
            self.keep(name)
        terms, axes, order, stage = self.open[name]
        bit = order[stage]
        own = lax.rem(lax.div(lax.axis_index("dp"), 1 << bit), 2)
        axis = axes.index(bit)
        terms = terms[:-1] + [self.after(terms[-1])]

        def pick(value, at):
            return lax.dynamic_index_in_dim(value, at, axis, keepdims=False)

        away = row_major(sum(pick(t, 1 - own).astype(F32) for t in terms).astype(BF16))
        self.token = away
        came = self.send(away, bit, self.rides[name])
        self.open[name] = ([pick(t, own) for t in terms] + [came], axes[:axis] + axes[axis + 1 :], order, stage + 1)

    def close(self, name):
        while self.open[name][3] < self.bits:
            self.move(name)
        terms = self.open.pop(name)[0]
        terms = terms[:-1] + [self.after(terms[-1])]
        return row_major(sum(t.astype(F32) for t in terms))


def make_body(dp_size, tensor_size):
    def body(hidden_in, seg_ids, attn_gain, wqkv, conv_weight, wrate, onorm_gain, wout, mlp_gain, wgu, wdown, cotangent):
        return step(hidden_in, seg_ids, attn_gain, wqkv, conv_weight, wrate, onorm_gain, wout, mlp_gain, wgu, wdown, cotangent)

    def step(hidden_in, seg_ids, attn_gain, wqkv, conv_weight, wrate, onorm_gain, wout, mlp_gain, wgu, wdown, cotangent):
        tokens, width = hidden_in.shape
        heads = wrate.shape[1]
        me = lax.axis_index("tensor")
        side, spot = lax.rem(me, 2), lax.div(me, 2)

        def swap(values, step):
            return lax.ppermute(values, "tensor", [(i, i ^ step) for i in range(tensor_size)])

        def columns(values, q):
            return lax.dynamic_slice_in_dim(values, q * width, width, 1)

        def quarter_sum(pick):
            away = jnp.concatenate([pick(2 * j + 1 - side).astype(BF16) for j in range(2)], axis=1)
            came = swap(away, 1)
            other = (pick(lax.rem(me + 2, 4)) + columns(came, 1 - spot).astype(F32)).astype(BF16)
            far = swap(other, 2)
            return pick(me) + columns(came, spot).astype(F32), far

        taps = conv_weight.astype(F32)
        rates = jnp.zeros((8, wrate.shape[0]), BF16).at[:heads].set(wrate.T)
        full_low, normed_one, proj, logits = project(hidden_in, attn_gain, rates, wqkv)
        cot_own, _ = lax.optimization_barrier((cotangent, logits))
        cot_far = swap(cot_own, 2)
        out_low, *kept = mixer_forward(proj, seg_ids, taps, logits, onorm_gain)
        middle, mid_low, normed_two, hidden, grad_gate, grad_up, full_cot, ffn_part = middle_step(out_low, wout, mlp_gain, cotangent, cot_far, full_low, wdown, wgu)
        line = Timeline(dp_size)
        cut = grad_up.shape[1] // 11 * 4
        line.scatter("down", full_cot, hidden, 0)
        line.scatter("gate", normed_two, grad_gate, 1)
        line.scatter("upx", normed_two, grad_up[:, cut:], 0)
        line.scatter("upz", normed_two, grad_up[:, :cut], 1)
        late_gate = line.after(grad_gate)
        grad_middle, full_grad_mid, grad_nout, gain_two = return_step(wout, mlp_gain, late_gate, grad_up, mid_low, full_cot, wgu)
        line.token = grad_nout
        line.move("down")
        line.scatter("out", full_grad_mid, out_low, 0)
        line.move("gate")
        line.move("upx")
        grad_proj, grad_logits, grad_conv, gain_onorm = mixer_backward(proj, seg_ids, taps, logits, onorm_gain, kept, line.after(grad_nout))
        line.token = grad_logits
        grad_logits = grad_logits.reshape(heads, tokens)
        line.move("down")
        line.move("upz")
        line.scatter("k", normed_one, grad_proj[1], 0)
        late_low, late_proj = line.after((full_low, grad_proj))
        grad_nin = jnp.einsum("ctk,cdk->td", late_proj, wqkv, preferred_element_type=F32)
        grad_nin = grad_nin + jnp.einsum("ht,dh->td", grad_logits, wrate, preferred_element_type=F32)
        full_in = late_low.astype(F32)
        scale_one = rms_scale(full_in)
        part_one, gain_one = norm_back(grad_nin, full_in * scale_one, scale_one, attn_gain)
        part_one = part_one.astype(BF16)
        line.token = (part_one, gain_one)
        wide = gain_one.shape[0]
        gains = butterfly(jnp.concatenate([gain_one, gain_two.reshape(-1), gain_onorm.reshape(-1)]), "tensor", tensor_size)
        shared = gains.shape[0]
        line.move("gate")
        grad_beta = jnp.einsum("td,ht->dh", normed_one, line.after(grad_logits), preferred_element_type=F32)
        line.move("out")
        small = jnp.concatenate([gains, grad_conv.reshape(-1), grad_beta.reshape(-1)])
        lanes = grad_proj.shape[2]
        extra = -small.shape[0] % (16 * lanes)
        line.rider = jnp.pad(small, (0, extra)).reshape(-1, lanes)
        line.scatter("v", normed_one, grad_proj[2], 0, ride=True)
        line.scatter("q", normed_one, grad_proj[0], 0)
        line.move("upx")
        line.move("k")
        line.move("upz")
        line.move("out")
        one, one_far = quarter_sum(lambda q: columns(part_one, q).astype(F32))
        line.move("v")
        late_ffn = line.after(ffn_part)
        ffn, ffn_far = quarter_sum(lambda q: columns(late_ffn, q).astype(F32))
        grad_down = line.close("down").T
        line.token = grad_down
        line.move("k")
        line.move("q")
        line.move("v")
        grad_gate_w = line.close("gate")
        grad_in = (grad_middle + one + line.after(one_far).astype(F32)).astype(BF16)
        line.token = (grad_gate_w, grad_in)
        grad_up_w = jnp.concatenate([line.close("upz"), line.close("upx")], axis=1)
        grad_gate_up = jnp.stack([grad_gate_w, grad_up_w])
        grad_out = line.close("out").T
        layer_out = (middle + ffn + line.after(ffn_far).astype(F32)).astype(BF16)
        line.token = (grad_gate_up, grad_out, layer_out)
        line.move("q")
        grad_k, grad_v = line.close("k"), line.close("v")
        small = line.rider.reshape(-1)
        grad_qkv = jnp.stack([grad_k, grad_k, grad_v])
        line.token = (grad_qkv, small)
        grad_qkv = lax.dynamic_update_slice(grad_qkv, line.close("q")[None], (0, 0, 0))
        gains = small[:shared]
        mine = grad_beta.shape[0] // dp_size
        rest = small[shared + grad_conv.size :]
        grad_conv = small[shared : shared + grad_conv.size].reshape(grad_conv.shape)
        grad_beta = rest[: grad_beta.size].reshape(grad_beta.shape)
        grad_beta = lax.dynamic_slice_in_dim(grad_beta, lax.axis_index("dp") * mine, mine, 0)
        return (
            layer_out,
            grad_in,
            gains[:wide],
            grad_qkv,
            grad_conv,
            grad_beta,
            gains[2 * wide :],
            grad_out,
            gains[wide : 2 * wide],
            grad_gate_up,
            grad_down,
        )

    return body


def solution(mesh):
    return jax.shard_map(
        make_body(mesh.shape["dp"], mesh.shape["tensor"]),
        mesh=mesh,
        in_specs=(
            P("dp", "tensor"),
            P("dp", None),
            P(),
            P(None, None, "tensor"),
            P(None, None, "tensor"),
            P(None, "tensor"),
            P(),
            P("tensor", None),
            P(),
            P(None, None, "tensor"),
            P("tensor", None),
            P("dp", "tensor"),
        ),
        out_specs=(
            P("dp", "tensor"),
            P("dp", "tensor"),
            P(),
            P(None, "dp", "tensor"),
            P(None, None, "tensor"),
            P("dp", "tensor"),
            P(),
            P("tensor", "dp"),
            P(),
            P(None, "dp", "tensor"),
            P("tensor", "dp"),
        ),
        check_vma=False,
    )
```

```python
import jax
import jax.numpy as jnp
from jax import lax
from jax.experimental import pallas as pl
from jax.experimental.pallas import tpu as pltpu
from jax.experimental.layout import Layout, with_layout_constraint
from jax.sharding import PartitionSpec as P

HEAD_DIM = 128
TAPS = 4
CHUNK = 128
HALO = 8
EPS = 1e-06
PAIR = 2
F32 = jnp.float32
BF16 = jnp.bfloat16


def dot_nn(a, b):
    return jnp.dot(a.astype(BF16), b.astype(BF16), preferred_element_type=F32)


def dot_nt(a, b):
    return lax.dot_general(a.astype(BF16), b.astype(BF16), (((1,), (1,)), ((), ())), preferred_element_type=F32)


def dot_tn(a, b):
    return lax.dot_general(a.astype(BF16), b.astype(BF16), (((0,), (0,)), ((), ())), preferred_element_type=F32)


def column(row):
    return jnp.broadcast_to(row, (CHUNK, CHUNK)).T


def logit_row(logit_ref, head, span):
    values = logit_ref[:, span]
    return jnp.sum(jnp.where(lax.broadcasted_iota(jnp.int32, values.shape, 0) == head, values, 0.0), axis=0, keepdims=True)


def load_segments(seg_ref, segcol, length):
    segcol[0:HALO, :] = jnp.full((HALO, CHUNK), -1.0, F32)
    segcol[HALO + length :, :] = jnp.full((HALO, CHUNK), -2.0, F32)
    for n in range(length // CHUNK):
        row = seg_ref[0, :, n * CHUNK : (n + 1) * CHUNK].astype(F32)
        segcol[HALO + n * CHUNK : HALO + (n + 1) * CHUNK, :] = column(row)


def seg_rows(segcol, n, shift):
    base = HALO + n * CHUNK + shift
    return segcol[base : base + CHUNK, :]


def back_masks(segcol, n):
    here = seg_rows(segcol, n, 0)
    return [None] + [(seg_rows(segcol, n, -s) == here).astype(F32) for s in range(1, TAPS)]


def state_masks(seg_ref, segcol, n):
    here = seg_rows(segcol, n, 0)
    row = jnp.broadcast_to(seg_ref[0, :, n * CHUNK : (n + 1) * CHUNK].astype(F32), (CHUNK, CHUNK))
    same = here == row
    before = segcol[HALO + n * CHUNK - 1 : HALO + n * CHUNK, :]
    last = segcol[HALO + (n + 1) * CHUNK - 1 : HALO + (n + 1) * CHUNK, :]
    carry = (here == before).astype(F32)
    tail = (here == last).astype(F32)
    carry_last = (last == before).astype(F32)
    return same, carry, tail, carry_last


def taps_in(proj_ref, c, h, n):
    lanes = slice(h * HEAD_DIM, (h + 1) * HEAD_DIM)
    if n == 0:
        return jnp.concatenate([jnp.zeros((HALO, HEAD_DIM), F32), proj_ref[c, 0:CHUNK, lanes].astype(F32)], axis=0)
    return proj_ref[c, n * CHUNK - HALO : (n + 1) * CHUNK, lanes].astype(F32)


def conv_rows(window, weight_ref, c, h, masks):
    lanes = slice(h * HEAD_DIM, (h + 1) * HEAD_DIM)
    total = weight_ref[c, TAPS - 1 : TAPS, lanes] * window[HALO:]
    for s in range(1, TAPS):
        total = total + weight_ref[c, TAPS - 1 - s : TAPS - s, lanes] * (masks[s] * window[HALO - s : HALO - s + CHUNK])
    return total


def grid_ids():
    rows = lax.broadcasted_iota(jnp.int32, (CHUNK, CHUNK), 0)
    cols = lax.broadcasted_iota(jnp.int32, (CHUNK, CHUNK), 1)
    return rows, cols


def forward_kernel(proj_ref, seg_ref, weight_ref, logit_ref, gain_ref, out_ref, mixed_ref, inv_ref, score_ref, state_ref, delta_ref, err_ref, segcol):
    length = proj_ref.shape[1]
    chunks = length // CHUNK
    load_segments(seg_ref, segcol, length)
    rows, cols = grid_ids()
    apart = rows ^ cols
    lower = rows > cols
    lower_incl = rows >= cols
    scale = HEAD_DIM**-0.5
    pieces, systems, inverses = {}, {}, {}
    for n in range(chunks):
        masks = back_masks(segcol, n)
        same, carry, tail, carry_last = state_masks(seg_ref, segcol, n)
        span = slice(n * CHUNK, (n + 1) * CHUNK)
        for h in range(PAIR):
            acts = []
            for c in range(3):
                conv = conv_rows(taps_in(proj_ref, c, h, n), weight_ref, c, h, masks)
                acts.append(conv * jax.nn.sigmoid(conv))
            q = (acts[0] * lax.rsqrt(jnp.sum(acts[0] * acts[0], axis=-1, keepdims=True) + EPS)).astype(BF16)
            k = (acts[1] * lax.rsqrt(jnp.sum(acts[1] * acts[1], axis=-1, keepdims=True) + EPS)).astype(BF16)
            v = acts[2].astype(BF16).astype(F32)
            rate = jax.nn.sigmoid(column(logit_row(logit_ref, PAIR * pl.program_id(1) + h, span)))
            gram = jnp.where(same & lower, dot_nt(k, k), 0.0)
            scores = (jnp.where(same & lower_incl, dot_nt(q, k), 0.0) * scale).astype(BF16)
            system = rate * gram
            score_ref[h, span, :] = scores
            systems[n, h] = system
            inverses[n, h] = jnp.where(rows == cols, 1.0, 0.0) - jnp.where(apart == 1, system, 0.0)
            pieces[n, h] = (q, k.astype(F32), v, gram, scores, rate, carry, tail, carry_last)
    level = 1
    while (2 << level) <= CHUNK:
        crossed = {}
        for key, inverse in inverses.items():
            crossed[key] = dot_nn(jnp.where((apart >> level) == 1, systems[key], 0.0), inverse)
        for key, inverse in inverses.items():
            inverses[key] = inverse - dot_nn(inverse, crossed[key])
        level += 1
    for n, h in pieces:
        q, kf, v, gram, scores, rate, carry, tail, carry_last = pieces[n, h]
        inverse = inverses[n, h].astype(BF16)
        inv_ref[h, n * CHUNK : (n + 1) * CHUNK, :] = inverse
        base = dot_nn(inverse, rate * v)
        back = dot_nn(inverse, rate * carry * kf)
        pieces[n, h] = (q, kf, v, gram, scores, base, back, carry, tail, carry_last)
    for h in range(PAIR):
        lanes = slice(h * HEAD_DIM, (h + 1) * HEAD_DIM)
        state = None
        for n in range(chunks):
            span = slice(n * CHUNK, (n + 1) * CHUNK)
            q, kf, v, gram, scores, base, back, carry, tail, carry_last = pieces[n, h]
            if n == 0:
                delta = base
                rest = v
                state_ref[h, span, :] = jnp.zeros((CHUNK, CHUNK), BF16)
            else:
                low = state.astype(BF16)
                state_ref[h, span, :] = low
                delta = base - dot_nn(back, low)
                rest = v - carry * dot_nn(kf, low)
            delta_low = delta.astype(BF16)
            moved = dot_tn(tail * kf, delta_low)
            mixed = dot_nn(scores, delta_low)
            if n > 0:
                mixed = mixed + (carry * scale) * dot_nn(q, low)
                moved = moved + carry_last * state
            state = moved
            delta_ref[span, lanes] = delta_low
            err_ref[span, lanes] = (rest - dot_nn(gram, delta_low)).astype(BF16)
            mixed_ref[span, lanes] = mixed
            root = lax.rsqrt(jnp.mean(mixed * mixed, axis=-1, keepdims=True) + EPS)
            out_ref[span, lanes] = (mixed * root * gain_ref[...]).astype(BF16)


def backward_kernel(proj_ref, seg_ref, weight_ref, logit_ref, gain_ref, mixed_ref, inv_ref, score_ref, state_ref, delta_ref, err_ref, nout_ref,
                    gproj_ref, glogit_ref, gconv_ref, gonorm_ref, segcol, gin_ref, act_ref, q_ref, k_ref, head_ref, dq_ref, dk_ref):
    length = proj_ref.shape[1]
    chunks = length // CHUNK
    pair, seq = pl.program_id(0), pl.program_id(1)
    load_segments(seg_ref, segcol, length)
    rows, cols = grid_ids()
    lower = rows > cols
    lower_incl = rows >= cols
    scale = HEAD_DIM**-0.5

    @pl.when((pair == 0) & (seq == 0))
    def _():
        gonorm_ref[...] = jnp.zeros_like(gonorm_ref)

    @pl.when(seq == 0)
    def _():
        gconv_ref[...] = jnp.zeros_like(gconv_ref)

    onorm = jnp.zeros((1, HEAD_DIM), F32)
    pieces = {}
    for n in range(chunks):
        masks = back_masks(segcol, n)
        same, carry, tail, carry_last = state_masks(seg_ref, segcol, n)
        span = slice(n * CHUNK, (n + 1) * CHUNK)
        for h in range(PAIR):
            lanes = slice(h * HEAD_DIM, (h + 1) * HEAD_DIM)
            for c in range(3):
                act_ref[h, c, span, :] = conv_rows(taps_in(proj_ref, c, h, n), weight_ref, c, h, masks)
            conv = act_ref[h, 0, span, :]
            act = conv * jax.nn.sigmoid(conv)
            q = (act * lax.rsqrt(jnp.sum(act * act, axis=-1, keepdims=True) + EPS)).astype(BF16)
            conv = act_ref[h, 1, span, :]
            act = conv * jax.nn.sigmoid(conv)
            k = (act * lax.rsqrt(jnp.sum(act * act, axis=-1, keepdims=True) + EPS)).astype(BF16)
            q_ref[h, span, :] = q
            k_ref[h, span, :] = k
            mixed = mixed_ref[span, lanes]
            root = lax.rsqrt(jnp.mean(mixed * mixed, axis=-1, keepdims=True) + EPS)
            unit = mixed * root
            grad = nout_ref[span, lanes].astype(F32)
            onorm = onorm + jnp.sum(grad * unit, axis=0, keepdims=True)
            scaled = grad * gain_ref[...]
            gmix = root * (scaled - unit * jnp.mean(scaled * unit, axis=-1, keepdims=True))
            glow = gmix.astype(BF16)
            inverse = inv_ref[h, span, :]
            delta = delta_ref[span, lanes]
            gscore = (jnp.where(same & lower_incl, dot_nt(glow, delta), 0.0) * scale).astype(BF16)
            dq = dot_nn(gscore, k)
            held = (scale * carry * gmix).astype(BF16)
            if n > 0:
                dq = dq + dot_nt(held, state_ref[h, span, :])
            dq_ref[h, span, :] = dq
            dk_ref[h, span, :] = dot_tn(gscore, q)
            start = dot_tn(inverse, dot_tn(score_ref[h, span, :], glow))
            kf = k.astype(F32)
            reach = dot_tn(inverse, tail * kf).astype(BF16)
            feed = dot_tn(q, held)
            pieces[n, h] = (start, reach, feed)
    gonorm_ref[...] += onorm
    for h in range(PAIR):
        lanes = slice(h * HEAD_DIM, (h + 1) * HEAD_DIM)
        flow = None
        for n in reversed(range(chunks)):
            span = slice(n * CHUNK, (n + 1) * CHUNK)
            same, carry, tail, carry_last = state_masks(seg_ref, segcol, n)
            rate = jax.nn.sigmoid(column(logit_row(logit_ref, PAIR * pair + h, span)))
            start, reach, feed = pieces[n, h]
            k = k_ref[h, span, :]
            delta = delta_ref[span, lanes]
            gtarget = start
            if flow is not None:
                low = flow.astype(BF16)
                gtarget = gtarget + dot_nn(reach, low)
            gval = rate * gtarget
            head_ref[h, span, :] = gval
            grecall = (carry * gval).astype(BF16)
            dk = dk_ref[h, span, :]
            if flow is not None:
                dk = dk + tail * dot_nt(delta, low)
            if n > 0:
                dk = dk - dot_nt(grecall, state_ref[h, span, :])
                nxt = feed - dot_tn(k, grecall)
                if flow is not None:
                    nxt = nxt + carry_last * flow
                flow = nxt
            ggram = jnp.where(same & lower, dot_nt(gval, delta), 0.0)
            dk_ref[h, span, :] = dk - dot_nn(ggram + ggram.T, k)
            grate = jnp.sum(err_ref[span, lanes].astype(F32) * gtarget, axis=-1, keepdims=True)
            glogit = jnp.broadcast_to(grate, (CHUNK, CHUNK)) * rate * (1.0 - rate)
            glogit_ref[h, :, span] = glogit.T[0:1, :].astype(BF16)
    for h in range(PAIR):
        lanes = slice(h * HEAD_DIM, (h + 1) * HEAD_DIM)
        for c in range(3):
            gin_ref[h, c, length:, :] = jnp.zeros((HALO, HEAD_DIM), F32)
        taps = [[jnp.zeros((1, HEAD_DIM), F32)] * TAPS for _ in range(3)]
        for n in range(chunks):
            masks = back_masks(segcol, n)
            span = slice(n * CHUNK, (n + 1) * CHUNK)
            for c in range(3):
                conv = act_ref[h, c, span, :]
                gate = jax.nn.sigmoid(conv)
                act = conv * gate
                if c == 2:
                    gact = head_ref[h, span, :]
                else:
                    gunit = (dq_ref if c == 0 else dk_ref)[h, span, :]
                    inv = lax.rsqrt(jnp.sum(act * act, axis=-1, keepdims=True) + EPS)
                    unit = act * inv
                    gact = inv * (gunit - unit * jnp.sum(gunit * unit, axis=-1, keepdims=True))
                gin = gact * (gate + act * (1.0 - gate))
                gin_ref[h, c, span, :] = gin
                window = taps_in(proj_ref, c, h, n)
                taps[c][TAPS - 1] = taps[c][TAPS - 1] + jnp.sum(gin * window[HALO:], axis=0, keepdims=True)
                for s in range(1, TAPS):
                    part = jnp.sum(gin * masks[s] * window[HALO - s : HALO - s + CHUNK], axis=0, keepdims=True)
                    taps[c][TAPS - 1 - s] = taps[c][TAPS - 1 - s] + part
        for c in range(3):
            gconv_ref[c, :, lanes] += jnp.concatenate(taps[c], axis=0)
        for n in range(chunks):
            span = slice(n * CHUNK, (n + 1) * CHUNK)
            here = seg_rows(segcol, n, 0)
            ahead = [None] + [(seg_rows(segcol, n, s) == here).astype(F32) for s in range(1, TAPS)]
            for c in range(3):
                total = weight_ref[c, TAPS - 1 : TAPS, lanes] * gin_ref[h, c, span, :]
                for s in range(1, TAPS):
                    later = gin_ref[h, c, n * CHUNK + s : (n + 1) * CHUNK + s, :]
                    total = total + weight_ref[c, TAPS - 1 - s : TAPS - s, lanes] * (ahead[s] * later)
                gproj_ref[c, span, lanes] = total.astype(BF16)


def mixer_shapes(proj, seg):
    seqs, length = seg.shape
    return seqs, length, proj.shape[2] // HEAD_DIM


def mixer_forward(proj, seg, weight, logits, gain):
    seqs, length, heads = mixer_shapes(proj, seg)
    tokens = seqs * length
    wide = PAIR * HEAD_DIM
    flat = pl.BlockSpec((length, wide), lambda s, p: (s, p))
    square = pl.BlockSpec((PAIR, length, CHUNK), lambda s, p: (p, s, 0))
    return pl.pallas_call(
        forward_kernel,
        grid=(seqs, heads // PAIR),
        in_specs=[
            pl.BlockSpec((3, length, wide), lambda s, p: (0, s, p)),
            pl.BlockSpec((1, 1, length), lambda s, p: (s, 0, 0)),
            pl.BlockSpec((3, TAPS, wide), lambda s, p: (0, 0, p)),
            pl.BlockSpec((logits.shape[0], length), lambda s, p: (0, s)),
            pl.BlockSpec((1, HEAD_DIM), lambda s, p: (0, 0)),
        ],
        out_specs=[flat, flat, square, square, square, flat, flat],
        out_shape=[
            jax.ShapeDtypeStruct((tokens, heads * HEAD_DIM), BF16),
            jax.ShapeDtypeStruct((tokens, heads * HEAD_DIM), F32),
            jax.ShapeDtypeStruct((heads, tokens, CHUNK), BF16),
            jax.ShapeDtypeStruct((heads, tokens, CHUNK), BF16),
            jax.ShapeDtypeStruct((heads, tokens, CHUNK), BF16),
            jax.ShapeDtypeStruct((tokens, heads * HEAD_DIM), BF16),
            jax.ShapeDtypeStruct((tokens, heads * HEAD_DIM), BF16),
        ],
        scratch_shapes=[pltpu.VMEM((length + 2 * HALO, CHUNK), F32)],
        compiler_params=pltpu.CompilerParams(vmem_limit_bytes=62 << 20),
        name="mixer_forward",
    )(proj, seg.reshape(seqs, 1, length), weight, logits, gain.reshape(1, HEAD_DIM))


def mixer_backward(proj, seg, weight, logits, gain, kept, grad_nout):
    seqs, length, heads = mixer_shapes(proj, seg)
    tokens = seqs * length
    wide = PAIR * HEAD_DIM
    mixed, inverse, scores, states, delta, err = kept
    flat = pl.BlockSpec((length, wide), lambda p, s: (s, p))
    square = pl.BlockSpec((PAIR, length, CHUNK), lambda p, s: (p, s, 0))
    cube = pl.BlockSpec((3, length, wide), lambda p, s: (0, s, p))
    taps = pl.BlockSpec((3, TAPS, wide), lambda p, s: (0, 0, p))
    line = pl.BlockSpec((PAIR, 1, length), lambda p, s: (p, 0, s))
    vector = pl.BlockSpec((1, HEAD_DIM), lambda p, s: (0, 0))
    return pl.pallas_call(
        backward_kernel,
        grid=(heads // PAIR, seqs),
        in_specs=[cube, pl.BlockSpec((1, 1, length), lambda p, s: (s, 0, 0)), taps, pl.BlockSpec((logits.shape[0], length), lambda p, s: (0, s)), vector, flat, square, square, square, flat, flat, flat],
        out_specs=[cube, line, taps, vector],
        out_shape=[
            jax.ShapeDtypeStruct(proj.shape, BF16),
            jax.ShapeDtypeStruct((heads, 1, tokens), BF16),
            jax.ShapeDtypeStruct(weight.shape, F32),
            jax.ShapeDtypeStruct((1, HEAD_DIM), F32),
        ],
        scratch_shapes=[
            pltpu.VMEM((length + 2 * HALO, CHUNK), F32),
            pltpu.VMEM((PAIR, 3, length + HALO, HEAD_DIM), F32),
            pltpu.VMEM((PAIR, 3, length, HEAD_DIM), F32),
            pltpu.VMEM((PAIR, length, HEAD_DIM), BF16),
            pltpu.VMEM((PAIR, length, HEAD_DIM), BF16),
            pltpu.VMEM((PAIR, length, HEAD_DIM), F32),
            pltpu.VMEM((PAIR, length, HEAD_DIM), F32),
            pltpu.VMEM((PAIR, length, HEAD_DIM), F32),
        ],
        compiler_params=pltpu.CompilerParams(vmem_limit_bytes=62 << 20),
        name="mixer_backward",
    )(proj, seg.reshape(seqs, 1, length), weight, logits, gain.reshape(1, HEAD_DIM), mixed, inverse, scores, states, delta, err, grad_nout)


MESH = pl.DeviceIdType.MESH
ROWS_PER = 128


def partners():
    me = lax.axis_index("tensor")
    near = me + 1 - 2 * lax.rem(me, 2)
    far = lax.rem(me + 2, 4)
    return me, near, far


def greet(near, far):
    barrier = pltpu.get_barrier_semaphore()
    for other in (near, far):
        pl.semaphore_signal(barrier, inc=1, device_id={"tensor": other}, device_id_type=MESH)
    pl.semaphore_wait(barrier, 2)


def push(src, dst, send, recv, other):
    return pltpu.make_async_remote_copy(src_ref=src, dst_ref=dst, send_sem=send, recv_sem=recv, device_id={"tensor": other}, device_id_type=MESH)


def band(m):
    return pl.ds(pl.multiple_of(m * ROWS_PER, ROWS_PER), ROWS_PER)


def part_of(q, width):
    return pl.ds(pl.multiple_of(q * width, width), width)


def loop(start, stop, body):
    lax.fori_loop(start, stop, lambda m, carry: (body(m), carry)[1], 0)


def project_kernel(x_ref, gain_ref, rate_ref, weight_ref, full_out, normed_out, proj_out, logit_ref,
                   full, weight, normed, proj, weight_sem, far_send, far_recv, near_send, near_recv, pass_send, pass_recv, full_sem, normed_sem, proj_sem):
    me, near, far = partners()
    width = x_ref.shape[1]
    chunks = x_ref.shape[0] // ROWS_PER
    mine, theirs = part_of(me, width), part_of(far, width)
    load = pltpu.make_async_copy(weight_ref, weight, weight_sem)
    load.start()
    greet(near, far)

    def to_far(m):
        return push(x_ref.at[band(m)], full.at[band(m), mine], far_send.at[m], far_recv.at[m], far)

    def to_near(m):
        return push(x_ref.at[band(m)], full.at[band(m), mine], near_send.at[m], near_recv.at[m], near)

    def onward(m):
        return push(full.at[band(m), theirs], full.at[band(m), theirs], pass_send.at[m], pass_recv.at[m], near)

    def out_full(m):
        return pltpu.make_async_copy(full.at[band(m)], full_out.at[band(m)], full_sem.at[m])

    def out_normed(m):
        return pltpu.make_async_copy(normed.at[band(m)], normed_out.at[band(m)], normed_sem.at[m])

    def out_proj(m):
        return pltpu.make_async_copy(proj.at[:, band(m)], proj_out.at[:, band(m)], proj_sem.at[m])

    def begin(m):
        to_far(m).start()
        to_near(m).start()
        full[band(m), mine] = x_ref[band(m), :]

    def compute(m):
        to_near(m).wait_recv()
        onward(m).wait_recv()
        values = full[band(m), :].astype(F32)
        low = (values * lax.rsqrt(jnp.mean(values * values, axis=-1, keepdims=True) + EPS) * gain_ref[...]).astype(BF16)
        normed[band(m), :] = low
        for c in range(3):
            proj[c, band(m), :] = jnp.dot(low, weight[c], preferred_element_type=F32)
        logit_ref[:, band(m)] = lax.dot_general(rate_ref[...], low, (((1,), (1,)), ((), ())), preferred_element_type=F32)
        out_full(m).start()
        out_normed(m).start()
        out_proj(m).start()

    def relay(m):
        to_far(m).wait_recv()
        onward(m).start()

    def both(m):
        pl.when(m < chunks)(lambda: relay(m))
        pl.when(m > 0)(lambda: compute(m - 1))

    def finish(m):
        to_far(m).wait_send()
        to_near(m).wait_send()
        onward(m).wait_send()
        out_full(m).wait()
        out_normed(m).wait()
        out_proj(m).wait()

    loop(0, chunks, begin)
    load.wait()
    loop(0, chunks + 1, both)
    loop(0, chunks, finish)


def in_vmem():
    return pl.BlockSpec(memory_space=pltpu.VMEM)


def in_hbm():
    return pl.BlockSpec(memory_space=pl.ANY)


def project(hidden_in, gain, rate, weight):
    tokens, _ = hidden_in.shape
    wide = weight.shape[1]
    chunks = tokens // ROWS_PER
    sems = pltpu.SemaphoreType.DMA((chunks,))
    return pl.pallas_call(
        project_kernel,
        in_specs=[in_vmem(), in_vmem(), in_vmem(), in_hbm()],
        out_specs=[in_hbm(), in_hbm(), in_hbm(), in_vmem()],
        out_shape=[
            jax.ShapeDtypeStruct((tokens, wide), BF16),
            jax.ShapeDtypeStruct((tokens, wide), BF16),
            jax.ShapeDtypeStruct((3, tokens, weight.shape[2]), F32),
            jax.ShapeDtypeStruct((rate.shape[0], tokens), F32),
        ],
        scratch_shapes=[
            pltpu.VMEM((tokens, wide), BF16),
            pltpu.VMEM(weight.shape, BF16),
            pltpu.VMEM((tokens, wide), BF16),
            pltpu.VMEM((3, tokens, weight.shape[2]), F32),
            pltpu.SemaphoreType.DMA,
        ] + [sems] * 9,
        compiler_params=pltpu.CompilerParams(collective_id=0, has_side_effects=True, vmem_limit_bytes=56 << 20),
        name="project",
    )(hidden_in, gain.reshape(1, wide), rate, weight)


def middle_kernel(low_ref, wout_ref, gain_ref, own_ref, other_ref, x_ref, wdown_ref, wgu_ref,
                  middle_out, mid_out, normed_out, hidden_out, gate_out, up_out, cot_out, ffn_out,
                  x_full, cot, wdown, wgu, keep, first, got_first, second, got_second, mid, middle, ghid, normed, acts, ffn,
                  load_sem, cot_send, cot_recv, a_send, a_recv, b_send, b_recv, c_send, c_recv, middle_sem, mid_sem, normed_sem, act_sem, cot_sem, ffn_sem):
    me, near, far = partners()
    width = own_ref.shape[1]
    chunks = low_ref.shape[0] // ROWS_PER
    side, spot = lax.rem(me, 2), lax.div(me, 2)
    mine, theirs = part_of(me, width), part_of(far, width)
    loads = [
        pltpu.make_async_copy(own_ref, cot.at[:, mine], load_sem.at[0]),
        pltpu.make_async_copy(other_ref, cot.at[:, theirs], load_sem.at[1]),
        pltpu.make_async_copy(wdown_ref, wdown, load_sem.at[2]),
        pltpu.make_async_copy(x_ref, x_full, load_sem.at[3]),
        pltpu.make_async_copy(wgu_ref, wgu, load_sem.at[4]),
    ]
    for load in loads:
        load.start()
    greet(near, far)

    def send_first(m):
        return push(first.at[band(m)], got_first.at[band(m)], a_send.at[m], a_recv.at[m], near)

    def send_second(m):
        return push(second.at[band(m)], got_second.at[band(m)], b_send.at[m], b_recv.at[m], far)

    def share(m, which):
        at = (mine, theirs)[which]
        return push(mid.at[band(m), at], mid.at[band(m), at], c_send.at[m, which], c_recv.at[m, which], near)

    def out_middle(m):
        return pltpu.make_async_copy(middle.at[band(m)], middle_out.at[band(m)], middle_sem.at[m])

    def out_mid(m):
        return pltpu.make_async_copy(mid.at[band(m)], mid_out.at[band(m)], mid_sem.at[m])

    def out_normed(m):
        slot = lax.rem(m, 2)
        return pltpu.make_async_copy(normed.at[slot], normed_out.at[band(m)], normed_sem.at[slot])

    def out_ffn(m):
        slot = lax.rem(m, 2)
        return pltpu.make_async_copy(ffn.at[slot], ffn_out.at[band(m)], ffn_sem.at[slot])

    def out_act(m, which):
        slot = lax.rem(m, 2)
        return pltpu.make_async_copy(acts.at[slot, which], (hidden_out, gate_out, up_out)[which].at[band(m)], act_sem.at[slot, which])

    def project_out(m):
        rows = low_ref[band(m), :]
        for j in range(2):
            slot = slice(j * width, (j + 1) * width)
            first[band(m), slot] = jnp.dot(rows, wout_ref[:, part_of(2 * j + 1 - side, width)], preferred_element_type=F32).astype(BF16)
        send_first(m).start()
        for j in range(2):
            slot = slice(j * width, (j + 1) * width)
            keep[band(m), slot] = jnp.dot(rows, wout_ref[:, part_of(2 * j + side, width)], preferred_element_type=F32)

    def pair_sum(m):
        send_first(m).wait_recv()
        second[band(m), :] = (keep[band(m), :] + got_first[band(m), :].astype(F32)).astype(BF16)
        send_second(m).start()

    def feed(m):
        pl.when(m < chunks)(lambda: project_out(m))
        pl.when(m > 0)(lambda: pair_sum(m - 1))

    def grad_hidden(m):
        ghid[band(m), :] = lax.dot_general(cot[band(m), :], wdown[...], (((1,), (1,)), ((), ())), preferred_element_type=F32)

    def total(m):
        send_second(m).wait_recv()
        for which, at, slot in ((0, mine, spot), (1, theirs, 1 - spot)):
            piece = part_of(slot, width)
            value = x_full[band(m), at].astype(F32) + (second[band(m), piece].astype(F32) + got_second[band(m), piece].astype(F32))
            if which == 0:
                middle[band(m), :] = value
            mid[band(m), at] = value.astype(BF16)
            share(m, which).start()
        out_middle(m).start()

    def compute(m):
        share(m, 0).wait_recv()
        share(m, 1).wait_recv()
        out_mid(m).start()
        slot = lax.rem(m, 2)

        @pl.when(m >= 2)
        def _():
            out_normed(m - 2).wait()
            out_ffn(m - 2).wait()
            for which in range(3):
                out_act(m - 2, which).wait()

        values = mid[band(m), :].astype(F32)
        low = (values * lax.rsqrt(jnp.mean(values * values, axis=-1, keepdims=True) + EPS) * gain_ref[...]).astype(BF16)
        normed[slot] = low
        out_normed(m).start()
        gate_pre = jnp.dot(low, wgu[0], preferred_element_type=F32)
        up_pre = jnp.dot(low, wgu[1], preferred_element_type=F32)
        gate = jax.nn.sigmoid(gate_pre)
        silu = gate_pre * gate
        grad = ghid[band(m), :]
        acts[slot, 0] = (silu * up_pre).astype(BF16)
        acts[slot, 1] = (grad * up_pre * (gate + silu * (1.0 - gate))).astype(BF16)
        acts[slot, 2] = (grad * silu).astype(BF16)
        for which in range(3):
            out_act(m, which).start()
        ffn[slot] = jnp.dot(acts[slot, 0], wdown[...], preferred_element_type=F32).astype(BF16)
        out_ffn(m).start()

    def both(m):
        pl.when(m < chunks)(lambda: total(m))
        pl.when(m > 0)(lambda: compute(m - 1))

    shares = [push(cot.at[:, at], cot.at[:, at], cot_send.at[i], cot_recv.at[i], near) for i, at in enumerate((mine, theirs))]
    loop(0, chunks + 1, feed)
    loads[0].wait()
    loads[1].wait()
    for copy in shares:
        copy.start()
    loads[2].wait()
    loads[3].wait()
    for copy in shares:
        copy.wait_recv()
    save = pltpu.make_async_copy(cot, cot_out, cot_sem)
    save.start()
    loop(0, chunks, grad_hidden)
    loads[4].wait()
    loop(0, chunks + 1, both)

    def finish(m):
        send_first(m).wait_send()
        send_second(m).wait_send()
        share(m, 0).wait_send()
        share(m, 1).wait_send()
        out_middle(m).wait()
        out_mid(m).wait()

    for m in (chunks - 2, chunks - 1):
        out_normed(m).wait()
        out_ffn(m).wait()
        for which in range(3):
            out_act(m, which).wait()
    for copy in shares:
        copy.wait_send()
    save.wait()
    loop(0, chunks, finish)


def middle_step(out_low, wout, gain, cot_own, cot_far, full_in, wdown, wgu):
    tokens, width = cot_own.shape
    wide, units = wgu.shape[1], wgu.shape[2]
    chunks = tokens // ROWS_PER
    dma = pltpu.SemaphoreType.DMA
    half = (tokens, wide // 2)
    return pl.pallas_call(
        middle_kernel,
        in_specs=[in_vmem(), in_vmem(), in_vmem()] + [in_hbm()] * 5,
        out_specs=[in_hbm()] * 8,
        out_shape=[
            jax.ShapeDtypeStruct((tokens, width), F32),
            jax.ShapeDtypeStruct((tokens, wide), BF16),
            jax.ShapeDtypeStruct((tokens, wide), BF16),
            jax.ShapeDtypeStruct((tokens, units), BF16),
            jax.ShapeDtypeStruct((tokens, units), BF16),
            jax.ShapeDtypeStruct((tokens, units), BF16),
            jax.ShapeDtypeStruct((tokens, wide), BF16),
            jax.ShapeDtypeStruct((tokens, wide), BF16),
        ],
        scratch_shapes=[
            pltpu.VMEM((tokens, wide), BF16),
            pltpu.VMEM((tokens, wide), BF16),
            pltpu.VMEM(wdown.shape, BF16),
            pltpu.VMEM(wgu.shape, BF16),
            pltpu.VMEM(half, F32),
            pltpu.VMEM(half, BF16),
            pltpu.VMEM(half, BF16),
            pltpu.VMEM(half, BF16),
            pltpu.VMEM(half, BF16),
            pltpu.VMEM((tokens, wide), BF16),
            pltpu.VMEM((tokens, width), F32),
            pltpu.VMEM((tokens, units), F32),
            pltpu.VMEM((2, ROWS_PER, wide), BF16),
            pltpu.VMEM((2, 3, ROWS_PER, units), BF16),
            pltpu.VMEM((2, ROWS_PER, wide), BF16),
            dma((5,)), dma((2,)), dma((2,)),
            dma((chunks,)), dma((chunks,)), dma((chunks,)), dma((chunks,)),
            dma((chunks, 2)), dma((chunks, 2)),
            dma((chunks,)), dma((chunks,)), dma((2,)), dma((2, 3)), dma, dma((2,)),
        ],
        compiler_params=pltpu.CompilerParams(collective_id=1, has_side_effects=True, vmem_limit_bytes=62 << 20),
        name="middle_step",
    )(out_low, wout, gain.reshape(1, wide), cot_own, cot_far, full_in, wdown, wgu)


def return_kernel(wout_ref, gain_ref, gate_ref, up_ref, mid_ref, cot_ref, wgu_ref,
                  gmid_out, full_out, nout_out, sum_ref,
                  gate, up, mid, cot, wgu, piece, keep, first, got_first, second, got_second, full, gmid, nout,
                  load_sem, a_send, a_recv, b_send, b_recv, c_send, c_recv, gmid_sem, full_sem, nout_sem):
    me, near, far = partners()
    width = gmid.shape[1]
    chunks = gmid.shape[0] // ROWS_PER
    side, spot = lax.rem(me, 2), lax.div(me, 2)
    mine, theirs = part_of(me, width), part_of(far, width)
    loads = [
        pltpu.make_async_copy(gate_ref, gate, load_sem.at[0]),
        pltpu.make_async_copy(wgu_ref.at[0], wgu.at[0], load_sem.at[1]),
        pltpu.make_async_copy(up_ref, up, load_sem.at[2]),
        pltpu.make_async_copy(wgu_ref.at[1], wgu.at[1], load_sem.at[3]),
        pltpu.make_async_copy(mid_ref, mid, load_sem.at[4]),
        pltpu.make_async_copy(cot_ref, cot, load_sem.at[5]),
    ]
    for load in loads:
        load.start()
    greet(near, far)
    sum_ref[...] = jnp.zeros_like(sum_ref)

    def send_first(m):
        return push(first.at[band(m)], got_first.at[band(m)], a_send.at[m], a_recv.at[m], near)

    def send_second(m):
        return push(second.at[band(m)], got_second.at[band(m)], b_send.at[m], b_recv.at[m], far)

    def share(m, which):
        at = (mine, theirs)[which]
        return push(full.at[band(m), at], full.at[band(m), at], c_send.at[m, which], c_recv.at[m, which], near)

    def outs(m):
        return [
            pltpu.make_async_copy(gmid.at[band(m)], gmid_out.at[band(m)], gmid_sem.at[m]),
            pltpu.make_async_copy(full.at[band(m)], full_out.at[band(m)], full_sem.at[m]),
            pltpu.make_async_copy(nout.at[band(m)], nout_out.at[band(m)], nout_sem.at[m]),
        ]

    def partial(m):
        dims = (((1,), (1,)), ((), ()))

        @pl.when(m == 0)
        def _():
            loads[0].wait()
            loads[1].wait()

        piece[...] = lax.dot_general(gate[band(m), :], wgu[0], dims, preferred_element_type=F32)

        @pl.when(m == 0)
        def _():
            for load in loads[2:5]:
                load.wait()

        grad = piece[...] + lax.dot_general(up[band(m), :], wgu[1], dims, preferred_element_type=F32)
        values = mid[band(m), :].astype(F32)
        scale = lax.rsqrt(jnp.mean(values * values, axis=-1, keepdims=True) + EPS)
        unit = values * scale
        sum_ref[...] += jnp.sum(grad * unit, axis=0, keepdims=True)
        scaled = grad * gain_ref[...]
        piece[...] = scale * (scaled - unit * jnp.mean(scaled * unit, axis=-1, keepdims=True))
        for j in range(2):
            slot = slice(j * width, (j + 1) * width)
            first[band(m), slot] = piece[:, part_of(2 * j + 1 - side, width)].astype(BF16)
            keep[band(m), slot] = piece[:, part_of(2 * j + side, width)]
        send_first(m).start()

    def pair_sum(m):
        send_first(m).wait_recv()
        second[band(m), :] = (keep[band(m), :] + got_first[band(m), :].astype(F32)).astype(BF16)
        send_second(m).start()

    def feed(m):
        pl.when(m < chunks)(lambda: partial(m))
        pl.when(m > 0)(lambda: pair_sum(m - 1))

    def total(m):
        send_second(m).wait_recv()
        for which, at, slot in ((0, mine, spot), (1, theirs, 1 - spot)):
            part = part_of(slot, width)
            value = cot[band(m), at].astype(F32) + (second[band(m), part].astype(F32) + got_second[band(m), part].astype(F32))
            if which == 0:
                gmid[band(m), :] = value
            full[band(m), at] = value.astype(BF16)
            share(m, which).start()
        outs(m)[0].start()

    def compute(m):
        share(m, 0).wait_recv()
        share(m, 1).wait_recv()
        outs(m)[1].start()
        nout[band(m), :] = lax.dot_general(full[band(m), :], wout_ref[...], (((1,), (1,)), ((), ())), preferred_element_type=F32)
        outs(m)[2].start()

    def both(m):
        pl.when(m < chunks)(lambda: total(m))
        pl.when(m > 0)(lambda: compute(m - 1))

    def finish(m):
        send_first(m).wait_send()
        send_second(m).wait_send()
        share(m, 0).wait_send()
        share(m, 1).wait_send()
        for copy in outs(m):
            copy.wait()

    loop(0, chunks + 1, feed)
    loads[5].wait()
    loop(0, chunks + 1, both)
    loop(0, chunks, finish)


def return_step(wout, gain, grad_gate, grad_up, full_mid, full_cot, wgu):
    tokens, wide = full_mid.shape
    units = wgu.shape[2]
    width = wide // 4
    chunks = tokens // ROWS_PER
    dma = pltpu.SemaphoreType.DMA
    half = (tokens, wide // 2)
    return pl.pallas_call(
        return_kernel,
        in_specs=[in_vmem(), in_vmem()] + [in_hbm()] * 5,
        out_specs=[in_hbm()] * 3 + [in_vmem()],
        out_shape=[
            jax.ShapeDtypeStruct((tokens, width), F32),
            jax.ShapeDtypeStruct((tokens, wide), BF16),
            jax.ShapeDtypeStruct((tokens, wout.shape[0]), F32),
            jax.ShapeDtypeStruct((1, wide), F32),
        ],
        scratch_shapes=[
            pltpu.VMEM((tokens, units), BF16),
            pltpu.VMEM((tokens, units), BF16),
            pltpu.VMEM((tokens, wide), BF16),
            pltpu.VMEM((tokens, wide), BF16),
            pltpu.VMEM(wgu.shape, BF16),
            pltpu.VMEM((ROWS_PER, wide), F32),
            pltpu.VMEM(half, F32),
            pltpu.VMEM(half, BF16),
            pltpu.VMEM(half, BF16),
            pltpu.VMEM(half, BF16),
            pltpu.VMEM(half, BF16),
            pltpu.VMEM((tokens, wide), BF16),
            pltpu.VMEM((tokens, width), F32),
            pltpu.VMEM((tokens, wout.shape[0]), F32),
            dma((6,)),
            dma((chunks,)), dma((chunks,)), dma((chunks,)), dma((chunks,)),
            dma((chunks, 2)), dma((chunks, 2)),
            dma((chunks,)), dma((chunks,)), dma((chunks,)),
        ],
        compiler_params=pltpu.CompilerParams(collective_id=2, has_side_effects=True, vmem_limit_bytes=62 << 20),
        name="return_step",
    )(wout, gain.reshape(1, wide), grad_gate, grad_up, full_mid, full_cot, wgu)


ROWS = (((0,), (0,)), ((), ()))


def rms_scale(values):
    return lax.rsqrt(jnp.mean(values * values, axis=-1, keepdims=True) + EPS)


def norm_back(grad_normed, unit_rows, scale_rows, gain):
    scaled_grad = grad_normed * gain
    grad_rows = scale_rows * (scaled_grad - unit_rows * jnp.mean(scaled_grad * unit_rows, axis=-1, keepdims=True))
    return grad_rows, jnp.sum(grad_normed * unit_rows, axis=0)


def butterfly(values, axis, size):
    step = 1
    while step < size:
        pairs = [(i, i ^ step) for i in range(size)]
        values = values + lax.ppermute(values, axis, pairs)
        step *= 2
    return values


def row_major(values):
    return with_layout_constraint(values, Layout(tuple(range(values.ndim))))


def tie(value, token):
    return value if token is None else lax.optimization_barrier((value, token))[0]


class Timeline:
    def __init__(self, size):
        self.size = size
        self.bits = size.bit_length() - 1
        self.token = None
        self.open = {}
        self.later = {}
        self.rider = None
        self.rides = {}

    def after(self, value):
        return tie(value, self.token)

    def swap(self, values, bit):
        return lax.ppermute(values, "dp", [(i, i ^ (1 << bit)) for i in range(self.size)])

    def send(self, away, bit, ride):
        if not ride:
            return self.swap(away, bit)
        flat = away.reshape(-1, away.shape[-1])
        rider = lax.reduce_precision(self.rider, 8, 7)
        self.token = row_major(jnp.concatenate([flat, rider.astype(BF16)]))
        came = self.swap(self.token, bit)
        self.rider = rider + came[flat.shape[0] :].astype(F32)
        return came[: flat.shape[0]].reshape(away.shape)

    def half(self, values, bit, other):
        own = lax.rem(lax.div(lax.axis_index("dp"), 1 << bit), 2)
        side = 1 - own if other else own
        run = values.shape[1] // self.size << bit
        pieces = [lax.dynamic_slice_in_dim(values, (2 * i + side) * run, run, 1) for i in range(self.size // 2 >> bit)]
        return pieces[0] if len(pieces) == 1 else jnp.concatenate(pieces, axis=1)

    def product(self, rows, values):
        grad = lax.dot_general(rows, values, ROWS, preferred_element_type=F32).astype(BF16)
        return row_major(grad).reshape((2,) * (self.bits - 1) + (2 * rows.shape[1] // self.size, values.shape[1]))

    def scatter(self, name, rows, values, bit, ride=False):
        whole = bit == 0 and values.shape[1] * 4 <= rows.shape[1]
        if whole:
            own = lax.rem(lax.div(lax.axis_index("dp"), 1 << bit), 2)
            grad = lax.dot_general(rows, self.after(values), ROWS, preferred_element_type=F32).astype(BF16)
            blocks = row_major(grad).reshape((2,) * self.bits + (rows.shape[1] // self.size, values.shape[1]))
            away = row_major(lax.dynamic_index_in_dim(blocks, 1 - own, self.bits - 1 - bit, keepdims=False))
        else:
            away = self.product(self.half(rows, bit, True), self.after(values))
        self.token = away
        came = self.send(away, bit, ride)
        self.rides[name] = ride
        order = [bit] + [i for i in range(self.bits) if i != bit]
        axes = [i for i in range(self.bits)[::-1] if i != bit]
        self.open[name] = ([came], axes, order, 1)
        if whole:
            self.open[name] = ([lax.dynamic_index_in_dim(blocks, own, self.bits - 1 - bit, keepdims=False), came], axes, order, 1)
        else:
            self.later[name] = (rows, values, bit)

    def keep(self, name):
        rows, values, bit = self.later.pop(name)
        own = self.product(self.half(self.after(rows), bit, False), values)
        self.token = own
        terms, axes, order, stage = self.open[name]
        self.open[name] = ([own] + terms, axes, order, stage)

    def move(self, name):
        if name in self.later:
            self.keep(name)
        terms, axes, order, stage = self.open[name]
        bit = order[stage]
        own = lax.rem(lax.div(lax.axis_index("dp"), 1 << bit), 2)
        axis = axes.index(bit)
        terms = terms[:-1] + [self.after(terms[-1])]

        def pick(value, at):
            return lax.dynamic_index_in_dim(value, at, axis, keepdims=False)

        away = row_major(sum(pick(t, 1 - own).astype(F32) for t in terms).astype(BF16))
        self.token = away
        came = self.send(away, bit, self.rides[name])
        self.open[name] = ([pick(t, own) for t in terms] + [came], axes[:axis] + axes[axis + 1 :], order, stage + 1)

    def close(self, name):
        while self.open[name][3] < self.bits:
            self.move(name)
        terms = self.open.pop(name)[0]
        terms = terms[:-1] + [self.after(terms[-1])]
        return row_major(sum(t.astype(F32) for t in terms))


def make_body(dp_size, tensor_size):
    def body(hidden_in, seg_ids, attn_gain, wqkv, conv_weight, wrate, onorm_gain, wout, mlp_gain, wgu, wdown, cotangent):
        return step(hidden_in, seg_ids, attn_gain, wqkv, conv_weight, wrate, onorm_gain, wout, mlp_gain, wgu, wdown, cotangent)

    def step(hidden_in, seg_ids, attn_gain, wqkv, conv_weight, wrate, onorm_gain, wout, mlp_gain, wgu, wdown, cotangent):
        tokens, width = hidden_in.shape
        heads = wrate.shape[1]
        me = lax.axis_index("tensor")
        side, spot = lax.rem(me, 2), lax.div(me, 2)

        def swap(values, step):
            return lax.ppermute(values, "tensor", [(i, i ^ step) for i in range(tensor_size)])

        def columns(values, q):
            return lax.dynamic_slice_in_dim(values, q * width, width, 1)

        def quarter_sum(pick):
            away = jnp.concatenate([pick(2 * j + 1 - side).astype(BF16) for j in range(2)], axis=1)
            came = swap(away, 1)
            other = (pick(lax.rem(me + 2, 4)) + columns(came, 1 - spot).astype(F32)).astype(BF16)
            far = swap(other, 2)
            return pick(me) + columns(came, spot).astype(F32), far, other

        taps = conv_weight.astype(F32)
        full_low, normed_one, proj, logits = project(hidden_in, attn_gain, wrate.T, wqkv)
        cot_own, _ = lax.optimization_barrier((cotangent, logits))
        cot_far = swap(cot_own, 2)
        out_low, *kept = mixer_forward(proj, seg_ids, taps, logits, onorm_gain)
        middle, mid_low, normed_two, hidden, grad_gate, grad_up, full_cot, ffn_part = middle_step(out_low, wout, mlp_gain, cotangent, cot_far, full_low, wdown, wgu)
        line = Timeline(dp_size)
        cut = grad_up.shape[1] // 11 * 4
        line.scatter("gate", normed_two, grad_gate, 1)
        line.scatter("down", full_cot, hidden, 0)
        line.scatter("upz", normed_two, grad_up[:, :cut], 1)
        line.scatter("upx", normed_two, grad_up[:, cut:], 0)
        late_gate = line.after(grad_gate)
        grad_middle, full_grad_mid, grad_nout, gain_two = return_step(wout, mlp_gain, late_gate, grad_up, mid_low, full_cot, wgu)
        line.token = grad_nout
        line.move("down")
        line.scatter("out", full_grad_mid, out_low, 0)
        line.move("gate")
        line.move("upx")
        grad_proj, grad_logits, grad_conv, gain_onorm = mixer_backward(proj, seg_ids, taps, logits, onorm_gain, kept, line.after(grad_nout))
        line.token = grad_logits
        grad_logits = grad_logits.reshape(heads, tokens)
        line.move("down")
        line.move("upz")
        line.scatter("k", normed_one, grad_proj[1], 0)
        late_low, late_proj = line.after((full_low, grad_proj))
        grad_nin = jnp.einsum("ctk,cdk->td", late_proj, wqkv, preferred_element_type=F32)
        grad_nin = grad_nin + jnp.einsum("ht,dh->td", grad_logits, wrate, preferred_element_type=F32)
        full_in = late_low.astype(F32)
        scale_one = rms_scale(full_in)
        part_one, gain_one = norm_back(grad_nin, full_in * scale_one, scale_one, attn_gain)
        part_one = part_one.astype(BF16)
        line.token = (part_one, gain_one)
        wide = gain_one.shape[0]
        lanes = grad_proj.shape[2]
        thin = jnp.concatenate([gain_one.reshape(-1, lanes), gain_two.reshape(-1, lanes), jnp.pad(gain_onorm, ((0, 0), (0, lanes - HEAD_DIM)))])
        gains = butterfly(thin, "tensor", tensor_size)
        line.move("gate")
        grad_beta = jnp.einsum("ht,td->hd", line.after(grad_logits), normed_one, preferred_element_type=F32)
        line.move("out")
        small = jnp.concatenate([grad_conv.reshape(-1, lanes), grad_beta.reshape(-1, lanes), gains])
        line.rider = jnp.pad(small, ((0, -small.shape[0] % 16), (0, 0)))
        line.scatter("v", normed_one, grad_proj[2], 0, ride=True)
        line.scatter("q", normed_one, grad_proj[0], 0)
        line.move("upx")
        line.move("k")
        line.move("upz")
        late_ffn, late_one = line.after((ffn_part, part_one))
        one, one_far, _ = quarter_sum(lambda q: columns(late_one, q).astype(F32))
        ffn, ffn_far, ffn_sent = quarter_sum(lambda q: columns(late_ffn, q).astype(F32))
        line.move("v")
        line.move("out")
        grad_down = line.close("down").T
        line.token = (grad_down, ffn_sent)
        line.move("k")
        line.move("q")
        grad_in = (grad_middle + one + line.after(one_far).astype(F32)).astype(BF16)
        line.token = (line.token, grad_in)
        line.move("v")
        grad_gate_w = line.close("gate")
        grad_up_w = jnp.concatenate([line.close("upz"), line.close("upx")], axis=1)
        line.token = (grad_gate_w, grad_up_w)
        line.move("q")
        grad_gate_up = jnp.stack([line.after(grad_gate_w), grad_up_w])
        grad_out = line.close("out").T
        layer_out = (middle + ffn + line.after(ffn_far).astype(F32)).astype(BF16)
        grad_k, grad_v = line.close("k"), line.close("v")
        small = line.rider
        grad_qkv = jnp.stack([grad_k, grad_k, grad_v])
        line.token = (grad_gate_up, grad_out, layer_out, grad_qkv, small)
        grad_qkv = lax.dynamic_update_slice(grad_qkv, line.close("q")[None], (0, 0, 0))
        conv_rows, beta_rows, gain_rows = grad_conv.size // lanes, grad_beta.size // lanes, wide // lanes
        grad_conv = small[:conv_rows].reshape(grad_conv.shape)
        grad_beta = small[conv_rows : conv_rows + beta_rows].reshape(grad_beta.shape)
        gains = small[conv_rows + beta_rows :]
        mine = wide // dp_size
        grad_beta = lax.dynamic_slice_in_dim(grad_beta, lax.axis_index("dp") * mine, mine, 1).T
        return (
            layer_out,
            grad_in,
            gains[:gain_rows].reshape(-1),
            grad_qkv,
            grad_conv,
            grad_beta,
            gains[2 * gain_rows, :HEAD_DIM],
            grad_out,
            gains[gain_rows : 2 * gain_rows].reshape(-1),
            grad_gate_up,
            grad_down,
        )

    return body


def solution(mesh):
    return jax.shard_map(
        make_body(mesh.shape["dp"], mesh.shape["tensor"]),
        mesh=mesh,
        in_specs=(
            P("dp", "tensor"),
            P("dp", None),
            P(),
            P(None, None, "tensor"),
            P(None, None, "tensor"),
            P(None, "tensor"),
            P(),
            P("tensor", None),
            P(),
            P(None, None, "tensor"),
            P("tensor", None),
            P("dp", "tensor"),
        ),
        out_specs=(
            P("dp", "tensor"),
            P("dp", "tensor"),
            P(),
            P(None, "dp", "tensor"),
            P(None, None, "tensor"),
            P("dp", "tensor"),
            P(),
            P("tensor", "dp"),
            P(),
            P(None, "dp", "tensor"),
            P("tensor", "dp"),
        ),
        check_vma=False,
    )
```
